128 devices in a mesh: gx: 16 (over z, y), gy: 8 (over x, core).
Axes of the slice: x: 4, y: 4, z: 4, core: 2. Of those that a mesh axis runs over, the one named last changes fastest.
Arguments:
- spectra: bfloat16 [128, 256, 2048], P('gx', 'gy'), may hold values from -48 to 48
- resample_index: int32 [2048], replicated, may hold values from 0 to 2046
- resample_weight: float32 [2048], replicated, may hold values from 0 to 1
- disp_phase: float32 [2048], replicated, may hold values from -3.140625 to 3.140625
- surface_block: int32 [128, 256], P('gx', 'gy'), may hold values from 0 to 3
Outputs:
- enface: float32 [640, 128, 256], P(('gx', 'gy'))
The draws below stay inside these ranges and needn't reach their ends.
All inputs are finite; a program needn't handle non-finite values.
Results may differ from the reference program's by a relative error of at most 0.003.
Values sent between devices are 32-bit elements; how exact they have to be, the bound alone decides.
A program may use at most 64 MiB of HBM per device.

```python
import math
import jax
import jax.numpy as jnp
from jax import lax

NK = 2048
BLOCK = 128
KEEP = 5
NX = 128
NY = 256


def draw_spectra(key, part):
    base_key = jax.random.fold_in(key, 11)
    first, second = jax.random.split(base_key, 2)
    position = jnp.arange(NX, dtype=jnp.float32) / max(NX - 1, 1)
    ramp = jnp.power(3.0, position)
    scales = jnp.exp(jax.random.uniform(second, (NX, NY), minval=0.0, maxval=jnp.log(10.0) / 2.0))
    noise = jax.random.normal(first, (NX, NY, NK))
    values = noise * ramp[:, None, None] * scales[:, :, None]
    return jnp.clip(values, -48.0, 48.0).astype(jnp.bfloat16)


def draw_resample_index(key, part):
    base_key = jax.random.fold_in(key, 23)
    jitter = jax.random.randint(base_key, (NK,), -3, 4)
    steps = jnp.arange(NK, dtype=jnp.int32)
    target = steps * (NK + 64) // NK + jitter
    return jnp.clip(target, 0, NK - 2).astype(jnp.int32)


def draw_surface_block(key, part):
    base_key = jax.random.fold_in(key, 37)
    first, second = jax.random.split(base_key, 2)
    span = NK // (2 * BLOCK) - KEEP
    tilt = jax.random.randint(first, (), span, 2 * span + 1)
    bump = jax.random.randint(second, (NX, NY), 0, 2)
    across = jnp.arange(NX, dtype=jnp.int32)[:, None]
    return jnp.minimum(span, tilt * across // NX + bump).astype(jnp.int32)


def setup_inputs(seed: int = 0) -> dict:
    splits = jax.random.split(jax.random.key(seed), 6)
    spectra = draw_spectra(jax.random.fold_in(splits[5], 71), 0)
    resample_index = draw_resample_index(jax.random.fold_in(splits[5], 71), 0)
    resample_weight = jnp.clip(jax.random.uniform(splits[2], (NK,), jnp.float32, 0.0, 1.0), 0.0, 1.0)
    disp_phase = jnp.clip(jax.random.uniform(splits[3], (NK,), jnp.float32, -3.140625, 3.140625), -3.140625, 3.140625)
    surface_block = draw_surface_block(jax.random.fold_in(splits[5], 71), 0)
    return dict(spectra=spectra, resample_index=resample_index, resample_weight=resample_weight, disp_phase=disp_phase, surface_block=surface_block)


def dft_table(samples, block):
    depths = samples // 2
    blocks = depths // block
    rows = jnp.arange(samples, dtype=jnp.int32)
    cols = jnp.arange(depths, dtype=jnp.int32)
    turns = ((rows[:, None] * cols[None, :]) % samples).astype(jnp.float32)
    angle = (2.0 * math.pi / samples) * turns
    cosine = jnp.cos(angle).astype(jnp.bfloat16).reshape(samples, blocks, block)
    sine = jnp.sin(angle).astype(jnp.bfloat16).reshape(samples, blocks, block)
    upper = jnp.concatenate([cosine, -sine], axis=2)
    lower = jnp.concatenate([sine, cosine], axis=2)
    return jnp.concatenate([upper, lower], axis=0)


def phase_planes(lines, resample_index, resample_weight, disp_phase):
    left = jnp.take(lines, resample_index, axis=1).astype(jnp.float32)
    right = jnp.take(lines, resample_index + 1, axis=1).astype(jnp.float32)
    resampled = (1.0 - resample_weight) * left + resample_weight * right
    real_part = (resampled * jnp.cos(disp_phase)).astype(jnp.bfloat16)
    imag_part = (resampled * jnp.sin(disp_phase)).astype(jnp.bfloat16)
    return jnp.concatenate([real_part, imag_part], axis=1)


def reference(spectra, resample_index, resample_weight, disp_phase, surface_block):
    blocks = NK // (2 * BLOCK)
    table = dft_table(NK, BLOCK).reshape(2 * NK, blocks * 2 * BLOCK)

    def one_line(operand):
        lines, surface = operand
        count = lines.shape[0]
        stacked = phase_planes(lines, resample_index, resample_weight, disp_phase)
        depth = jnp.dot(stacked, table, preferred_element_type=jnp.float32).reshape(count, blocks, 2, BLOCK)
        power = depth[:, :, 0] * depth[:, :, 0] + depth[:, :, 1] * depth[:, :, 1]
        picked = surface[:, None] + jnp.arange(KEEP, dtype=jnp.int32)[None, :]
        picked = jnp.broadcast_to(picked[:, :, None], (count, KEEP, BLOCK))
        kept = jnp.take_along_axis(power, picked, axis=1)
        return kept.reshape(count, KEEP * BLOCK)

    flat = lax.map(one_line, (spectra, surface_block))
    level = jnp.sum(flat) / (NX * NY * KEEP * BLOCK) + 1e-6
    image = jnp.log1p(flat / level)
    return jnp.transpose(image, (2, 0, 1))
```

```python
import functools
import math

import jax
import jax.numpy as jnp
import numpy as np
from jax import lax
from jax.experimental import pallas as pl
from jax.experimental.pallas import tpu as pltpu
from jax.sharding import PartitionSpec as P

NK = 2048
BLOCK = 128
KEEP = 5
RADIX = 16
GX = 16
GY = 8
DEV = GX * GY
TX = 8
TY = 32
LINES = TX * TY
ROWS = KEEP * BLOCK // DEV
COUNT = 128 * 256 * KEEP * BLOCK
MESH = pl.DeviceIdType.MESH


def base_table():
    n = np.arange(RADIX)[:, None, None]
    r = np.arange(BLOCK)[None, :, None]
    m = np.arange(NK // RADIX)[None, None, :]
    angle = 2.0 * math.pi * (((RADIX * m + n) * r) % NK) / NK
    c, s = np.cos(angle), np.sin(angle)
    top = np.concatenate([c, s], axis=2)
    low = np.concatenate([-s, c], axis=2)
    return np.concatenate([top, low], axis=1).astype(np.float32)


def rot(z, k, n):
    re, im = z
    k = k % n
    if k == 0:
        return re, im
    if 4 * k == n:
        return im, -re
    if 2 * k == n:
        return -re, -im
    if 4 * k == 3 * n:
        return -im, re
    if 8 * k == n:
        h = math.sqrt(0.5)
        return h * (re + im), h * (im - re)
    if 8 * k == 3 * n:
        h = math.sqrt(0.5)
        return h * (im - re), -h * (re + im)
    c, s = math.cos(2 * math.pi * k / n), math.sin(2 * math.pi * k / n)
    return c * re + s * im, c * im - s * re


def add(a, b):
    return a[0] + b[0], a[1] + b[1]


def sub(a, b):
    return a[0] - b[0], a[1] - b[1]


def fft(z):
    n = len(z)
    if n == 1:
        return z
    even, odd = fft(z[0::2]), fft(z[1::2])
    odd = [rot(odd[k], k, n) for k in range(n // 2)]
    return [add(even[k], odd[k]) for k in range(n // 2)] + [
        sub(even[k], odd[k]) for k in range(n // 2)
    ]


def half_fft(z):
    n = len(z)
    even, odd = fft(z[0::2]), fft(z[1::2])
    return [add(even[k], rot(odd[k], k, n)) for k in range(n // 2)]


def local_kernel(spectra, par, surface, table, msg, part, z, y):
    nt = (((1,), (1,)), ((), ()))
    lines = jnp.concatenate(
        [spectra[2 * p + q] for q in range(2) for p in range(4)], axis=0
    )
    shifted = jnp.concatenate([lines[:, 1:], lines[:, :1]], axis=1)
    both = jnp.concatenate([lines, shifted], axis=0)
    col = lax.broadcasted_iota(jnp.int32, (BLOCK, NK), 1).astype(jnp.float32)
    for n in range(RADIX):
        index = par[:, n : n + 1]
        weight = par[:, RADIX + n : RADIX + n + 1]
        cosp = par[:, 2 * RADIX + n : 2 * RADIX + n + 1]
        sinp = par[:, 3 * RADIX + n : 3 * RADIX + n + 1]
        hit = jnp.where(col == index, 1.0, 0.0).astype(jnp.bfloat16)
        pair = lax.dot_general(hit, both, nt, preferred_element_type=jnp.float32)
        value = (1.0 - weight) * pair[:, :LINES] + weight * pair[:, LINES:]
        z[n, :BLOCK, :] = (value * cosp).astype(jnp.bfloat16)
        z[n, BLOCK:, :] = (value * sinp).astype(jnp.bfloat16)
    for n in range(RADIX):
        y[n] = jnp.dot(table[n], z[n], preferred_element_type=jnp.float32)

    def group(g, acc):
        r0 = pl.multiple_of(g * 8, 8)
        for q in range(2):
            lane = pl.ds(q * 128, 128)
            pts = [
                (y[n, pl.ds(r0, 8), lane], y[n, pl.ds(BLOCK + r0, 8), lane])
                for n in range(RADIX)
            ]
            power = [re * re + im * im for re, im in half_fft(pts)]
            top = surface[q : q + 1, :]
            for k in range(KEEP):
                kept = power[k]
                for s in range(1, 4):
                    kept = jnp.where(top == s, power[k + s], kept)
                acc = acc + kept
                msg[pl.ds(k * BLOCK + r0, 8), q, :] = kept
        return acc

    acc = lax.fori_loop(0, BLOCK // 8, group, jnp.zeros((8, 128), jnp.float32))
    part[...] = jnp.sum(acc, axis=0, keepdims=True).reshape(1, 1, 128)


def exchange_kernel(msg, part, recv, sums, sem):
    gx, gy = lax.axis_index("gx"), lax.axis_index("gy")
    me = gx * GY + gy

    def peer(i):
        dz, dy, dx, dc = i // 32, (i // 8) % 4, (i // 2) % 4, i % 2
        pz, py = (gx // 4 + dz) % 4, (gx % 4 + dy) % 4
        px, pc = (gy // 2 + dx) % 4, (gy % 2 + dc) % 2
        return pz * 4 + py, px * 2 + pc

    barrier = pltpu.get_barrier_semaphore()

    def greet(i, _):
        pl.semaphore_signal(barrier, inc=1, device_id=peer(i), device_id_type=MESH)
        return 0

    lax.fori_loop(1, DEV, greet, 0)
    own = pltpu.make_async_copy(msg.at[pl.ds(ROWS * me, ROWS)], recv.at[me], sem.at[4])
    own.start()
    own_sum = pltpu.make_async_copy(part, sums.at[pl.ds(me, 1)], sem.at[5])
    own_sum.start()
    pl.semaphore_wait(barrier, DEV - 1)

    def send(i, _):
        px, py = peer(i)
        pltpu.make_async_remote_copy(
            src_ref=msg.at[pl.ds(ROWS * (px * GY + py), ROWS)],
            dst_ref=recv.at[me],
            send_sem=sem.at[0],
            recv_sem=sem.at[1],
            device_id=(px, py),
            device_id_type=MESH,
        ).start()
        pltpu.make_async_remote_copy(
            src_ref=part,
            dst_ref=sums.at[pl.ds(me, 1)],
            send_sem=sem.at[2],
            recv_sem=sem.at[3],
            device_id=(px, py),
            device_id_type=MESH,
        ).start()
        return 0

    lax.fori_loop(1, DEV, send, 0)
    most = recv.at[pl.ds(0, DEV - 1)]
    few = sums.at[pl.ds(0, DEV - 1)]
    pltpu.make_async_copy(most, most, sem.at[0]).wait()
    pltpu.make_async_copy(few, few, sem.at[2]).wait()
    own.wait()
    own_sum.wait()
    pltpu.make_async_copy(few, few, sem.at[3]).wait()
    pltpu.make_async_copy(most, most, sem.at[1]).wait()


def place_kernel(recv, sums, out):
    level = jnp.sum(sums[...]) / COUNT + 1e-6
    lane = lax.broadcasted_iota(jnp.int32, (8, 128), 1) // TY
    sub_ = lax.broadcasted_iota(jnp.int32, (8, 128), 0) // 2
    step = (sub_ - lane) % 4

    def body(gx, _):
        x0 = pl.multiple_of(gx * TX, TX)
        for r in range(ROWS):
            for h in range(2):
                v = recv[pl.ds(gx * GY + 4 * h, 4), r].reshape(8, 128)
                w = v
                for k in range(1, 4):
                    turned = pltpu.roll(pltpu.roll(v, 2 * k, 0), (128 - TY * k) % 128, 1)
                    w = jnp.where(step == k, turned, w)
                out[r, pl.ds(x0, TX), h * 128 : (h + 1) * 128] = jnp.log1p(w / level)
        return 0

    lax.fori_loop(0, GX, body, 0)


def on_device(spectra, resample_index, resample_weight, disp_phase, surface_block):
    f32 = jnp.float32
    vm = pl.BlockSpec(memory_space=pltpu.VMEM)
    table = jnp.asarray(base_table(), jnp.bfloat16)
    par = jnp.concatenate(
        [
            resample_index.astype(f32).reshape(BLOCK, RADIX),
            resample_weight.reshape(BLOCK, RADIX),
            jnp.cos(disp_phase).reshape(BLOCK, RADIX),
            jnp.sin(disp_phase).reshape(BLOCK, RADIX),
        ],
        axis=1,
    )
    surface = jnp.transpose(surface_block.reshape(4, 2, TY), (1, 0, 2)).reshape(2, 128)
    msg, part = pl.pallas_call(
        local_kernel,
        out_shape=(
            jax.ShapeDtypeStruct((KEEP * BLOCK, 2, 128), f32),
            jax.ShapeDtypeStruct((1, 1, 128), f32),
        ),
        in_specs=[vm] * 4,
        out_specs=[vm] * 2,
        scratch_shapes=[
            pltpu.VMEM((RADIX, 2 * BLOCK, LINES), jnp.bfloat16),
            pltpu.VMEM((RADIX, 2 * BLOCK, LINES), f32),
        ],
        compiler_params=pltpu.CompilerParams(vmem_limit_bytes=48 * 1024 * 1024),
        name="local",
    )(spectra, par, surface, table)
    recv, sums = pl.pallas_call(
        exchange_kernel,
        out_shape=(
            jax.ShapeDtypeStruct((DEV, ROWS, 2, 128), f32),
            jax.ShapeDtypeStruct((DEV, 1, 128), f32),
        ),
        in_specs=[vm] * 2,
        out_specs=[vm] * 2,
        scratch_shapes=[pltpu.SemaphoreType.DMA((6,))],
        compiler_params=pltpu.CompilerParams(collective_id=0, has_side_effects=True),
        name="exchange",
    )(msg, part)
    return pl.pallas_call(
        place_kernel,
        out_shape=jax.ShapeDtypeStruct((ROWS, GX * TX, GY * TY), f32),
        in_specs=[vm] * 2,
        out_specs=vm,
        name="place",
    )(recv, sums)


def solution(mesh):
    return jax.shard_map(
        on_device,
        mesh=mesh,
        in_specs=(P("gx", "gy", None), P(), P(), P(), P("gx", "gy")),
        out_specs=P(("gx", "gy"), None, None),
        check_vma=False,
    )
```

```python
import functools
import math

import jax
import jax.numpy as jnp
import numpy as np
from jax import lax
from jax.experimental import pallas as pl
from jax.experimental.pallas import tpu as pltpu
from jax.sharding import PartitionSpec as P

NK = 2048
BLOCK = 128
KEEP = 5
RADIX = 16
GX = 16
GY = 8
DEV = GX * GY
TX = 8
TY = 32
LINES = TX * TY
ROWS = KEEP * BLOCK // DEV
COUNT = 128 * 256 * KEEP * BLOCK
MESH = pl.DeviceIdType.MESH


def base_table():
    c = np.arange(RADIX)[:, None, None]
    b = np.arange(NK // (2 * RADIX))[None, :, None]
    m = np.arange(BLOCK)[None, None, :]
    angle = 2.0 * math.pi * ((m * (RADIX * b + c)) % NK) / NK
    cos, sin = np.cos(angle), np.sin(angle)
    top = np.concatenate([cos, sin], axis=2)
    low = np.concatenate([-sin, cos], axis=2)
    return np.concatenate([top, low], axis=1).astype(np.float32)


def rot(z, k, n):
    re, im = z
    k = k % n
    if k == 0:
        return re, im
    if 4 * k == n:
        return im, -re
    if 2 * k == n:
        return -re, -im
    if 4 * k == 3 * n:
        return -im, re
    if 8 * k == n:
        h = math.sqrt(0.5)
        return h * (re + im), h * (im - re)
    if 8 * k == 3 * n:
        h = math.sqrt(0.5)
        return h * (im - re), -h * (re + im)
    c, s = math.cos(2 * math.pi * k / n), math.sin(2 * math.pi * k / n)
    return c * re + s * im, c * im - s * re


def add(a, b):
    return a[0] + b[0], a[1] + b[1]


def sub(a, b):
    return a[0] - b[0], a[1] - b[1]


def fft(z):
    n = len(z)
    if n == 1:
        return z
    even, odd = fft(z[0::2]), fft(z[1::2])
    odd = [rot(odd[k], k, n) for k in range(n // 2)]
    return [add(even[k], odd[k]) for k in range(n // 2)] + [
        sub(even[k], odd[k]) for k in range(n // 2)
    ]


def peer(i, gx, gy):
    dz, dy, dx, dc = i // 32, (i // 8) % 4, (i // 2) % 4, i % 2
    pz, py = (gx // 4 + dz) % 4, (gx % 4 + dy) % 4
    px, pc = (gy // 2 + dx) % 4, (gy % 2 + dc) % 2
    return pz * 4 + py, px * 2 + pc


def main_kernel(
    spectra, index, weight, phase, surface, table, recv, sums,
    both, params, idx, surf, tab, x, y, msg, part, load, sem,
):
    gx, gy = lax.axis_index("gx"), lax.axis_index("gy")
    me = gx * GY + gy
    barrier = pltpu.get_barrier_semaphore()
    f32 = jnp.float32

    small = [
        pltpu.make_async_copy(index, idx, load.at[0]),
        pltpu.make_async_copy(weight, params.at[0], load.at[1]),
        pltpu.make_async_copy(phase, params.at[1], load.at[2]),
        pltpu.make_async_copy(surface, surf, load.at[3]),
    ]
    tiles = [
        pltpu.make_async_copy(
            spectra.at[2 * p + q], both.at[pl.ds((4 * q + p) * TY, TY)], load.at[4 + 4 * q + p]
        )
        for q in range(2)
        for p in range(4)
    ]
    big = pltpu.make_async_copy(table, tab, load.at[12])
    for copy in tiles + small + [big]:
        copy.start()

    def greet(i, _):
        pl.semaphore_signal(barrier, inc=1, device_id=peer(i, gx, gy), device_id_type=MESH)
        return 0

    lax.fori_loop(1, DEV, greet, 0)

    for copy in tiles + small:
        copy.wait()
    lines = both[:LINES, :]
    both[LINES:, :] = jnp.concatenate([lines[:, 1:], lines[:, :1]], axis=1)
    row = lax.broadcasted_iota(jnp.int32, (NK, 2 * BLOCK), 0)
    for j in range(RADIX // 2):
        pick = jnp.concatenate([idx[2 * j : 2 * j + 1, :], idx[2 * j + 1 : 2 * j + 2, :]], axis=1)
        hit = jnp.where(row == pick, 1.0, 0.0).astype(jnp.bfloat16)
        pair = jnp.dot(both[...], hit, preferred_element_type=f32)
        for h in range(2):
            lane = slice(h * BLOCK, (h + 1) * BLOCK)
            w = params[0, 2 * j + h : 2 * j + h + 1, :]
            x[2 * j + h] = (1.0 - w) * pair[:LINES, lane] + w * pair[LINES:, lane]
    cosp = jnp.cos(params[1])
    sinp = jnp.sin(params[1])
    params[0] = cosp
    params[1] = sinp

    def spread(g, _):
        r0 = pl.multiple_of(g * 16, 16)
        halves = []
        for h in range(2):
            value = [x[n, pl.ds(r0 + 8 * h, 8), :] for n in range(RADIX)]
            halves.append(
                fft([(v * params[0, n : n + 1, :], v * params[1, n : n + 1, :]) for n, v in enumerate(value)])
            )
        for c in range(RADIX):
            for o in range(2):
                both_rows = jnp.concatenate([halves[0][c][o], halves[1][c][o]], axis=0)
                y[c, pl.ds(r0, 16), o * BLOCK : (o + 1) * BLOCK] = both_rows.astype(jnp.bfloat16)
        return 0

    lax.fori_loop(0, LINES // 16, spread, 0)
    big.wait()
    nt = (((1,), (1,)), ((), ()))
    tops = [
        jnp.concatenate([surf[2 * p + q : 2 * p + q + 1, :] for p in range(4)], axis=1)
        for q in range(2)
    ]
    acc = jnp.zeros((8, 128), f32)
    for c in range(RADIX):
        depth = lax.dot_general(tab[c], y[c], nt, preferred_element_type=f32)
        power = depth[:64] * depth[:64] + depth[64:] * depth[64:]
        for q in range(2):
            tile = [power[8 * b : 8 * b + 8, q * 128 : (q + 1) * 128] for b in range(8)]
            for k in range(KEEP):
                kept = tile[k]
                for s in range(1, 4):
                    kept = jnp.where(tops[q] == s, tile[k + s], kept)
                acc = acc + kept
                msg[pl.ds(k * BLOCK + c, 8, stride=RADIX), q, :] = kept
    part[...] = jnp.sum(acc, axis=0, keepdims=True).reshape(1, 1, 128)

    own = pltpu.make_async_copy(msg.at[pl.ds(ROWS * me, ROWS)], recv.at[me], sem.at[4])
    own.start()
    own_sum = pltpu.make_async_copy(part, sums.at[pl.ds(me, 1)], sem.at[5])
    own_sum.start()
    pl.semaphore_wait(barrier, DEV - 1)

    def send(i, _):
        px, py = peer(DEV - i, gx, gy)
        pltpu.make_async_remote_copy(
            src_ref=part,
            dst_ref=sums.at[pl.ds(me, 1)],
            send_sem=sem.at[2],
            recv_sem=sem.at[3],
            device_id=(px, py),
            device_id_type=MESH,
        ).start()
        pltpu.make_async_remote_copy(
            src_ref=msg.at[pl.ds(ROWS * (px * GY + py), ROWS)],
            dst_ref=recv.at[me],
            send_sem=sem.at[0],
            recv_sem=sem.at[1],
            device_id=(px, py),
            device_id_type=MESH,
        ).start()
        return 0

    lax.fori_loop(1, DEV, send, 0)
    most = recv.at[pl.ds(0, DEV - 1)]
    few = sums.at[pl.ds(0, DEV - 1)]
    pltpu.make_async_copy(most, most, sem.at[0]).wait()
    pltpu.make_async_copy(few, few, sem.at[2]).wait()
    own.wait()
    own_sum.wait()
    pltpu.make_async_copy(few, few, sem.at[3]).wait()
    pltpu.make_async_copy(most, most, sem.at[1]).wait()


def place_kernel(recv, sums, out):
    level = jnp.sum(sums[...]) / COUNT + 1e-6
    lane = lax.broadcasted_iota(jnp.int32, (8, 128), 1) // TY
    sub_ = lax.broadcasted_iota(jnp.int32, (8, 128), 0) // 2
    step = (sub_ - lane) % 4

    def body(gx, _):
        x0 = pl.multiple_of(gx * TX, TX)
        for r in range(ROWS):
            for h in range(2):
                v = recv[pl.ds(gx * GY + 4 * h, 4), r].reshape(8, 128)
                w = v
                for k in range(1, 4):
                    turned = pltpu.roll(pltpu.roll(v, 2 * k, 0), (128 - TY * k) % 128, 1)
                    w = jnp.where(step == k, turned, w)
                out[r, pl.ds(x0, TX), h * 128 : (h + 1) * 128] = jnp.log1p(w / level)
        return 0

    lax.fori_loop(0, GX, body, 0)


def on_device(spectra, resample_index, resample_weight, disp_phase, surface_block):
    f32 = jnp.float32
    bf16 = jnp.bfloat16
    vm = pl.BlockSpec(memory_space=pltpu.VMEM)
    hbm = pl.BlockSpec(memory_space=pltpu.HBM)
    table = jnp.asarray(base_table(), bf16)
    recv, sums = pl.pallas_call(
        main_kernel,
        out_shape=(
            jax.ShapeDtypeStruct((DEV, ROWS, 2, 128), f32),
            jax.ShapeDtypeStruct((DEV, 1, 128), f32),
        ),
        in_specs=[hbm] * 6,
        out_specs=[vm] * 2,
        scratch_shapes=[
            pltpu.VMEM((2 * LINES, NK), bf16),
            pltpu.VMEM((2, RADIX, BLOCK), f32),
            pltpu.VMEM((RADIX, BLOCK), jnp.int32),
            pltpu.VMEM((TX, TY), jnp.int32),
            pltpu.VMEM((RADIX, BLOCK, 2 * BLOCK), bf16),
            pltpu.VMEM((RADIX, LINES, BLOCK), f32),
            pltpu.VMEM((RADIX, LINES, 2 * BLOCK), bf16),
            pltpu.VMEM((KEEP * BLOCK, 2, 128), f32),
            pltpu.VMEM((1, 1, 128), f32),
            pltpu.SemaphoreType.DMA((13,)),
            pltpu.SemaphoreType.DMA((6,)),
        ],
        compiler_params=pltpu.CompilerParams(
            collective_id=0, has_side_effects=True, vmem_limit_bytes=48 * 1024 * 1024
        ),
        name="main",
    )(
        spectra,
        resample_index.reshape(RADIX, BLOCK),
        resample_weight.reshape(RADIX, BLOCK),
        disp_phase.reshape(RADIX, BLOCK),
        surface_block,
        table,
    )
    return pl.pallas_call(
        place_kernel,
        out_shape=jax.ShapeDtypeStruct((ROWS, GX * TX, GY * TY), f32),
        in_specs=[vm] * 2,
        out_specs=vm,
        name="place",
    )(recv, sums)


def solution(mesh):
    return jax.shard_map(
        on_device,
        mesh=mesh,
        in_specs=(P("gx", "gy", None), P(), P(), P(), P("gx", "gy")),
        out_specs=P(("gx", "gy"), None, None),
        check_vma=False,
    )
```

```python
import itertools
import math

import jax
import jax.numpy as jnp
import numpy as np
from jax import lax
from jax.experimental import pallas as pl
from jax.experimental.pallas import tpu as pltpu
from jax.sharding import PartitionSpec as P

NK = 2048
BLOCK = 128
KEEP = 5
RADIX = 16
GX = 16
GY = 8
DEV = GX * GY
TX = 8
TY = 32
LINES = TX * TY
ROWS = KEEP * BLOCK // DEV
COUNT = 128 * 256 * KEEP * BLOCK
MESH = pl.DeviceIdType.MESH
VMEM_BYTES = 67043328


def base_table():
    c = np.arange(RADIX)[:, None, None]
    b = np.arange(NK // (2 * RADIX))[None, :, None]
    m = np.arange(BLOCK)[None, None, :]
    angle = 2.0 * math.pi * ((m * (RADIX * b + c)) % NK) / NK
    cos, sin = np.cos(angle), np.sin(angle)
    top = np.concatenate([cos, sin], axis=2)
    low = np.concatenate([-sin, cos], axis=2)
    return np.concatenate([top, low], axis=1).astype(np.float32)


def rot(z, k, n):
    re, im = z
    k = k % n
    if k == 0:
        return re, im
    if 4 * k == n:
        return im, -re
    if 2 * k == n:
        return -re, -im
    if 4 * k == 3 * n:
        return -im, re
    if 8 * k == n:
        h = math.sqrt(0.5)
        return h * (re + im), h * (im - re)
    if 8 * k == 3 * n:
        h = math.sqrt(0.5)
        return h * (im - re), -h * (re + im)
    c, s = math.cos(2 * math.pi * k / n), math.sin(2 * math.pi * k / n)
    return c * re + s * im, c * im - s * re


def add(a, b):
    return a[0] + b[0], a[1] + b[1]


def sub(a, b):
    return a[0] - b[0], a[1] - b[1]


def fft(z):
    n = len(z)
    if n == 1:
        return z
    even, odd = fft(z[0::2]), fft(z[1::2])
    odd = [rot(odd[k], k, n) for k in range(n // 2)]
    return [add(even[k], odd[k]) for k in range(n // 2)] + [
        sub(even[k], odd[k]) for k in range(n // 2)
    ]


def hops(o):
    return sum((0, 1, 2, 1)[v] for v in o[:3])


OFFSETS = sorted(
    [o for o in itertools.product(range(4), range(4), range(4), range(2)) if any(o)],
    key=lambda o: (-hops(o), o),
)


def main_kernel(
    spectra, index, weight, phase, surface, table, recv, sums,
    both, params, idx, surf, tab, hits, x, y, msg, part, load, sem,
):
    f32, bf16 = jnp.float32, jnp.bfloat16
    half = LINES // 2
    gx, gy = lax.axis_index("gx"), lax.axis_index("gy")
    me = gx * GY + gy
    zs = [(gx // 4 + d) % 4 for d in range(4)]
    ys = [(gx % 4 + d) % 4 for d in range(4)]
    xs = [(gy // 2 + d) % 4 for d in range(4)]
    cs = [(gy % 2 + d) % 2 for d in range(2)]
    zy = [[z * 4 + v for v in ys] for z in zs]
    xc = [[v * 2 + c for c in cs] for v in xs]
    peers = [(zy[o[0]][o[1]], xc[o[2]][o[3]]) for o in OFFSETS]
    barrier = pltpu.get_barrier_semaphore()

    small = [
        pltpu.make_async_copy(index, idx, load.at[0]),
        pltpu.make_async_copy(weight, params.at[0], load.at[1]),
        pltpu.make_async_copy(phase, params.at[1], load.at[2]),
        pltpu.make_async_copy(surface, surf, load.at[3]),
    ]
    tiles = [
        pltpu.make_async_copy(
            spectra.at[2 * p + q], both.at[q, pl.ds(p * TY, TY)], load.at[4 + 4 * q + p]
        )
        for q in range(2)
        for p in range(4)
    ]
    big = pltpu.make_async_copy(table, tab, load.at[12])
    for copy in small + tiles + [big]:
        copy.start()
    for to in peers:
        pl.semaphore_signal(barrier, inc=1, device_id=to, device_id_type=MESH)
    for copy in small:
        copy.wait()
    cosp = jnp.cos(params[1])
    sinp = jnp.sin(params[1])
    params[1] = cosp
    params[2] = sinp
    tops = [
        jnp.concatenate([surf[2 * p + q : 2 * p + q + 1, :] for p in range(4)], axis=1)
        for q in range(2)
    ]
    row = lax.broadcasted_iota(jnp.int32, (NK, 2 * BLOCK), 0)
    nt = (((1,), (1,)), ((), ()))

    def compute(q, acc):
        for copy in tiles[4 * q : 4 * q + 4]:
            copy.wait()
        lines = both[q, :half, :]
        both[q, half:, :] = jnp.concatenate([lines[:, 1:], lines[:, :1]], axis=1)
        for j in range(RADIX // 2):
            if q == 0:
                pick = jnp.concatenate(
                    [idx[2 * j : 2 * j + 1, :], idx[2 * j + 1 : 2 * j + 2, :]], axis=1
                )
                hits[j] = jnp.where(row == pick, 1.0, 0.0).astype(bf16)
            pair = jnp.dot(both[q], hits[j], preferred_element_type=f32)
            for h in range(2):
                lane = slice(h * BLOCK, (h + 1) * BLOCK)
                w = params[0, 2 * j + h : 2 * j + h + 1, :]
                x[2 * j + h] = (1.0 - w) * pair[:half, lane] + w * pair[half:, lane]

        def spread(g, _):
            r0 = pl.multiple_of(g * 16, 16)
            parts = []
            for n in range(RADIX):
                v = x[n, pl.ds(r0, 16), :]
                parts.append(
                    [
                        (v * params[1 + o, n : n + 1, :]).astype(bf16).astype(f32)
                        for o in range(2)
                    ]
                )
            low = fft([(re[:8], im[:8]) for re, im in parts])
            high = fft([(re[8:], im[8:]) for re, im in parts])
            for c in range(RADIX):
                for o in range(2):
                    rows = jnp.concatenate([low[c][o], high[c][o]], axis=0)
                    y[c, pl.ds(r0, 16), o * BLOCK : (o + 1) * BLOCK] = rows.astype(bf16)
            return 0

        lax.fori_loop(0, half // 16, spread, 0)
        if q == 0:
            big.wait()
        for c in range(RADIX):
            depth = lax.dot_general(tab[c], y[c], nt, preferred_element_type=f32)
            power = depth[:64] * depth[:64] + depth[64:] * depth[64:]
            tile = [power[8 * b : 8 * b + 8] for b in range(8)]
            for k in range(KEEP):
                kept = tile[k]
                for s in range(1, 4):
                    kept = jnp.where(tops[q] == s, tile[k + s], kept)
                acc = acc + kept
                msg[pl.ds((q * KEEP + k) * BLOCK + c, 8, stride=RADIX), 0, :] = kept
        return acc

    def slab(q, dest):
        return msg.at[pl.ds(q * KEEP * BLOCK + ROWS * dest, ROWS)]

    def landing(q):
        return recv.at[pl.ds((2 * me + q) * ROWS, ROWS)]

    def send(q):
        for px, py in peers:
            pltpu.make_async_remote_copy(
                src_ref=slab(q, px * GY + py),
                dst_ref=landing(q),
                send_sem=sem.at[2 * q],
                recv_sem=sem.at[2 * q + 1],
                device_id=(px, py),
                device_id_type=MESH,
            ).start()

    acc = compute(0, jnp.zeros((8, 128), f32))
    pl.semaphore_wait(barrier, DEV - 1)
    send(0)
    acc = compute(1, acc)
    part[...] = jnp.sum(acc, axis=0, keepdims=True).reshape(1, 1, 128)
    for px, py in peers:
        pltpu.make_async_remote_copy(
            src_ref=part,
            dst_ref=sums.at[pl.ds(me, 1)],
            send_sem=sem.at[4],
            recv_sem=sem.at[5],
            device_id=(px, py),
            device_id_type=MESH,
        ).start()
    send(1)
    own = [pltpu.make_async_copy(slab(q, me), landing(q), sem.at[6 + q]) for q in range(2)]
    own.append(pltpu.make_async_copy(part, sums.at[pl.ds(me, 1)], sem.at[8]))
    for copy in own:
        copy.start()
    for copy in own:
        copy.wait()
    most = recv.at[pl.ds(0, (DEV - 1) * ROWS)]
    few = sums.at[pl.ds(0, DEV - 1)]
    for ref, s in ((most, 0), (most, 2), (few, 4), (most, 1), (few, 5), (most, 3)):
        pltpu.make_async_copy(ref, ref, sem.at[s]).wait()


def place_kernel(recv, sums, out):
    level = jnp.sum(sums[...]) / COUNT + 1e-6
    scale = 1.0 / jnp.full((8, 128), level, jnp.float32)
    lane = lax.broadcasted_iota(jnp.int32, (8, 128), 1) // TY
    line = lax.broadcasted_iota(jnp.int32, (8, 128), 0) // 2
    step = (line - lane) % 4

    def body(gx, _):
        x0 = pl.multiple_of(gx * TX, TX)
        for h in range(2):
            for r in range(ROWS):
                v = recv[pl.ds((gx * GY + 4 * h) * 2 * ROWS + r, 8, stride=ROWS), 0, :]
                w = v
                for k in range(1, 4):
                    turned = pltpu.roll(pltpu.roll(v, 2 * k, 0), 128 - TY * k, 1)
                    w = jnp.where(step == k, turned, w)
                out[r, pl.ds(x0, TX), h * 128 : (h + 1) * 128] = jnp.log(1.0 + w * scale)
        return 0

    lax.fori_loop(0, GX, body, 0, unroll=2)


def on_device(spectra, resample_index, resample_weight, disp_phase, surface_block):
    f32 = jnp.float32
    bf16 = jnp.bfloat16
    vm = pl.BlockSpec(memory_space=pltpu.VMEM)
    hbm = pl.BlockSpec(memory_space=pltpu.HBM)
    table = jnp.asarray(base_table(), bf16)
    recv, sums = pl.pallas_call(
        main_kernel,
        out_shape=(
            jax.ShapeDtypeStruct((DEV * ROWS * 2, 1, 128), f32),
            jax.ShapeDtypeStruct((DEV, 1, 128), f32),
        ),
        in_specs=[hbm] * 6,
        out_specs=[vm] * 2,
        scratch_shapes=[
            pltpu.VMEM((2, LINES, NK), bf16),
            pltpu.VMEM((3, RADIX, BLOCK), f32),
            pltpu.VMEM((RADIX, BLOCK), jnp.int32),
            pltpu.VMEM((TX, TY), jnp.int32),
            pltpu.VMEM((RADIX, BLOCK, 2 * BLOCK), bf16),
            pltpu.VMEM((RADIX // 2, NK, 2 * BLOCK), bf16),
            pltpu.VMEM((RADIX, LINES // 2, BLOCK), f32),
            pltpu.VMEM((RADIX, LINES // 2, 2 * BLOCK), bf16),
            pltpu.VMEM((2 * KEEP * BLOCK, 1, 128), f32),
            pltpu.VMEM((1, 1, 128), f32),
            pltpu.SemaphoreType.DMA((13,)),
            pltpu.SemaphoreType.DMA((9,)),
        ],
        compiler_params=pltpu.CompilerParams(
            collective_id=0, has_side_effects=True, vmem_limit_bytes=VMEM_BYTES
        ),
        name="main",
    )(
        spectra,
        resample_index.reshape(RADIX, BLOCK),
        resample_weight.reshape(RADIX, BLOCK),
        disp_phase.reshape(RADIX, BLOCK),
        surface_block,
        table,
    )
    return pl.pallas_call(
        place_kernel,
        out_shape=jax.ShapeDtypeStruct((ROWS, GX * TX, GY * TY), f32),
        in_specs=[vm] * 2,
        out_specs=vm,
        name="place",
    )(recv, sums)


def solution(mesh):
    return jax.shard_map(
        on_device,
        mesh=mesh,
        in_specs=(P("gx", "gy", None), P(), P(), P(), P("gx", "gy")),
        out_specs=P(("gx", "gy"), None, None),
        check_vma=False,
    )
```

```python
import itertools
import math

import jax
import jax.numpy as jnp
import numpy as np
from jax import lax
from jax.experimental import pallas as pl
from jax.experimental.pallas import tpu as pltpu
from jax.sharding import PartitionSpec as P

NK = 2048
BLOCK = 128
KEEP = 5
RADIX = 16
GX = 16
GY = 8
DEV = GX * GY
TX = 8
TY = 32
LINES = TX * TY
ROWS = KEEP * BLOCK // DEV
COUNT = 128 * 256 * KEEP * BLOCK
MESH = pl.DeviceIdType.MESH
VMEM_BYTES = 67043328 - 660 * 1024


def base_table():
    c = np.arange(RADIX)[:, None, None]
    b = np.arange(NK // (2 * RADIX))[None, :, None]
    m = np.arange(BLOCK)[None, None, :]
    angle = 2.0 * math.pi * ((m * (RADIX * b + c)) % NK) / NK
    cos, sin = np.cos(angle), np.sin(angle)
    top = np.concatenate([cos, sin], axis=2)
    low = np.concatenate([-sin, cos], axis=2)
    return np.concatenate([top, low], axis=1).astype(np.float32)


def rot(z, k, n):
    re, im = z
    k = k % n
    if k == 0:
        return re, im
    if 4 * k == n:
        return im, -re
    if 2 * k == n:
        return -re, -im
    if 4 * k == 3 * n:
        return -im, re
    if 8 * k == n:
        h = math.sqrt(0.5)
        return h * (re + im), h * (im - re)
    if 8 * k == 3 * n:
        h = math.sqrt(0.5)
        return h * (im - re), -h * (re + im)
    c, s = math.cos(2 * math.pi * k / n), math.sin(2 * math.pi * k / n)
    return c * re + s * im, c * im - s * re


def add(a, b):
    return a[0] + b[0], a[1] + b[1]


def sub(a, b):
    return a[0] - b[0], a[1] - b[1]


def fft(z):
    n = len(z)
    if n == 1:
        return z
    even, odd = fft(z[0::2]), fft(z[1::2])
    odd = [rot(odd[k], k, n) for k in range(n // 2)]
    return [add(even[k], odd[k]) for k in range(n // 2)] + [
        sub(even[k], odd[k]) for k in range(n // 2)
    ]


def hops(o):
    return sum((0, 1, 2, 1)[v] for v in o[:3])


OFFSETS = sorted(
    [o for o in itertools.product(range(4), range(4), range(4), range(2)) if any(o)],
    key=lambda o: (-hops(o), o),
)


def main_kernel(
    spectra, index, weight, phase, surface, table, out,
    both, params, idx, surf, tab, hits, x, y, msg, part, recv, sums, load, sem,
):
    f32, bf16 = jnp.float32, jnp.bfloat16
    half = LINES // 2
    gx, gy = lax.axis_index("gx"), lax.axis_index("gy")
    me = gx * GY + gy
    zs = [(gx // 4 + d) % 4 for d in range(4)]
    ys = [(gx % 4 + d) % 4 for d in range(4)]
    xs = [(gy // 2 + d) % 4 for d in range(4)]
    cs = [(gy % 2 + d) % 2 for d in range(2)]
    zy = [[z * 4 + v for v in ys] for z in zs]
    xc = [[v * 2 + c for c in cs] for v in xs]
    peers = [(zy[o[0]][o[1]], xc[o[2]][o[3]]) for o in OFFSETS]
    barrier = pltpu.get_barrier_semaphore()

    small = [
        pltpu.make_async_copy(index, idx, load.at[0]),
        pltpu.make_async_copy(weight, params.at[0], load.at[1]),
        pltpu.make_async_copy(phase, params.at[1], load.at[2]),
        pltpu.make_async_copy(surface, surf, load.at[3]),
    ]
    tiles = [
        pltpu.make_async_copy(
            spectra.at[2 * p + q], both.at[q, pl.ds(p * TY, TY)], load.at[4 + 4 * q + p]
        )
        for q in range(2)
        for p in range(4)
    ]
    big = pltpu.make_async_copy(table, tab, load.at[12])
    for copy in small + tiles + [big]:
        copy.start()
    for to in peers:
        pl.semaphore_signal(barrier, inc=1, device_id=to, device_id_type=MESH)
    for copy in small:
        copy.wait()
    cosp = jnp.cos(params[1])
    sinp = jnp.sin(params[1])
    params[1] = cosp
    params[2] = sinp
    tops = [
        jnp.concatenate([surf[2 * p + q : 2 * p + q + 1, :] for p in range(4)], axis=1)
        for q in range(2)
    ]
    row = lax.broadcasted_iota(jnp.int32, (BLOCK, 2 * BLOCK), 0).astype(jnp.int16)
    one = jnp.ones((BLOCK, 2 * BLOCK), bf16)
    zero = jnp.zeros((BLOCK, 2 * BLOCK), bf16)
    nt = (((1,), (1,)), ((), ()))

    def compute(q, acc):
        for copy in tiles[4 * q : 4 * q + 4]:
            copy.wait()
        lines = both[q, :half, :]
        both[q, half:, :] = jnp.concatenate([lines[:, 1:], lines[:, :1]], axis=1)
        for j in range(RADIX // 2):
            if q == 0:
                pick = jnp.concatenate(
                    [idx[2 * j : 2 * j + 1, :], idx[2 * j + 1 : 2 * j + 2, :]], axis=1
                )
                pick = pick.astype(jnp.int16)
                for k in range(NK // 128):
                    seen = row + jnp.int16(128 * k) == pick
                    hits[j, k * 128 : (k + 1) * 128, :] = jnp.where(seen, one, zero)
            pair = jnp.dot(both[q], hits[j], preferred_element_type=f32)
            for h in range(2):
                lane = slice(h * BLOCK, (h + 1) * BLOCK)
                w = params[0, 2 * j + h : 2 * j + h + 1, :]
                x[2 * j + h] = (1.0 - w) * pair[:half, lane] + w * pair[half:, lane]

        def spread(g, _):
            r0 = pl.multiple_of(g * 16, 16)
            parts = []
            for n in range(RADIX):
                v = x[n, pl.ds(r0, 16), :]
                parts.append(
                    [
                        (v * params[1 + o, n : n + 1, :]).astype(bf16).astype(f32)
                        for o in range(2)
                    ]
                )
            low = fft([(re[:8], im[:8]) for re, im in parts])
            high = fft([(re[8:], im[8:]) for re, im in parts])
            for c in range(RADIX):
                for o in range(2):
                    rows = jnp.concatenate([low[c][o], high[c][o]], axis=0)
                    y[c, pl.ds(r0, 16), o * BLOCK : (o + 1) * BLOCK] = rows.astype(bf16)
            return 0

        lax.fori_loop(0, half // 16, spread, 0)
        if q == 0:
            big.wait()
        for c in range(RADIX):
            depth = lax.dot_general(tab[c], y[c], nt, preferred_element_type=f32)
            power = depth[:64] * depth[:64] + depth[64:] * depth[64:]
            tile = [power[8 * b : 8 * b + 8] for b in range(8)]
            for k in range(KEEP):
                kept = tile[k]
                for s in range(1, 4):
                    kept = jnp.where(tops[q] == s, tile[k + s], kept)
                acc = acc + kept
                msg[pl.ds((q * KEEP + k) * BLOCK + c, 8, stride=RADIX), 0, :] = kept
        return acc

    def slab(q, dest):
        return msg.at[pl.ds(q * KEEP * BLOCK + ROWS * dest, ROWS)]

    def landing(q):
        return recv.at[pl.ds((2 * me + q) * ROWS, ROWS)]

    def send(q):
        for px, py in peers:
            pltpu.make_async_remote_copy(
                src_ref=slab(q, px * GY + py),
                dst_ref=landing(q),
                send_sem=sem.at[2 * q],
                recv_sem=sem.at[2 * q + 1],
                device_id=(px, py),
                device_id_type=MESH,
            ).start()

    acc = compute(0, jnp.zeros((8, 128), f32))
    pl.semaphore_wait(barrier, DEV - 1)
    send(0)
    acc = compute(1, acc)
    part[...] = jnp.sum(acc, axis=0, keepdims=True).reshape(1, 1, 128)
    for px, py in peers:
        pltpu.make_async_remote_copy(
            src_ref=part,
            dst_ref=sums.at[pl.ds(me, 1)],
            send_sem=sem.at[4],
            recv_sem=sem.at[5],
            device_id=(px, py),
            device_id_type=MESH,
        ).start()
    send(1)
    own = [pltpu.make_async_copy(slab(q, me), landing(q), sem.at[6 + q]) for q in range(2)]
    own.append(pltpu.make_async_copy(part, sums.at[pl.ds(me, 1)], sem.at[8]))
    for copy in own:
        copy.start()
    for copy in own:
        copy.wait()
    most = recv.at[pl.ds(0, (DEV - 1) * ROWS)]
    few = sums.at[pl.ds(0, DEV - 1)]
    for ref, s in ((most, 0), (most, 2), (few, 4), (most, 1), (few, 5), (most, 3)):
        pltpu.make_async_copy(ref, ref, sem.at[s]).wait()
    place(recv, sums, out)


def place(recv, sums, out):
    level = jnp.sum(sums[...]) / COUNT + 1e-6
    scale = 1.0 / jnp.full((8, 128), level, jnp.float32)
    lane = lax.broadcasted_iota(jnp.int32, (8, 128), 1) // TY
    line = lax.broadcasted_iota(jnp.int32, (8, 128), 0) // 2
    step = (line - lane) % 4

    def body(gx, _):
        x0 = pl.multiple_of(gx * TX, TX)
        for h in range(2):
            for r in range(ROWS):
                v = recv[pl.ds((gx * GY + 4 * h) * 2 * ROWS + r, 8, stride=ROWS), 0, :]
                w = v
                for k in range(1, 4):
                    turned = pltpu.roll(pltpu.roll(v, 2 * k, 0), 128 - TY * k, 1)
                    w = jnp.where(step == k, turned, w)
                out[r, pl.ds(x0, TX), h * 128 : (h + 1) * 128] = jnp.log(1.0 + w * scale)
        return 0

    lax.fori_loop(0, GX, body, 0, unroll=2)


def on_device(spectra, resample_index, resample_weight, disp_phase, surface_block):
    f32 = jnp.float32
    bf16 = jnp.bfloat16
    vm = pl.BlockSpec(memory_space=pltpu.VMEM)
    hbm = pl.BlockSpec(memory_space=pltpu.HBM)
    table = jnp.asarray(base_table(), bf16)
    return pl.pallas_call(
        main_kernel,
        out_shape=jax.ShapeDtypeStruct((ROWS, GX * TX, GY * TY), f32),
        in_specs=[hbm] * 6,
        out_specs=vm,
        scratch_shapes=[
            pltpu.VMEM((2, LINES, NK), bf16),
            pltpu.VMEM((3, RADIX, BLOCK), f32),
            pltpu.VMEM((RADIX, BLOCK), jnp.int32),
            pltpu.VMEM((TX, TY), jnp.int32),
            pltpu.VMEM((RADIX, BLOCK, 2 * BLOCK), bf16),
            pltpu.VMEM((RADIX // 2, NK, 2 * BLOCK), bf16),
            pltpu.VMEM((RADIX, LINES // 2, BLOCK), f32),
            pltpu.VMEM((RADIX, LINES // 2, 2 * BLOCK), bf16),
            pltpu.VMEM((2 * KEEP * BLOCK, 1, 128), f32),
            pltpu.VMEM((1, 1, 128), f32),
            pltpu.VMEM((DEV * ROWS * 2, 1, 128), f32),
            pltpu.VMEM((DEV, 1, 128), f32),
            pltpu.SemaphoreType.DMA((13,)),
            pltpu.SemaphoreType.DMA((9,)),
        ],
        compiler_params=pltpu.CompilerParams(
            collective_id=0, has_side_effects=True, vmem_limit_bytes=VMEM_BYTES
        ),
        name="main",
    )(
        spectra,
        resample_index.reshape(RADIX, BLOCK),
        resample_weight.reshape(RADIX, BLOCK),
        disp_phase.reshape(RADIX, BLOCK),
        surface_block,
        table,
    )

def solution(mesh):
    return jax.shard_map(
        on_device,
        mesh=mesh,
        in_specs=(P("gx", "gy", None), P(), P(), P(), P("gx", "gy")),
        out_specs=P(("gx", "gy"), None, None),
        check_vma=False,
    )
```

```python
import itertools
import math

import jax
import jax.numpy as jnp
import numpy as np
from jax import lax
from jax.experimental import pallas as pl
from jax.experimental.pallas import tpu as pltpu
from jax.sharding import PartitionSpec as P

NK = 2048
BLOCK = 128
KEEP = 5
RADIX = 16
GX = 16
GY = 8
DEV = GX * GY
TX = 8
TY = 32
LINES = TX * TY
ROWS = KEEP * BLOCK // DEV
COUNT = 128 * 256 * KEEP * BLOCK
MESH = pl.DeviceIdType.MESH
VMEM_BYTES = 67043328 - 660 * 1024


def base_table():
    c = np.arange(RADIX)[:, None, None]
    b = np.arange(NK // (2 * RADIX))[None, :, None]
    m = np.arange(BLOCK)[None, None, :]
    angle = 2.0 * math.pi * ((m * (RADIX * b + c)) % NK) / NK
    cos, sin = np.cos(angle), np.sin(angle)
    top = np.concatenate([cos, sin], axis=2)
    low = np.concatenate([-sin, cos], axis=2)
    return np.concatenate([top, low], axis=1).astype(np.float32)


def rot(z, k, n):
    re, im = z
    k = k % n
    if k == 0:
        return re, im
    if 4 * k == n:
        return im, -re
    if 2 * k == n:
        return -re, -im
    if 4 * k == 3 * n:
        return -im, re
    if 8 * k == n:
        h = math.sqrt(0.5)
        return h * (re + im), h * (im - re)
    if 8 * k == 3 * n:
        h = math.sqrt(0.5)
        return h * (im - re), -h * (re + im)
    c, s = math.cos(2 * math.pi * k / n), math.sin(2 * math.pi * k / n)
    return c * re + s * im, c * im - s * re


def add(a, b):
    return a[0] + b[0], a[1] + b[1]


def sub(a, b):
    return a[0] - b[0], a[1] - b[1]


def fft(z):
    n = len(z)
    if n == 1:
        return z
    even, odd = fft(z[0::2]), fft(z[1::2])
    odd = [rot(odd[k], k, n) for k in range(n // 2)]
    return [add(even[k], odd[k]) for k in range(n // 2)] + [
        sub(even[k], odd[k]) for k in range(n // 2)
    ]


def hops(o):
    return sum((0, 1, 2, 1)[v] for v in o[:3])


OFFSETS = sorted(
    [o for o in itertools.product(range(4), range(4), range(4), range(2)) if any(o)],
    key=lambda o: (-hops(o), o),
)


def main_kernel(
    spectra, index, weight, phase, surface, table, out, level,
    both, params, idx, surf, tab, hits, x, y, msg, part, recv, sums, load, sem, groups,
):
    f32, bf16 = jnp.float32, jnp.bfloat16
    half = LINES // 2
    gx, gy = lax.axis_index("gx"), lax.axis_index("gy")
    me = gx * GY + gy
    zs = [(gx // 4 + d) % 4 for d in range(4)]
    ys = [(gx % 4 + d) % 4 for d in range(4)]
    xs = [(gy // 2 + d) % 4 for d in range(4)]
    cs = [(gy % 2 + d) % 2 for d in range(2)]
    zy = [[z * 4 + v for v in ys] for z in zs]
    xc = [[v * 2 + c for c in cs] for v in xs]
    peers = [(zy[o[0]][o[1]], xc[o[2]][o[3]]) for o in OFFSETS]
    barrier = pltpu.get_barrier_semaphore()

    small = [
        pltpu.make_async_copy(index, idx, load.at[0]),
        pltpu.make_async_copy(weight, params.at[0], load.at[1]),
        pltpu.make_async_copy(phase, params.at[1], load.at[2]),
        pltpu.make_async_copy(surface, surf, load.at[3]),
    ]
    tiles = [
        pltpu.make_async_copy(
            spectra.at[2 * p + q], both.at[q, pl.ds(p * TY, TY)], load.at[4 + 4 * q + p]
        )
        for q in range(2)
        for p in range(4)
    ]
    big = pltpu.make_async_copy(table, tab, load.at[12])
    for copy in small + tiles + [big]:
        copy.start()
    for to in peers:
        pl.semaphore_signal(barrier, inc=1, device_id=to, device_id_type=MESH)
    for copy in small:
        copy.wait()
    cosp = jnp.cos(params[1])
    sinp = jnp.sin(params[1])
    params[1] = cosp
    params[2] = sinp
    tops = [
        jnp.concatenate([surf[2 * p + q : 2 * p + q + 1, :] for p in range(4)], axis=1)
        for q in range(2)
    ]
    row = lax.broadcasted_iota(jnp.int32, (BLOCK, 2 * BLOCK), 0).astype(jnp.int16)
    one = jnp.ones((BLOCK, 2 * BLOCK), bf16)
    zero = jnp.zeros((BLOCK, 2 * BLOCK), bf16)
    nt = (((1,), (1,)), ((), ()))

    def compute(q, acc):
        for copy in tiles[4 * q : 4 * q + 4]:
            copy.wait()
        lines = both[q, :half, :]
        both[q, half:, :] = jnp.concatenate([lines[:, 1:], lines[:, :1]], axis=1)
        for j in range(RADIX // 2):
            if q == 0:
                pick = jnp.concatenate(
                    [idx[2 * j : 2 * j + 1, :], idx[2 * j + 1 : 2 * j + 2, :]], axis=1
                )
                pick = pick.astype(jnp.int16)
                for k in range(NK // 128):
                    seen = row + jnp.int16(128 * k) == pick
                    hits[j, k * 128 : (k + 1) * 128, :] = jnp.where(seen, one, zero)
            pair = jnp.dot(both[q], hits[j], preferred_element_type=f32)
            for h in range(2):
                lane = slice(h * BLOCK, (h + 1) * BLOCK)
                w = params[0, 2 * j + h : 2 * j + h + 1, :]
                x[2 * j + h] = (1.0 - w) * pair[:half, lane] + w * pair[half:, lane]

        def spread(g, _):
            r0 = pl.multiple_of(g * 16, 16)
            parts = []
            for n in range(RADIX):
                v = x[n, pl.ds(r0, 16), :]
                parts.append(
                    [
                        (v * params[1 + o, n : n + 1, :]).astype(bf16).astype(f32)
                        for o in range(2)
                    ]
                )
            low = fft([(re[:8], im[:8]) for re, im in parts])
            high = fft([(re[8:], im[8:]) for re, im in parts])
            for c in range(RADIX):
                for o in range(2):
                    rows = jnp.concatenate([low[c][o], high[c][o]], axis=0)
                    y[c, pl.ds(r0, 16), o * BLOCK : (o + 1) * BLOCK] = rows.astype(bf16)
            return 0

        lax.fori_loop(0, half // 16, spread, 0)
        if q == 0:
            big.wait()
        for c in range(RADIX):
            depth = lax.dot_general(tab[c], y[c], nt, preferred_element_type=f32)
            power = depth[:64] * depth[:64] + depth[64:] * depth[64:]
            tile = [power[8 * b : 8 * b + 8] for b in range(8)]
            for k in range(KEEP):
                kept = tile[k]
                for s in range(1, 4):
                    kept = jnp.where(tops[q] == s, tile[k + s], kept)
                acc = acc + kept
                msg[pl.ds((q * KEEP + k) * BLOCK + c, 8, stride=RADIX), 0, :] = kept
        return acc

    def slab(q, dest):
        return msg.at[pl.ds(q * KEEP * BLOCK + ROWS * dest, ROWS)]

    def landing(q):
        return recv.at[pl.ds((2 * me + q) * ROWS, ROWS)]

    def send(q):
        arrived = sem.at[1] if q == 0 else groups.at[gx]
        for px, py in peers:
            pltpu.make_async_remote_copy(
                src_ref=slab(q, px * GY + py),
                dst_ref=landing(q),
                send_sem=sem.at[2 * q],
                recv_sem=arrived,
                device_id=(px, py),
                device_id_type=MESH,
            ).start()

    acc = compute(0, jnp.zeros((8, 128), f32))
    pl.semaphore_wait(barrier, DEV - 1)
    send(0)
    acc = compute(1, acc)
    part[...] = jnp.sum(acc, axis=0, keepdims=True).reshape(1, 1, 128)
    for px, py in peers:
        pltpu.make_async_remote_copy(
            src_ref=part,
            dst_ref=sums.at[pl.ds(me, 1)],
            send_sem=sem.at[4],
            recv_sem=sem.at[5],
            device_id=(px, py),
            device_id_type=MESH,
        ).start()
    send(1)
    own = [pltpu.make_async_copy(slab(q, me), landing(q), sem.at[6 + q]) for q in range(2)]
    own.append(pltpu.make_async_copy(part, sums.at[pl.ds(me, 1)], sem.at[8]))
    for copy in own:
        copy.start()
    for copy in own:
        copy.wait()
    most = recv.at[pl.ds(0, (DEV - 1) * ROWS)]
    few = sums.at[pl.ds(0, DEV - 1)]
    for ref, s in ((most, 0), (most, 2), (few, 4), (most, 1)):
        pltpu.make_async_copy(ref, ref, sem.at[s]).wait()
    lane = lax.broadcasted_iota(jnp.int32, (8, 128), 1) // TY
    line = lax.broadcasted_iota(jnp.int32, (8, 128), 0) // 2
    step = (line - lane) % 4
    for dz, dy in sorted(itertools.product(range(4), repeat=2), key=lambda o: -hops(o + (0,))):
        source = zs[-dz % 4] * 4 + ys[-dy % 4]
        come = GY if dz or dy else GY - 1
        block = recv.at[pl.ds(0, come * ROWS)]
        pltpu.make_async_copy(block, block, groups.at[source]).wait()
        x0 = pl.multiple_of(source * TX, TX)
        for h in range(2):
            for r in range(ROWS):
                v = recv[pl.ds((source * GY + 4 * h) * 2 * ROWS + r, 8, stride=ROWS), 0, :]
                w = v
                for k in range(1, 4):
                    turned = pltpu.roll(pltpu.roll(v, 2 * k, 0), 128 - TY * k, 1)
                    w = jnp.where(step == k, turned, w)
                out[r, pl.ds(x0, TX), h * 128 : (h + 1) * 128] = w
    pltpu.make_async_copy(few, few, sem.at[5]).wait()
    level[...] = jnp.full((8, 128), jnp.sum(sums[...]) / COUNT + 1e-6, f32)


def on_device(spectra, resample_index, resample_weight, disp_phase, surface_block):
    f32 = jnp.float32
    bf16 = jnp.bfloat16
    vm = pl.BlockSpec(memory_space=pltpu.VMEM)
    hbm = pl.BlockSpec(memory_space=pltpu.HBM)
    table = jnp.asarray(base_table(), bf16)
    flat, level = pl.pallas_call(
        main_kernel,
        out_shape=(
            jax.ShapeDtypeStruct((ROWS, GX * TX, GY * TY), f32),
            jax.ShapeDtypeStruct((8, 128), f32),
        ),
        in_specs=[hbm] * 6,
        out_specs=[vm] * 2,
        scratch_shapes=[
            pltpu.VMEM((2, LINES, NK), bf16),
            pltpu.VMEM((3, RADIX, BLOCK), f32),
            pltpu.VMEM((RADIX, BLOCK), jnp.int32),
            pltpu.VMEM((TX, TY), jnp.int32),
            pltpu.VMEM((RADIX, BLOCK, 2 * BLOCK), bf16),
            pltpu.VMEM((RADIX // 2, NK, 2 * BLOCK), bf16),
            pltpu.VMEM((RADIX, LINES // 2, BLOCK), f32),
            pltpu.VMEM((RADIX, LINES // 2, 2 * BLOCK), bf16),
            pltpu.VMEM((2 * KEEP * BLOCK, 1, 128), f32),
            pltpu.VMEM((1, 1, 128), f32),
            pltpu.VMEM((DEV * ROWS * 2, 1, 128), f32),
            pltpu.VMEM((DEV, 1, 128), f32),
            pltpu.SemaphoreType.DMA((13,)),
            pltpu.SemaphoreType.DMA((9,)),
            pltpu.SemaphoreType.DMA((GX,)),
        ],
        compiler_params=pltpu.CompilerParams(
            collective_id=0, has_side_effects=True, vmem_limit_bytes=VMEM_BYTES
        ),
        name="main",
    )(
        spectra,
        resample_index.reshape(RADIX, BLOCK),
        resample_weight.reshape(RADIX, BLOCK),
        disp_phase.reshape(RADIX, BLOCK),
        surface_block,
        table,
    )
    return jnp.log1p(flat / level[0, 0])

def solution(mesh):
    return jax.shard_map(
        on_device,
        mesh=mesh,
        in_specs=(P("gx", "gy", None), P(), P(), P(), P("gx", "gy")),
        out_specs=P(("gx", "gy"), None, None),
        check_vma=False,
    )
```

```python
import itertools
import math

import jax
import jax.numpy as jnp
import numpy as np
from jax import lax
from jax.experimental import pallas as pl
from jax.experimental.pallas import tpu as pltpu
from jax.sharding import PartitionSpec as P

NK = 2048
BLOCK = 128
KEEP = 5
RADIX = 16
GX = 16
GY = 8
DEV = GX * GY
TX = 8
TY = 32
LINES = TX * TY
ROWS = KEEP * BLOCK // DEV
COUNT = 128 * 256 * KEEP * BLOCK
MESH = pl.DeviceIdType.MESH
VMEM_BYTES = 67043328


def base_table():
    c = np.arange(RADIX)[:, None, None]
    b = np.arange(NK // (2 * RADIX))[None, :, None]
    m = np.arange(BLOCK)[None, None, :]
    angle = 2.0 * math.pi * ((m * (RADIX * b + c)) % NK) / NK
    cos, sin = np.cos(angle), np.sin(angle)
    top = np.concatenate([cos, sin], axis=2)
    low = np.concatenate([-sin, cos], axis=2)
    return np.concatenate([top, low], axis=1).astype(np.float32)


def rot(z, k, n):
    re, im = z
    k = k % n
    if k == 0:
        return re, im
    if 4 * k == n:
        return im, -re
    if 2 * k == n:
        return -re, -im
    if 4 * k == 3 * n:
        return -im, re
    if 8 * k == n:
        h = math.sqrt(0.5)
        return h * (re + im), h * (im - re)
    if 8 * k == 3 * n:
        h = math.sqrt(0.5)
        return h * (im - re), -h * (re + im)
    c, s = math.cos(2 * math.pi * k / n), math.sin(2 * math.pi * k / n)
    return c * re + s * im, c * im - s * re


def add(a, b):
    return a[0] + b[0], a[1] + b[1]


def sub(a, b):
    return a[0] - b[0], a[1] - b[1]


def fft4(z):
    a, b = add(z[0], z[2]), sub(z[0], z[2])
    c, d = add(z[1], z[3]), sub(z[1], z[3])
    d = rot(d, 1, 4)
    return [add(a, c), add(b, d), sub(a, c), sub(b, d)]


def hops(o):
    return sum((0, 1, 2, 1)[v] for v in o[:3])


OFFSETS = sorted(
    [o for o in itertools.product(range(4), range(4), range(4), range(2)) if any(o)],
    key=lambda o: (-hops(o), o),
)


def main_kernel(
    spectra, index, weight, phase, surface, table, out,
    both, params, idx, surf, tab, hits, x, mid, y, msg, part, recv, sums, placed, load, sem, groups,
):
    f32, bf16 = jnp.float32, jnp.bfloat16
    half = LINES // 2
    gx, gy = lax.axis_index("gx"), lax.axis_index("gy")
    me = gx * GY + gy
    zs = [(gx // 4 + d) % 4 for d in range(4)]
    ys = [(gx % 4 + d) % 4 for d in range(4)]
    xs = [(gy // 2 + d) % 4 for d in range(4)]
    cs = [(gy % 2 + d) % 2 for d in range(2)]
    zy = [[z * 4 + v for v in ys] for z in zs]
    xc = [[v * 2 + c for c in cs] for v in xs]
    peers = [(zy[o[0]][o[1]], xc[o[2]][o[3]]) for o in OFFSETS]
    barrier = pltpu.get_barrier_semaphore()

    small = [
        pltpu.make_async_copy(index, idx, load.at[0]),
        pltpu.make_async_copy(weight, params.at[0], load.at[1]),
        pltpu.make_async_copy(phase, params.at[1], load.at[2]),
        pltpu.make_async_copy(surface, surf, load.at[3]),
    ]
    tiles = [
        pltpu.make_async_copy(
            spectra.at[2 * p + q], both.at[q, pl.ds(p * TY, TY)], load.at[4 + 4 * q + p]
        )
        for q in range(2)
        for p in range(4)
    ]
    big = pltpu.make_async_copy(table, tab, load.at[12])
    for copy in small + tiles + [big]:
        copy.start()
    for to in peers:
        pl.semaphore_signal(barrier, inc=1, device_id=to, device_id_type=MESH)
    for copy in small:
        copy.wait()
    cosp = jnp.cos(params[1])
    sinp = jnp.sin(params[1])
    params[1] = cosp
    params[2] = sinp
    tops = [
        jnp.concatenate([surf[2 * p + q : 2 * p + q + 1, :] for p in range(4)], axis=1)
        for q in range(2)
    ]
    row = lax.broadcasted_iota(jnp.int32, (BLOCK, 2 * BLOCK), 0).astype(jnp.int16)
    one = jnp.ones((BLOCK, 2 * BLOCK), bf16)
    zero = jnp.zeros((BLOCK, 2 * BLOCK), bf16)
    nt = (((1,), (1,)), ((), ()))

    def compute(q, acc):
        for copy in tiles[4 * q : 4 * q + 4]:
            copy.wait()
        lines = both[q, :half, :]
        both[q, half:, :] = jnp.concatenate([lines[:, 1:], lines[:, :1]], axis=1)
        for n in range(4):
            for e in range(2):
                if q == 0:
                    pick = jnp.concatenate(
                        [idx[n + 8 * e + 4 * h : n + 8 * e + 4 * h + 1, :] for h in range(2)], axis=1
                    ).astype(jnp.int16)
                    for k in range(NK // 128):
                        seen = row + jnp.int16(128 * k) == pick
                        hits[2 * n + e, k * 128 : (k + 1) * 128, :] = jnp.where(seen, one, zero)
                pair = jnp.dot(both[q], hits[2 * n + e], preferred_element_type=f32)
                for h in range(2):
                    at = n + 8 * e + 4 * h
                    lane = slice(h * BLOCK, (h + 1) * BLOCK)
                    w = params[0, at : at + 1, :]
                    x[at] = (1.0 - w) * pair[:half, lane] + w * pair[half:, lane]
            for g in range(half // 16):
                rows = slice(16 * g, 16 * g + 16)
                z = []
                for m in range(4):
                    at = n + 4 * m
                    v = x[at, rows, :]
                    z.append(
                        [
                            (v * params[1 + o, at : at + 1, :]).astype(bf16).astype(f32)
                            for o in range(2)
                        ]
                    )
                for c, value in enumerate(fft4(z)):
                    for o, half_value in enumerate(rot(value, n * c, RADIX)):
                        mid[n, c, o, rows, :] = half_value
        if q == 0:
            big.wait()
        for low in range(4):
            for g in range(half // 16):
                rows = slice(16 * g, 16 * g + 16)
                z = [[mid[n, low, o, rows, :] for o in range(2)] for n in range(4)]
                for high, value in enumerate(fft4(z)):
                    for o in range(2):
                        y[low + 4 * high, rows, o * BLOCK : (o + 1) * BLOCK] = value[o].astype(bf16)
            for c in range(low, RADIX, 4):
                depth = lax.dot_general(tab[c], y[c], nt, preferred_element_type=f32)
                power = depth[:64] * depth[:64] + depth[64:] * depth[64:]
                tile = [power[8 * b : 8 * b + 8] for b in range(8)]
                for k in range(KEEP):
                    kept = tile[k]
                    for s in range(1, 4):
                        kept = jnp.where(tops[q] == s, tile[k + s], kept)
                    acc = acc + kept
                    msg[pl.ds((q * KEEP + k) * BLOCK + c, 8, stride=RADIX), 0, :] = kept
        return acc

    def slab(q, dest):
        return msg.at[pl.ds(q * KEEP * BLOCK + ROWS * dest, ROWS)]

    def landing(q):
        return recv.at[pl.ds((2 * me + q) * ROWS, ROWS)]

    def send(q):
        arrived = sem.at[1] if q == 0 else groups.at[gx]
        for px, py in peers:
            pltpu.make_async_remote_copy(
                src_ref=slab(q, px * GY + py),
                dst_ref=landing(q),
                send_sem=sem.at[2 * q],
                recv_sem=arrived,
                device_id=(px, py),
                device_id_type=MESH,
            ).start()

    acc = compute(0, jnp.zeros((8, 128), f32))
    pl.semaphore_wait(barrier, DEV - 1)
    send(0)
    acc = compute(1, acc)
    part[...] = jnp.sum(acc, axis=0, keepdims=True).reshape(1, 1, 128)
    for px, py in peers:
        pltpu.make_async_remote_copy(
            src_ref=part,
            dst_ref=sums.at[pl.ds(me, 1)],
            send_sem=sem.at[4],
            recv_sem=sem.at[5],
            device_id=(px, py),
            device_id_type=MESH,
        ).start()
    send(1)
    own = [pltpu.make_async_copy(slab(q, me), landing(q), sem.at[6 + q]) for q in range(2)]
    own.append(pltpu.make_async_copy(part, sums.at[pl.ds(me, 1)], sem.at[8]))
    for copy in own:
        copy.start()
    for copy in own:
        copy.wait()
    most = recv.at[pl.ds(0, (DEV - 1) * ROWS)]
    few = sums.at[pl.ds(0, DEV - 1)]
    for ref, s in ((most, 0), (most, 2), (few, 4), (few, 5), (most, 1)):
        pltpu.make_async_copy(ref, ref, sem.at[s]).wait()
    level = jnp.sum(sums[...]) / COUNT + 1e-6
    scale = 1.0 / jnp.full((8, 128), level, f32)
    lane = lax.broadcasted_iota(jnp.int32, (8, 128), 1) // TY
    line = lax.broadcasted_iota(jnp.int32, (8, 128), 0) // 2
    step = (line - lane) % 4
    for dz, dy in sorted(itertools.product(range(4), repeat=2), key=lambda o: -hops(o + (0,))):
        source = zs[-dz % 4] * 4 + ys[-dy % 4]
        come = GY if dz or dy else GY - 1
        block = recv.at[pl.ds(0, come * ROWS)]
        pltpu.make_async_copy(block, block, groups.at[source]).wait()
        x0 = pl.multiple_of(source * TX, TX)
        for h in range(2):
            for r in range(ROWS):
                v = recv[pl.ds((source * GY + 4 * h) * 2 * ROWS + r, 8, stride=ROWS), 0, :]
                w = v
                for k in range(1, 4):
                    turned = pltpu.roll(pltpu.roll(v, 2 * k, 0), 128 - TY * k, 1)
                    w = jnp.where(step == k, turned, w)
                placed[r, pl.ds(x0, TX), h * 128 : (h + 1) * 128] = jnp.log(1.0 + w * scale)
        gone = pltpu.make_async_copy(
            placed.at[:, pl.ds(x0, TX)], out.at[:, pl.ds(x0, TX)], sem.at[9]
        )
        gone.start()
    pltpu.make_async_copy(placed, out, sem.at[9]).wait()


def on_device(spectra, resample_index, resample_weight, disp_phase, surface_block):
    f32 = jnp.float32
    bf16 = jnp.bfloat16
    hbm = pl.BlockSpec(memory_space=pltpu.HBM)
    table = jnp.asarray(base_table(), bf16)
    return pl.pallas_call(
        main_kernel,
        out_shape=jax.ShapeDtypeStruct((ROWS, GX * TX, GY * TY), f32),
        in_specs=[hbm] * 6,
        out_specs=hbm,
        scratch_shapes=[
            pltpu.VMEM((2, LINES, NK), bf16),
            pltpu.VMEM((3, RADIX, BLOCK), f32),
            pltpu.VMEM((RADIX, BLOCK), jnp.int32),
            pltpu.VMEM((TX, TY), jnp.int32),
            pltpu.VMEM((RADIX, BLOCK, 2 * BLOCK), bf16),
            pltpu.VMEM((RADIX // 2, NK, 2 * BLOCK), bf16),
            pltpu.VMEM((RADIX, LINES // 2, BLOCK), f32),
            pltpu.VMEM((4, 4, 2, LINES // 2, BLOCK), f32),
            pltpu.VMEM((RADIX, LINES // 2, 2 * BLOCK), bf16),
            pltpu.VMEM((2 * KEEP * BLOCK, 1, 128), f32),
            pltpu.VMEM((1, 1, 128), f32),
            pltpu.VMEM((DEV * ROWS * 2, 1, 128), f32),
            pltpu.VMEM((DEV, 1, 128), f32),
            pltpu.VMEM((ROWS, GX * TX, GY * TY), f32),
            pltpu.SemaphoreType.DMA((13,)),
            pltpu.SemaphoreType.DMA((10,)),
            pltpu.SemaphoreType.DMA((GX,)),
        ],
        compiler_params=pltpu.CompilerParams(
            collective_id=0, has_side_effects=True, vmem_limit_bytes=VMEM_BYTES
        ),
        name="main",
    )(
        spectra,
        resample_index.reshape(RADIX, BLOCK),
        resample_weight.reshape(RADIX, BLOCK),
        disp_phase.reshape(RADIX, BLOCK),
        surface_block,
        table,
    )

def solution(mesh):
    return jax.shard_map(
        on_device,
        mesh=mesh,
        in_specs=(P("gx", "gy", None), P(), P(), P(), P("gx", "gy")),
        out_specs=P(("gx", "gy"), None, None),
        check_vma=False,
    )
```

```python
import itertools
import math

import jax
import jax.numpy as jnp
import numpy as np
from jax import lax
from jax.experimental import pallas as pl
from jax.experimental.pallas import tpu as pltpu
from jax.sharding import PartitionSpec as P

NK = 2048
BLOCK = 128
KEEP = 5
RADIX = 16
GX = 16
GY = 8
DEV = GX * GY
TX = 8
TY = 32
LINES = TX * TY
ROWS = KEEP * BLOCK // DEV
COUNT = 128 * 256 * KEEP * BLOCK
MESH = pl.DeviceIdType.MESH
VMEM_BYTES = 67043328


def base_table():
    c = np.arange(RADIX)[:, None, None]
    b = np.arange(NK // (2 * RADIX))[None, :, None]
    m = np.arange(BLOCK)[None, None, :]
    angle = 2.0 * math.pi * ((m * (RADIX * b + c)) % NK) / NK
    cos, sin = np.cos(angle), np.sin(angle)
    top = np.concatenate([cos, sin], axis=2)
    low = np.concatenate([-sin, cos], axis=2)
    return np.concatenate([top, low], axis=1).astype(np.float32)


def rot(z, k, n):
    re, im = z
    k = k % n
    if k == 0:
        return re, im
    if 4 * k == n:
        return im, -re
    if 2 * k == n:
        return -re, -im
    if 4 * k == 3 * n:
        return -im, re
    if 8 * k == n:
        h = math.sqrt(0.5)
        return h * (re + im), h * (im - re)
    if 8 * k == 3 * n:
        h = math.sqrt(0.5)
        return h * (im - re), -h * (re + im)
    c, s = math.cos(2 * math.pi * k / n), math.sin(2 * math.pi * k / n)
    return c * re + s * im, c * im - s * re


def add(a, b):
    return a[0] + b[0], a[1] + b[1]


def sub(a, b):
    return a[0] - b[0], a[1] - b[1]


def fft4(z):
    a, b = add(z[0], z[2]), sub(z[0], z[2])
    c, d = add(z[1], z[3]), sub(z[1], z[3])
    d = rot(d, 1, 4)
    return [add(a, c), add(b, d), sub(a, c), sub(b, d)]


def hops(o):
    return sum((0, 1, 2, 1)[v] for v in o[:3])


OFFSETS = sorted(
    [o for o in itertools.product(range(4), range(4), range(4), range(2)) if any(o)],
    key=lambda o: (-hops(o), o),
)


def main_kernel(
    spectra, index, weight, phase, surface, table, out,
    both, params, idx, surf, tab, hits, x, mid, y, msg, part, recv, sums, placed, load, sem, groups,
):
    f32, bf16 = jnp.float32, jnp.bfloat16
    half = LINES // 2
    gx, gy = lax.axis_index("gx"), lax.axis_index("gy")
    me = gx * GY + gy
    zs = [(gx // 4 + d) % 4 for d in range(4)]
    ys = [(gx % 4 + d) % 4 for d in range(4)]
    xs = [(gy // 2 + d) % 4 for d in range(4)]
    cs = [(gy % 2 + d) % 2 for d in range(2)]
    zy = [[z * 4 + v for v in ys] for z in zs]
    xc = [[v * 2 + c for c in cs] for v in xs]
    peers = [(zy[o[0]][o[1]], xc[o[2]][o[3]]) for o in OFFSETS]
    barrier = pltpu.get_barrier_semaphore()

    small = [
        pltpu.make_async_copy(index, idx, load.at[0]),
        pltpu.make_async_copy(weight, params.at[0], load.at[1]),
        pltpu.make_async_copy(phase, params.at[1], load.at[2]),
        pltpu.make_async_copy(surface, surf, load.at[3]),
    ]
    tiles = [
        pltpu.make_async_copy(
            spectra.at[2 * p + q], both.at[q, pl.ds(p * TY, TY)], load.at[4 + 4 * q + p]
        )
        for q in range(2)
        for p in range(4)
    ]
    big = pltpu.make_async_copy(table, tab, load.at[12])
    for copy in small + tiles + [big]:
        copy.start()
    for to in peers:
        pl.semaphore_signal(barrier, inc=1, device_id=to, device_id_type=MESH)
    for copy in small:
        copy.wait()
    cosp = jnp.cos(params[1])
    sinp = jnp.sin(params[1])
    params[1] = cosp
    params[2] = sinp
    tops = [
        jnp.concatenate([surf[2 * p + q : 2 * p + q + 1, :] for p in range(4)], axis=1)
        for q in range(2)
    ]
    row = lax.broadcasted_iota(jnp.int32, (BLOCK, 2 * BLOCK), 0).astype(jnp.int16)
    one = jnp.ones((BLOCK, 2 * BLOCK), bf16)
    zero = jnp.zeros((BLOCK, 2 * BLOCK), bf16)
    nt = (((1,), (1,)), ((), ()))

    def compute(q, acc):
        for copy in tiles[4 * q : 4 * q + 4]:
            copy.wait()
        lines = both[q, :half, :]
        both[q, half:, :] = jnp.concatenate([lines[:, 1:], lines[:, :1]], axis=1)
        for n in range(4):
            for e in range(2):
                if q == 0:
                    pick = jnp.concatenate(
                        [idx[n + 8 * e + 4 * h : n + 8 * e + 4 * h + 1, :] for h in range(2)], axis=1
                    ).astype(jnp.int16)
                    for k in range(NK // 128):
                        seen = row + jnp.int16(128 * k) == pick
                        hits[2 * n + e, k * 128 : (k + 1) * 128, :] = jnp.where(seen, one, zero)
                pair = jnp.dot(both[q], hits[2 * n + e], preferred_element_type=f32)
                for h in range(2):
                    at = n + 8 * e + 4 * h
                    lane = slice(h * BLOCK, (h + 1) * BLOCK)
                    w = params[0, at : at + 1, :]
                    x[at] = (1.0 - w) * pair[:half, lane] + w * pair[half:, lane]
            for g in range(half // 16):
                rows = slice(16 * g, 16 * g + 16)
                z = []
                for m in range(4):
                    at = n + 4 * m
                    v = x[at, rows, :]
                    z.append(
                        [
                            (v * params[1 + o, at : at + 1, :]).astype(bf16).astype(f32)
                            for o in range(2)
                        ]
                    )
                for c, value in enumerate(fft4(z)):
                    for o, half_value in enumerate(rot(value, n * c, RADIX)):
                        mid[n, c, o, rows, :] = half_value
        if q == 0:
            big.wait()
        for low in range(4):
            for g in range(half // 16):
                rows = slice(16 * g, 16 * g + 16)
                z = [[mid[n, low, o, rows, :] for o in range(2)] for n in range(4)]
                for high, value in enumerate(fft4(z)):
                    for o in range(2):
                        y[low + 4 * high, rows, o * BLOCK : (o + 1) * BLOCK] = value[o].astype(bf16)
            for c in range(low, RADIX, 4):
                depth = lax.dot_general(tab[c], y[c], nt, preferred_element_type=f32)
                power = depth[:64] * depth[:64] + depth[64:] * depth[64:]
                tile = [power[8 * b : 8 * b + 8] for b in range(8)]
                for k in range(KEEP):
                    kept = tile[k]
                    for s in range(1, 4):
                        kept = jnp.where(tops[q] == s, tile[k + s], kept)
                    acc = acc + kept
                    msg[pl.ds((q * KEEP + k) * BLOCK + c, 8, stride=RADIX), :] = kept
        return acc

    def slab(q, dest):
        return msg.at[pl.ds(q * KEEP * BLOCK + ROWS * dest, ROWS)]

    def landing(q):
        return recv.at[pl.ds((2 * me + q) * ROWS, ROWS)]

    def send(q):
        arrived = sem.at[1] if q == 0 else groups.at[gx]
        for px, py in peers:
            pltpu.make_async_remote_copy(
                src_ref=slab(q, px * GY + py),
                dst_ref=landing(q),
                send_sem=sem.at[2 * q],
                recv_sem=arrived,
                device_id=(px, py),
                device_id_type=MESH,
            ).start()

    acc = compute(0, jnp.zeros((8, 128), f32))
    pl.semaphore_wait(barrier, DEV - 1)
    send(0)
    acc = compute(1, acc)
    part[...] = jnp.sum(acc, axis=0, keepdims=True).reshape(1, 1, 128)
    for px, py in peers:
        pltpu.make_async_remote_copy(
            src_ref=part,
            dst_ref=sums.at[pl.ds(me, 1)],
            send_sem=sem.at[4],
            recv_sem=sem.at[5],
            device_id=(px, py),
            device_id_type=MESH,
        ).start()
    send(1)
    own = [pltpu.make_async_copy(slab(q, me), landing(q), sem.at[6 + q]) for q in range(2)]
    own.append(pltpu.make_async_copy(part, sums.at[pl.ds(me, 1)], sem.at[8]))
    for copy in own:
        copy.start()
    for copy in own:
        copy.wait()
    most = recv.at[pl.ds(0, (DEV - 1) * ROWS)]
    few = sums.at[pl.ds(0, DEV - 1)]
    for ref, s in ((most, 0), (most, 2), (few, 4), (few, 5), (most, 1)):
        pltpu.make_async_copy(ref, ref, sem.at[s]).wait()
    level = jnp.sum(sums[...]) / COUNT + 1e-6
    scale = 1.0 / jnp.full((8, 128), level, f32)
    lane = lax.broadcasted_iota(jnp.int32, (8, 128), 1) // TY
    line = lax.broadcasted_iota(jnp.int32, (8, 128), 0) // 2
    step = (line - lane) % 4
    around = sorted(itertools.product(range(4), repeat=2), key=lambda o: -hops(o + (0,)))
    for batch in (around[:5], around[5:11], around[11:]):
        sources = [zs[-dz % 4] * 4 + ys[-dy % 4] for dz, dy in batch]
        for (dz, dy), source in zip(batch, sources):
            block = recv.at[pl.ds(0, (GY if dz or dy else GY - 1) * ROWS)]
            pltpu.make_async_copy(block, block, groups.at[source]).wait()
        for source in sources:
            x0 = pl.multiple_of(source * TX, TX)
            for h in range(2):
                for r in range(ROWS):
                    v = recv[pl.ds((source * GY + 4 * h) * 2 * ROWS + r, 8, stride=ROWS), :]
                    w = v
                    for k in range(1, 4):
                        turned = pltpu.roll(pltpu.roll(v, 2 * k, 0), 128 - TY * k, 1)
                        w = jnp.where(step == k, turned, w)
                    placed[r, pl.ds(x0, TX), h * 128 : (h + 1) * 128] = jnp.log(1.0 + w * scale)
            pltpu.make_async_copy(
                placed.at[:, pl.ds(x0, TX)], out.at[:, pl.ds(x0, TX)], sem.at[9]
            ).start()
    pltpu.make_async_copy(placed, out, sem.at[9]).wait()


def on_device(spectra, resample_index, resample_weight, disp_phase, surface_block):
    f32 = jnp.float32
    bf16 = jnp.bfloat16
    hbm = pl.BlockSpec(memory_space=pltpu.HBM)
    table = jnp.asarray(base_table(), bf16)
    return pl.pallas_call(
        main_kernel,
        out_shape=jax.ShapeDtypeStruct((ROWS, GX * TX, GY * TY), f32),
        in_specs=[hbm] * 6,
        out_specs=hbm,
        scratch_shapes=[
            pltpu.VMEM((2, LINES, NK), bf16),
            pltpu.VMEM((3, RADIX, BLOCK), f32),
            pltpu.VMEM((RADIX, BLOCK), jnp.int32),
            pltpu.VMEM((TX, TY), jnp.int32),
            pltpu.VMEM((RADIX, BLOCK, 2 * BLOCK), bf16),
            pltpu.VMEM((RADIX // 2, NK, 2 * BLOCK), bf16),
            pltpu.VMEM((RADIX, LINES // 2, BLOCK), f32),
            pltpu.VMEM((4, 4, 2, LINES // 2, BLOCK), f32),
            pltpu.VMEM((RADIX, LINES // 2, 2 * BLOCK), bf16),
            pltpu.VMEM((2 * KEEP * BLOCK, 128), f32),
            pltpu.VMEM((1, 1, 128), f32),
            pltpu.VMEM((DEV * ROWS * 2, 128), f32),
            pltpu.VMEM((DEV, 1, 128), f32),
            pltpu.VMEM((ROWS, GX * TX, GY * TY), f32),
            pltpu.SemaphoreType.DMA((13,)),
            pltpu.SemaphoreType.DMA((10,)),
            pltpu.SemaphoreType.DMA((GX,)),
        ],
        compiler_params=pltpu.CompilerParams(
            collective_id=0, has_side_effects=True, vmem_limit_bytes=VMEM_BYTES
        ),
        name="main",
    )(
        spectra,
        resample_index.reshape(RADIX, BLOCK),
        resample_weight.reshape(RADIX, BLOCK),
        disp_phase.reshape(RADIX, BLOCK),
        surface_block,
        table,
    )

def solution(mesh):
    return jax.shard_map(
        on_device,
        mesh=mesh,
        in_specs=(P("gx", "gy", None), P(), P(), P(), P("gx", "gy")),
        out_specs=P(("gx", "gy"), None, None),
        check_vma=False,
    )
```

```python
import itertools
import math

import jax
import jax.numpy as jnp
import numpy as np
from jax import lax
from jax.experimental import pallas as pl
from jax.experimental.pallas import tpu as pltpu
from jax.sharding import PartitionSpec as P

NK = 2048
BLOCK = 128
KEEP = 5
RADIX = 16
GX = 16
GY = 8
DEV = GX * GY
TX = 8
TY = 32
LINES = TX * TY
ROWS = KEEP * BLOCK // DEV
COUNT = 128 * 256 * KEEP * BLOCK
MESH = pl.DeviceIdType.MESH
VMEM_BYTES = 67043328
FAR = 64


def base_table():
    c = np.arange(RADIX)[:, None, None]
    b = np.arange(NK // (2 * RADIX))[None, :, None]
    m = np.arange(BLOCK)[None, None, :]
    angle = 2.0 * math.pi * ((m * (RADIX * b + c)) % NK) / NK
    cos, sin = np.cos(angle), np.sin(angle)
    top = np.concatenate([cos, sin], axis=2)
    low = np.concatenate([-sin, cos], axis=2)
    return np.concatenate([top, low], axis=1).astype(np.float32)


def rot(z, k, n):
    re, im = z
    k = k % n
    if k == 0:
        return re, im
    if 4 * k == n:
        return im, -re
    if 2 * k == n:
        return -re, -im
    if 4 * k == 3 * n:
        return -im, re
    if 8 * k == n:
        h = math.sqrt(0.5)
        return h * (re + im), h * (im - re)
    if 8 * k == 3 * n:
        h = math.sqrt(0.5)
        return h * (im - re), -h * (re + im)
    c, s = math.cos(2 * math.pi * k / n), math.sin(2 * math.pi * k / n)
    return c * re + s * im, c * im - s * re


def add(a, b):
    return a[0] + b[0], a[1] + b[1]


def sub(a, b):
    return a[0] - b[0], a[1] - b[1]


def fft4(z):
    a, b = add(z[0], z[2]), sub(z[0], z[2])
    c, d = add(z[1], z[3]), sub(z[1], z[3])
    d = rot(d, 1, 4)
    return [add(a, c), add(b, d), sub(a, c), sub(b, d)]


def hops(o):
    return sum((0, 1, 2, 1)[v] for v in o[:3])


OFFSETS = sorted(
    [o for o in itertools.product(range(4), range(4), range(4), range(2)) if any(o)],
    key=lambda o: (-hops(o), o),
)


def main_kernel(
    spectra, index, weight, phase, surface, table, out,
    both, params, idx, surf, tab, hits, x, mid, y, msg, part, row_part, recv, row_sums, sums, placed, load, sem, groups,
):
    f32, bf16 = jnp.float32, jnp.bfloat16
    half = LINES // 2
    gx, gy = lax.axis_index("gx"), lax.axis_index("gy")
    me = gx * GY + gy
    zs = [(gx // 4 + d) % 4 for d in range(4)]
    ys = [(gx % 4 + d) % 4 for d in range(4)]
    xs = [(gy // 2 + d) % 4 for d in range(4)]
    cs = [(gy % 2 + d) % 2 for d in range(2)]
    zy = [[z * 4 + v for v in ys] for z in zs]
    xc = [[v * 2 + c for c in cs] for v in xs]
    peers = [(zy[o[0]][o[1]], xc[o[2]][o[3]]) for o in OFFSETS]
    barrier = pltpu.get_barrier_semaphore()

    small = [
        pltpu.make_async_copy(index, idx, load.at[0]),
        pltpu.make_async_copy(weight, params.at[0], load.at[1]),
        pltpu.make_async_copy(phase, params.at[1], load.at[2]),
        pltpu.make_async_copy(surface, surf, load.at[3]),
    ]
    tiles = [
        pltpu.make_async_copy(
            spectra.at[2 * p + q], both.at[q, pl.ds(p * TY, TY)], load.at[4 + 4 * q + p]
        )
        for q in range(2)
        for p in range(4)
    ]
    big = pltpu.make_async_copy(table, tab, load.at[12])
    for copy in small + tiles + [big]:
        copy.start()
    for to in peers:
        pl.semaphore_signal(barrier, inc=1, device_id=to, device_id_type=MESH)
    for copy in small:
        copy.wait()
    cosp = jnp.cos(params[1])
    sinp = jnp.sin(params[1])
    params[1] = cosp
    params[2] = sinp
    tops = [
        jnp.concatenate([surf[2 * p + q : 2 * p + q + 1, :] for p in range(4)], axis=1)
        for q in range(2)
    ]
    row = lax.broadcasted_iota(jnp.int32, (BLOCK, 2 * BLOCK), 0).astype(jnp.int16)
    one = jnp.ones((BLOCK, 2 * BLOCK), bf16)
    zero = jnp.zeros((BLOCK, 2 * BLOCK), bf16)
    nt = (((1,), (1,)), ((), ()))

    def compute(q, acc):
        lines = both[q, :half, :]
        both[q, half:, :] = jnp.concatenate([lines[:, 1:], lines[:, :1]], axis=1)
        for n in range(4):
            for e in range(2):
                if q == 0:
                    pick = jnp.concatenate(
                        [idx[n + 8 * e + 4 * h : n + 8 * e + 4 * h + 1, :] for h in range(2)], axis=1
                    ).astype(jnp.int16)
                    for k in range(NK // 128):
                        seen = row + jnp.int16(128 * k) == pick
                        hits[2 * n + e, k * 128 : (k + 1) * 128, :] = jnp.where(seen, one, zero)
                pair = jnp.dot(both[q], hits[2 * n + e], preferred_element_type=f32)
                for h in range(2):
                    at = n + 8 * e + 4 * h
                    lane = slice(h * BLOCK, (h + 1) * BLOCK)
                    w = params[0, at : at + 1, :]
                    x[at] = (1.0 - w) * pair[:half, lane] + w * pair[half:, lane]
            for g in range(half // 16):
                rows = slice(16 * g, 16 * g + 16)
                z = []
                for m in range(4):
                    at = n + 4 * m
                    v = x[at, rows, :]
                    z.append(
                        [
                            (v * params[1 + o, at : at + 1, :]).astype(bf16).astype(f32)
                            for o in range(2)
                        ]
                    )
                for c, value in enumerate(fft4(z)):
                    for o, half_value in enumerate(rot(value, n * c, RADIX)):
                        mid[n, c, o, rows, :] = half_value
        if q == 0:
            big.wait()
        for low in range(4):
            for g in range(half // 16):
                rows = slice(16 * g, 16 * g + 16)
                z = [[mid[n, low, o, rows, :] for o in range(2)] for n in range(4)]
                for high, value in enumerate(fft4(z)):
                    for o in range(2):
                        y[low + 4 * high, rows, o * BLOCK : (o + 1) * BLOCK] = value[o].astype(bf16)
            for c in range(low, RADIX, 4):
                depth = lax.dot_general(tab[c], y[c], nt, preferred_element_type=f32)
                power = depth[:64] * depth[:64] + depth[64:] * depth[64:]
                tile = [power[8 * b : 8 * b + 8] for b in range(8)]
                for k in range(KEEP):
                    kept = tile[k]
                    for s in range(1, 4):
                        kept = jnp.where(tops[q] == s, tile[k + s], kept)
                    acc = acc + kept
                    msg[pl.ds((q * KEEP + k) * BLOCK + c, 8, stride=RADIX), :] = kept
        return acc

    def slab(q, dest):
        return msg.at[pl.ds(q * KEEP * BLOCK + ROWS * dest, ROWS)]

    def landing(q):
        return recv.at[pl.ds((2 * me + q) * ROWS, ROWS)]

    def send(q, among):
        arrived = sem.at[1] if q == 0 else groups.at[gx]
        for px, py in among:
            pltpu.make_async_remote_copy(
                src_ref=slab(q, px * GY + py),
                dst_ref=landing(q),
                send_sem=sem.at[2 * q],
                recv_sem=arrived,
                device_id=(px, py),
                device_id_type=MESH,
            ).start()

    def share(source, target, s, among):
        for to in among:
            pltpu.make_async_remote_copy(
                src_ref=source,
                dst_ref=target,
                send_sem=sem.at[s],
                recv_sem=sem.at[s + 1],
                device_id=to,
                device_id_type=MESH,
            ).start()

    for copy in tiles[:4]:
        copy.wait()
    acc = compute(0, jnp.zeros((8, 128), f32))
    for copy in tiles[4:]:
        copy.wait()
    pl.semaphore_wait(barrier, DEV - 1)
    send(0, peers)
    acc = compute(1, acc)
    part[...] = jnp.sum(acc, axis=0, keepdims=True).reshape(1, 1, 128)
    row_peers = [to for o, to in zip(OFFSETS, peers) if not any(o[:2])]
    column_peers = [to for o, to in zip(OFFSETS, peers) if not any(o[2:])]
    send(1, peers[:8])
    share(part, row_sums.at[pl.ds(gy, 1)], 4, row_peers)
    own = [
        pltpu.make_async_copy(part, row_sums.at[pl.ds(gy, 1)], sem.at[8]),
        pltpu.make_async_copy(slab(0, me), landing(0), sem.at[6]),
        pltpu.make_async_copy(slab(1, me), landing(1), sem.at[7]),
    ]
    for copy in own:
        copy.start()
    send(1, peers[8:FAR])
    own[0].wait()
    few = row_sums.at[pl.ds(0, GY - 1)]
    pltpu.make_async_copy(few, few, sem.at[5]).wait()
    row_part[...] = jnp.sum(row_sums[...], axis=0, keepdims=True)
    send(1, peers[FAR : FAR + 8])
    share(row_part, sums.at[pl.ds(gx, 1)], 10, column_peers)
    own.append(pltpu.make_async_copy(row_part, sums.at[pl.ds(gx, 1)], sem.at[12]))
    own[-1].start()
    send(1, peers[FAR + 8 :])
    for copy in own[1:]:
        copy.wait()
    most = recv.at[pl.ds(0, (DEV - 1) * ROWS)]
    line = sums.at[pl.ds(0, GX - 1)]
    for ref, s in ((most, 0), (most, 2), (few, 4), (line, 10), (line, 11), (most, 1)):
        pltpu.make_async_copy(ref, ref, sem.at[s]).wait()
    level = jnp.sum(sums[...]) / COUNT + 1e-6
    scale = 1.0 / jnp.full((8, 128), level, f32)
    lane = lax.broadcasted_iota(jnp.int32, (8, 128), 1) // TY
    pair = lax.broadcasted_iota(jnp.int32, (8, 128), 0) // 2
    step = (pair - lane) % 4
    around = sorted(itertools.product(range(4), repeat=2), key=lambda o: -hops(o + (0,)))
    for batch in (around[:5], around[5:11], around[11:]):
        sources = [zs[-dz % 4] * 4 + ys[-dy % 4] for dz, dy in batch]
        for (dz, dy), source in zip(batch, sources):
            block = recv.at[pl.ds(0, (GY if dz or dy else GY - 1) * ROWS)]
            pltpu.make_async_copy(block, block, groups.at[source]).wait()
        for source in sources:
            x0 = pl.multiple_of(source * TX, TX)
            for h in range(2):
                for r in range(ROWS):
                    v = recv[pl.ds((source * GY + 4 * h) * 2 * ROWS + r, 8, stride=ROWS), :]
                    w = v
                    for k in range(1, 4):
                        turned = pltpu.roll(pltpu.roll(v, 2 * k, 0), 128 - TY * k, 1)
                        w = jnp.where(step == k, turned, w)
                    placed[r, pl.ds(x0, TX), h * 128 : (h + 1) * 128] = jnp.log(1.0 + w * scale)
            pltpu.make_async_copy(
                placed.at[:, pl.ds(x0, TX)], out.at[:, pl.ds(x0, TX)], sem.at[9]
            ).start()
    pltpu.make_async_copy(placed, out, sem.at[9]).wait()


def on_device(spectra, resample_index, resample_weight, disp_phase, surface_block):
    f32 = jnp.float32
    bf16 = jnp.bfloat16
    hbm = pl.BlockSpec(memory_space=pltpu.HBM)
    table = jnp.asarray(base_table(), bf16)
    return pl.pallas_call(
        main_kernel,
        out_shape=jax.ShapeDtypeStruct((ROWS, GX * TX, GY * TY), f32),
        in_specs=[hbm] * 6,
        out_specs=hbm,
        scratch_shapes=[
            pltpu.VMEM((2, LINES, NK), bf16),
            pltpu.VMEM((3, RADIX, BLOCK), f32),
            pltpu.VMEM((RADIX, BLOCK), jnp.int32),
            pltpu.VMEM((TX, TY), jnp.int32),
            pltpu.VMEM((RADIX, BLOCK, 2 * BLOCK), bf16),
            pltpu.VMEM((RADIX // 2, NK, 2 * BLOCK), bf16),
            pltpu.VMEM((RADIX, LINES // 2, BLOCK), f32),
            pltpu.VMEM((4, 4, 2, LINES // 2, BLOCK), f32),
            pltpu.VMEM((RADIX, LINES // 2, 2 * BLOCK), bf16),
            pltpu.VMEM((2 * KEEP * BLOCK, 128), f32),
            pltpu.VMEM((1, 1, 128), f32),
            pltpu.VMEM((1, 1, 128), f32),
            pltpu.VMEM((DEV * ROWS * 2, 128), f32),
            pltpu.VMEM((GY, 1, 128), f32),
            pltpu.VMEM((GX, 1, 128), f32),
            pltpu.VMEM((ROWS, GX * TX, GY * TY), f32),
            pltpu.SemaphoreType.DMA((13,)),
            pltpu.SemaphoreType.DMA((13,)),
            pltpu.SemaphoreType.DMA((GX,)),
        ],
        compiler_params=pltpu.CompilerParams(
            collective_id=0, has_side_effects=True, vmem_limit_bytes=VMEM_BYTES
        ),
        name="main",
    )(
        spectra,
        resample_index.reshape(RADIX, BLOCK),
        resample_weight.reshape(RADIX, BLOCK),
        disp_phase.reshape(RADIX, BLOCK),
        surface_block,
        table,
    )

def solution(mesh):
    return jax.shard_map(
        on_device,
        mesh=mesh,
        in_specs=(P("gx", "gy", None), P(), P(), P(), P("gx", "gy")),
        out_specs=P(("gx", "gy"), None, None),
        check_vma=False,
    )
```

```python
import itertools
import math

import jax
import jax.numpy as jnp
import numpy as np
from jax import lax
from jax.experimental import pallas as pl
from jax.experimental.pallas import tpu as pltpu
from jax.sharding import PartitionSpec as P

NK = 2048
BLOCK = 128
KEEP = 5
RADIX = 16
GX = 16
GY = 8
DEV = GX * GY
TX = 8
TY = 32
LINES = TX * TY
ROWS = KEEP * BLOCK // DEV
COUNT = 128 * 256 * KEEP * BLOCK
FLAT = pl.DeviceIdType.LOGICAL
VMEM_BYTES = 67043328


def base_table():
    c = np.arange(RADIX)[:, None, None]
    b = np.arange(NK // (2 * RADIX))[None, :, None]
    m = np.arange(BLOCK)[None, None, :]
    angle = 2.0 * math.pi * ((m * (RADIX * b + c)) % NK) / NK
    cos, sin = np.cos(angle), np.sin(angle)
    top = np.concatenate([cos, sin], axis=2)
    low = np.concatenate([-sin, cos], axis=2)
    return np.concatenate([top, low], axis=1).astype(np.float32)


def rot(z, k, n):
    re, im = z
    k = k % n
    if k == 0:
        return re, im
    if 4 * k == n:
        return im, -re
    if 2 * k == n:
        return -re, -im
    if 4 * k == 3 * n:
        return -im, re
    if 8 * k == n:
        h = math.sqrt(0.5)
        return h * (re + im), h * (im - re)
    if 8 * k == 3 * n:
        h = math.sqrt(0.5)
        return h * (im - re), -h * (re + im)
    c, s = math.cos(2 * math.pi * k / n), math.sin(2 * math.pi * k / n)
    return c * re + s * im, c * im - s * re


def add(a, b):
    return a[0] + b[0], a[1] + b[1]


def sub(a, b):
    return a[0] - b[0], a[1] - b[1]


def fft4(z):
    a, b = add(z[0], z[2]), sub(z[0], z[2])
    c, d = add(z[1], z[3]), sub(z[1], z[3])
    d = rot(d, 1, 4)
    return [add(a, c), add(b, d), sub(a, c), sub(b, d)]


def hops(o):
    return sum((0, 1, 2, 1)[v] for v in o[:3])


OFFSETS = sorted(
    [o for o in itertools.product(range(4), range(4), range(4), range(2)) if any(o)],
    key=lambda o: (-hops(o), o),
)


def main_kernel(
    spectra, index, weight, phase, surface, table, out,
    both, params, idx, surf, tab, hits, x, mid, y, msg, part, halves, recv, sums, placed, load, sem, groups,
):
    f32, bf16 = jnp.float32, jnp.bfloat16
    half = LINES // 2
    gx, gy = lax.axis_index("gx"), lax.axis_index("gy")
    me = gx * GY + gy
    zs = [(gx // 4 + d) % 4 for d in range(4)]
    ys = [(gx % 4 + d) % 4 for d in range(4)]
    xs = [(gy // 2 + d) % 4 for d in range(4)]
    cs = [(gy % 2 + d) % 2 for d in range(2)]
    zy = [[(z * 4 + v) * GY for v in ys] for z in zs]
    xc = [[v * 2 + c for c in cs] for v in xs]
    peers = [zy[o[0]][o[1]] + xc[o[2]][o[3]] for o in OFFSETS]
    alike = [to for o, to in zip(OFFSETS, peers) if o[3] == 0]
    partner = zy[0][0] + xc[0][1]
    chip = gx * (GY // 2) + gy // 2
    barrier = pltpu.get_barrier_semaphore()

    small = [
        pltpu.make_async_copy(index, idx, load.at[0]),
        pltpu.make_async_copy(weight, params.at[0], load.at[1]),
        pltpu.make_async_copy(phase, params.at[1], load.at[2]),
        pltpu.make_async_copy(surface, surf, load.at[3]),
    ]
    tiles = [
        pltpu.make_async_copy(
            spectra.at[2 * p + q], both.at[q, pl.ds(p * TY, TY)], load.at[4 + 4 * q + p]
        )
        for q in range(2)
        for p in range(4)
    ]
    big = pltpu.make_async_copy(table, tab, load.at[12])
    for copy in small + tiles + [big]:
        copy.start()
    for to in peers:
        pl.semaphore_signal(barrier, inc=1, device_id=to, device_id_type=FLAT)
    for copy in small:
        copy.wait()
    cosp = jnp.cos(params[1])
    sinp = jnp.sin(params[1])
    params[1] = cosp
    params[2] = sinp
    tops = [
        jnp.concatenate([surf[2 * p + q : 2 * p + q + 1, :] for p in range(4)], axis=1)
        for q in range(2)
    ]
    row = lax.broadcasted_iota(jnp.int32, (BLOCK, 2 * BLOCK), 0).astype(jnp.int16)
    one = jnp.ones((BLOCK, 2 * BLOCK), bf16)
    zero = jnp.zeros((BLOCK, 2 * BLOCK), bf16)
    nt = (((1,), (1,)), ((), ()))

    def shift(q):
        for copy in tiles[4 * q : 4 * q + 4]:
            copy.wait()
        lines = both[q, :half, :]
        both[q, half:, :] = jnp.concatenate([lines[:, 1:], lines[:, :1]], axis=1)

    def compute(q, acc):
        for n in range(4):
            for e in range(2):
                if q == 0:
                    pick = jnp.concatenate(
                        [idx[n + 8 * e + 4 * h : n + 8 * e + 4 * h + 1, :] for h in range(2)], axis=1
                    ).astype(jnp.int16)
                    for k in range(NK // 128):
                        seen = row + jnp.int16(128 * k) == pick
                        hits[2 * n + e, k * 128 : (k + 1) * 128, :] = jnp.where(seen, one, zero)
                pair = jnp.dot(both[q], hits[2 * n + e], preferred_element_type=f32)
                for h in range(2):
                    at = n + 8 * e + 4 * h
                    lane = slice(h * BLOCK, (h + 1) * BLOCK)
                    w = params[0, at : at + 1, :]
                    x[at] = (1.0 - w) * pair[:half, lane] + w * pair[half:, lane]
            for g in range(half // 16):
                rows = slice(16 * g, 16 * g + 16)
                z = []
                for m in range(4):
                    at = n + 4 * m
                    v = x[at, rows, :]
                    z.append(
                        [
                            (v * params[1 + o, at : at + 1, :]).astype(bf16).astype(f32)
                            for o in range(2)
                        ]
                    )
                for c, value in enumerate(fft4(z)):
                    for o, half_value in enumerate(rot(value, n * c, RADIX)):
                        mid[n, c, o, rows, :] = half_value
        if q == 0:
            big.wait()
        for low in range(4):
            for g in range(half // 16):
                rows = slice(16 * g, 16 * g + 16)
                z = [[mid[n, low, o, rows, :] for o in range(2)] for n in range(4)]
                for high, value in enumerate(fft4(z)):
                    for o in range(2):
                        y[low + 4 * high, rows, o * BLOCK : (o + 1) * BLOCK] = value[o].astype(bf16)
            for c in range(low, RADIX, 4):
                depth = lax.dot_general(tab[c], y[c], nt, preferred_element_type=f32)
                power = depth[:64] * depth[:64] + depth[64:] * depth[64:]
                tile = [power[8 * b : 8 * b + 8] for b in range(8)]
                for k in range(KEEP):
                    kept = tile[k]
                    for s in range(1, 4):
                        kept = jnp.where(tops[q] == s, tile[k + s], kept)
                    acc = acc + kept
                    msg[pl.ds((q * KEEP + k) * BLOCK + c, 8, stride=RADIX), :] = kept
        return acc

    def slab(q, dest):
        return msg.at[pl.ds(q * KEEP * BLOCK + ROWS * dest, ROWS)]

    def landing(q):
        return recv.at[pl.ds((2 * me + q) * ROWS, ROWS)]

    def send(q, among):
        arrived = sem.at[1] if q == 0 else groups.at[gx]
        for to in among:
            pltpu.make_async_remote_copy(
                src_ref=slab(q, to),
                dst_ref=landing(q),
                send_sem=sem.at[2 * q],
                recv_sem=arrived,
                device_id=to,
                device_id_type=FLAT,
            ).start()

    shift(0)
    acc = compute(0, jnp.zeros((8, 128), f32))
    shift(1)
    pl.semaphore_wait(barrier, DEV - 1)
    send(0, peers)
    acc = compute(1, acc)
    part[...] = jnp.sum(acc, axis=0, keepdims=True).reshape(1, 1, 128)
    send(1, peers[:8])
    for to in alike:
        pltpu.make_async_remote_copy(
            src_ref=part,
            dst_ref=sums.at[pl.ds(chip, 1)],
            send_sem=sem.at[4],
            recv_sem=sem.at[5],
            device_id=to,
            device_id_type=FLAT,
        ).start()
    send(1, peers[8:])
    own = [pltpu.make_async_copy(slab(q, me), landing(q), sem.at[6 + q]) for q in range(2)]
    own.append(pltpu.make_async_copy(part, sums.at[pl.ds(chip, 1)], sem.at[8]))
    for copy in own:
        copy.start()
    for copy in own:
        copy.wait()
    most = recv.at[pl.ds(0, (DEV - 1) * ROWS)]
    few = sums.at[pl.ds(0, DEV // 2 - 1)]
    pltpu.make_async_copy(few, few, sem.at[5]).wait()
    halves[0] = jnp.sum(sums[...], axis=0)
    for ref, s in ((most, 0), (most, 2), (few, 4), (most, 1)):
        pltpu.make_async_copy(ref, ref, sem.at[s]).wait()
    swap = pltpu.make_async_remote_copy(
        src_ref=halves.at[0],
        dst_ref=halves.at[1],
        send_sem=sem.at[10],
        recv_sem=sem.at[11],
        device_id=partner,
        device_id_type=FLAT,
    )
    swap.start()
    swap.wait()
    level = jnp.sum(halves[...]) / COUNT + 1e-6
    scale = 1.0 / jnp.full((8, 128), level, f32)
    lane = lax.broadcasted_iota(jnp.int32, (8, 128), 1) // TY
    line = lax.broadcasted_iota(jnp.int32, (8, 128), 0) // 2
    step = (line - lane) % 4
    around = sorted(itertools.product(range(4), repeat=2), key=lambda o: -hops(o + (0,)))
    for batch in (around[:5], around[5:11], around[11:]):
        sources = [zs[-dz % 4] * 4 + ys[-dy % 4] for dz, dy in batch]
        for (dz, dy), source in zip(batch, sources):
            block = recv.at[pl.ds(0, (GY if dz or dy else GY - 1) * ROWS)]
            pltpu.make_async_copy(block, block, groups.at[source]).wait()
        for source in sources:
            x0 = pl.multiple_of(source * TX, TX)
            for h in range(2):
                for r in range(ROWS):
                    v = recv[pl.ds((source * GY + 4 * h) * 2 * ROWS + r, 8, stride=ROWS), :]
                    w = v
                    for k in range(1, 4):
                        turned = pltpu.roll(pltpu.roll(v, 2 * k, 0), 128 - TY * k, 1)
                        w = jnp.where(step == k, turned, w)
                    placed[r, pl.ds(x0, TX), h * 128 : (h + 1) * 128] = jnp.log(1.0 + w * scale)
            pltpu.make_async_copy(
                placed.at[:, pl.ds(x0, TX)], out.at[:, pl.ds(x0, TX)], sem.at[9]
            ).start()
    pltpu.make_async_copy(placed, out, sem.at[9]).wait()


def on_device(spectra, resample_index, resample_weight, disp_phase, surface_block):
    f32 = jnp.float32
    bf16 = jnp.bfloat16
    hbm = pl.BlockSpec(memory_space=pltpu.HBM)
    table = jnp.asarray(base_table(), bf16)
    return pl.pallas_call(
        main_kernel,
        out_shape=jax.ShapeDtypeStruct((ROWS, GX * TX, GY * TY), f32),
        in_specs=[hbm] * 6,
        out_specs=hbm,
        scratch_shapes=[
            pltpu.VMEM((2, LINES, NK), bf16),
            pltpu.VMEM((3, RADIX, BLOCK), f32),
            pltpu.VMEM((RADIX, BLOCK), jnp.int32),
            pltpu.VMEM((TX, TY), jnp.int32),
            pltpu.VMEM((RADIX, BLOCK, 2 * BLOCK), bf16),
            pltpu.VMEM((RADIX // 2, NK, 2 * BLOCK), bf16),
            pltpu.VMEM((RADIX, LINES // 2, BLOCK), f32),
            pltpu.VMEM((4, 4, 2, LINES // 2, BLOCK), f32),
            pltpu.VMEM((RADIX, LINES // 2, 2 * BLOCK), bf16),
            pltpu.VMEM((2 * KEEP * BLOCK, 128), f32),
            pltpu.VMEM((1, 1, 128), f32),
            pltpu.VMEM((2, 1, 128), f32),
            pltpu.VMEM((DEV * ROWS * 2, 128), f32),
            pltpu.VMEM((DEV // 2, 1, 128), f32),
            pltpu.VMEM((ROWS, GX * TX, GY * TY), f32),
            pltpu.SemaphoreType.DMA((13,)),
            pltpu.SemaphoreType.DMA((12,)),
            pltpu.SemaphoreType.DMA((GX,)),
        ],
        compiler_params=pltpu.CompilerParams(
            collective_id=0, has_side_effects=True, vmem_limit_bytes=VMEM_BYTES
        ),
        name="main",
    )(
        spectra,
        resample_index.reshape(RADIX, BLOCK),
        resample_weight.reshape(RADIX, BLOCK),
        disp_phase.reshape(RADIX, BLOCK),
        surface_block,
        table,
    )

def solution(mesh):
    return jax.shard_map(
        on_device,
        mesh=mesh,
        in_specs=(P("gx", "gy", None), P(), P(), P(), P("gx", "gy")),
        out_specs=P(("gx", "gy"), None, None),
        check_vma=False,
    )
```

```python
import itertools
import math

import jax
import jax.numpy as jnp
import numpy as np
from jax import lax
from jax.experimental import pallas as pl
from jax.experimental.pallas import tpu as pltpu
from jax.sharding import PartitionSpec as P

NK = 2048
BLOCK = 128
KEEP = 5
RADIX = 16
GX = 16
GY = 8
DEV = GX * GY
TX = 8
TY = 32
LINES = TX * TY
ROWS = KEEP * BLOCK // DEV
COUNT = 128 * 256 * KEEP * BLOCK
MESH = pl.DeviceIdType.MESH
VMEM_BYTES = 67043328
CHUNKS = 8


def base_table():
    c = np.arange(RADIX)[:, None, None]
    b = np.arange(NK // (2 * RADIX))[None, :, None]
    m = np.arange(BLOCK)[None, None, :]
    angle = 2.0 * math.pi * ((m * (RADIX * b + c)) % NK) / NK
    cos, sin = np.cos(angle), np.sin(angle)
    top = np.concatenate([cos, sin], axis=2)
    low = np.concatenate([-sin, cos], axis=2)
    return np.concatenate([top, low], axis=1).astype(np.float32)


def rot(z, k, n):
    re, im = z
    k = k % n
    if k == 0:
        return re, im
    if 4 * k == n:
        return im, -re
    if 2 * k == n:
        return -re, -im
    if 4 * k == 3 * n:
        return -im, re
    if 8 * k == n:
        h = math.sqrt(0.5)
        return h * (re + im), h * (im - re)
    if 8 * k == 3 * n:
        h = math.sqrt(0.5)
        return h * (im - re), -h * (re + im)
    c, s = math.cos(2 * math.pi * k / n), math.sin(2 * math.pi * k / n)
    return c * re + s * im, c * im - s * re


def add(a, b):
    return a[0] + b[0], a[1] + b[1]


def sub(a, b):
    return a[0] - b[0], a[1] - b[1]


def fft4(z):
    a, b = add(z[0], z[2]), sub(z[0], z[2])
    c, d = add(z[1], z[3]), sub(z[1], z[3])
    d = rot(d, 1, 4)
    return [add(a, c), add(b, d), sub(a, c), sub(b, d)]


def hops(o):
    return sum((0, 1, 2, 1)[v] for v in o[:3])


OFFSETS = sorted(
    [o for o in itertools.product(range(4), range(4), range(4), range(2)) if any(o)],
    key=lambda o: (-hops(o), o),
)


def main_kernel(
    spectra, index, weight, phase, surface, table, recv, totals,
    both, params, idx, surf, tab, hits, x, mid, y, msg, part, total, sums, load, sem,
):
    f32, bf16 = jnp.float32, jnp.bfloat16
    half = LINES // 2
    gx, gy = lax.axis_index("gx"), lax.axis_index("gy")
    me = gx * GY + gy
    zs = [(gx // 4 + d) % 4 for d in range(4)]
    ys = [(gx % 4 + d) % 4 for d in range(4)]
    xs = [(gy // 2 + d) % 4 for d in range(4)]
    cs = [(gy % 2 + d) % 2 for d in range(2)]
    zy = [[z * 4 + v for v in ys] for z in zs]
    xc = [[v * 2 + c for c in cs] for v in xs]
    peers = [(zy[o[0]][o[1]], xc[o[2]][o[3]]) for o in OFFSETS]
    alike = [to for o, to in zip(OFFSETS, peers) if o[3] == 0]
    partner = (zy[0][0], xc[0][1])
    chip = gx * (GY // 2) + gy // 2
    barrier = pltpu.get_barrier_semaphore()

    small = [
        pltpu.make_async_copy(index, idx, load.at[0]),
        pltpu.make_async_copy(weight, params.at[0], load.at[1]),
        pltpu.make_async_copy(phase, params.at[1], load.at[2]),
        pltpu.make_async_copy(surface, surf, load.at[3]),
    ]
    tiles = [
        pltpu.make_async_copy(
            spectra.at[2 * p + q], both.at[q, pl.ds(p * TY, TY)], load.at[4 + 4 * q + p]
        )
        for q in range(2)
        for p in range(4)
    ]
    big = pltpu.make_async_copy(table, tab, load.at[12])
    for copy in small + tiles + [big]:
        copy.start()
    for to in peers:
        pl.semaphore_signal(barrier, inc=1, device_id=to, device_id_type=MESH)
    for copy in small:
        copy.wait()
    cosp = jnp.cos(params[1])
    sinp = jnp.sin(params[1])
    params[1] = cosp
    params[2] = sinp
    tops = [
        jnp.concatenate([surf[2 * p + q : 2 * p + q + 1, :] for p in range(4)], axis=1)
        for q in range(2)
    ]
    row = lax.broadcasted_iota(jnp.int32, (BLOCK, 2 * BLOCK), 0).astype(jnp.int16)
    one = jnp.ones((BLOCK, 2 * BLOCK), bf16)
    zero = jnp.zeros((BLOCK, 2 * BLOCK), bf16)
    nt = (((1,), (1,)), ((), ()))

    def shift(q):
        for copy in tiles[4 * q : 4 * q + 4]:
            copy.wait()
        lines = both[q, :half, :]
        both[q, half:, :] = jnp.concatenate([lines[:, 1:], lines[:, :1]], axis=1)

    def compute(q, acc):
        for n in range(4):
            for e in range(2):
                if q == 0:
                    pick = jnp.concatenate(
                        [idx[n + 8 * e + 4 * h : n + 8 * e + 4 * h + 1, :] for h in range(2)], axis=1
                    ).astype(jnp.int16)
                    for k in range(NK // 128):
                        seen = row + jnp.int16(128 * k) == pick
                        hits[2 * n + e, k * 128 : (k + 1) * 128, :] = jnp.where(seen, one, zero)
                pair = jnp.dot(both[q], hits[2 * n + e], preferred_element_type=f32)
                for h in range(2):
                    at = n + 8 * e + 4 * h
                    lane = slice(h * BLOCK, (h + 1) * BLOCK)
                    w = params[0, at : at + 1, :]
                    x[at] = (1.0 - w) * pair[:half, lane] + w * pair[half:, lane]
            for g in range(half // 16):
                rows = slice(16 * g, 16 * g + 16)
                z = []
                for m in range(4):
                    at = n + 4 * m
                    v = x[at, rows, :]
                    z.append(
                        [
                            (v * params[1 + o, at : at + 1, :]).astype(bf16).astype(f32)
                            for o in range(2)
                        ]
                    )
                for c, value in enumerate(fft4(z)):
                    for o, half_value in enumerate(rot(value, n * c, RADIX)):
                        mid[n, c, o, rows, :] = half_value
        if q == 0:
            big.wait()
        for low in range(4):
            for g in range(half // 16):
                rows = slice(16 * g, 16 * g + 16)
                z = [[mid[n, low, o, rows, :] for o in range(2)] for n in range(4)]
                for high, value in enumerate(fft4(z)):
                    for o in range(2):
                        y[low + 4 * high, rows, o * BLOCK : (o + 1) * BLOCK] = value[o].astype(bf16)
            for c in range(low, RADIX, 4):
                depth = lax.dot_general(tab[c], y[c], nt, preferred_element_type=f32)
                power = depth[:64] * depth[:64] + depth[64:] * depth[64:]
                tile = [power[8 * b : 8 * b + 8] for b in range(8)]
                for k in range(KEEP):
                    kept = tile[k]
                    for s in range(1, 4):
                        kept = jnp.where(tops[q] == s, tile[k + s], kept)
                    acc = acc + kept
                    msg[pl.ds((q * KEEP + k) * BLOCK + c, 8, stride=RADIX), :] = kept
        return acc

    def slab(q, dest):
        return msg.at[pl.ds(q * KEEP * BLOCK + ROWS * dest, ROWS)]

    def landing(q):
        return recv.at[pl.ds((2 * me + q) * ROWS, ROWS)]

    def send(q, among):
        for to in among:
            pltpu.make_async_remote_copy(
                src_ref=slab(q, to[0] * GY + to[1]),
                dst_ref=landing(q),
                send_sem=sem.at[2 * q],
                recv_sem=sem.at[2 * q + 1],
                device_id=to,
                device_id_type=MESH,
            ).start()

    shift(0)
    acc = compute(0, jnp.zeros((8, 128), f32))
    shift(1)
    pl.semaphore_wait(barrier, DEV - 1)
    send(0, peers)
    acc = compute(1, acc)
    part[...] = jnp.sum(acc, axis=0, keepdims=True).reshape(1, 1, 128)
    for to in alike:
        pltpu.make_async_remote_copy(
            src_ref=part,
            dst_ref=sums.at[pl.ds(chip, 1)],
            send_sem=sem.at[4],
            recv_sem=sem.at[5],
            device_id=to,
            device_id_type=MESH,
        ).start()
    send(1, peers)
    own = [pltpu.make_async_copy(slab(q, me), landing(q), sem.at[6 + q]) for q in range(2)]
    own.append(pltpu.make_async_copy(part, sums.at[pl.ds(chip, 1)], sem.at[8]))
    for copy in own:
        copy.start()
    for copy in own:
        copy.wait()
    most = recv.at[pl.ds(0, (DEV - 1) * ROWS)]
    few = sums.at[pl.ds(0, DEV // 2 - 1)]
    pltpu.make_async_copy(few, few, sem.at[5]).wait()
    total[...] = jnp.sum(sums[...], axis=0, keepdims=True)
    for ref, s in ((most, 0), (most, 2), (few, 4), (most, 1)):
        pltpu.make_async_copy(ref, ref, sem.at[s]).wait()
    swap = pltpu.make_async_remote_copy(
        src_ref=total,
        dst_ref=totals.at[pl.ds(1, 1)],
        send_sem=sem.at[9],
        recv_sem=sem.at[10],
        device_id=partner,
        device_id_type=MESH,
    )
    swap.start()
    keep = pltpu.make_async_copy(total, totals.at[pl.ds(0, 1)], sem.at[11])
    keep.start()
    keep.wait()
    swap.wait()
    pltpu.make_async_copy(most, most, sem.at[3]).wait()


def place_kernel(recv, totals, out, rows, both, placed, sem):
    step_rows = DEV * ROWS * 2 // CHUNKS
    step_lines = GX * TX // CHUNKS
    first = pltpu.make_async_copy(totals, both, sem.at[CHUNKS])
    first.start()
    chunks = []
    for i in range(CHUNKS):
        at = pl.ds(i * step_rows, step_rows)
        chunks.append(pltpu.make_async_copy(recv.at[at], rows.at[at], sem.at[i]))
        chunks[-1].start()
    first.wait()
    level = jnp.sum(both[...]) / COUNT + 1e-6
    scale = 1.0 / jnp.full((8, 128), level, jnp.float32)
    lane = lax.broadcasted_iota(jnp.int32, (8, 128), 1) // TY
    pair = lax.broadcasted_iota(jnp.int32, (8, 128), 0) // 2
    step = (pair - lane) % 4
    for i in range(CHUNKS):
        chunks[i].wait()
        for source in range(i * GX // CHUNKS, (i + 1) * GX // CHUNKS):
            for h in range(2):
                for r in range(ROWS):
                    v = rows[pl.ds((source * GY + 4 * h) * 2 * ROWS + r, 8, stride=ROWS), :]
                    w = v
                    for k in range(1, 4):
                        turned = pltpu.roll(pltpu.roll(v, 2 * k, 0), 128 - TY * k, 1)
                        w = jnp.where(step == k, turned, w)
                    placed[r, source * TX : (source + 1) * TX, h * 128 : (h + 1) * 128] = jnp.log(
                        1.0 + w * scale
                    )
        at = pl.ds(i * step_lines, step_lines)
        pltpu.make_async_copy(placed.at[:, at], out.at[:, at], sem.at[CHUNKS + 1]).start()
    pltpu.make_async_copy(placed, out, sem.at[CHUNKS + 1]).wait()


def on_device(spectra, resample_index, resample_weight, disp_phase, surface_block):
    f32 = jnp.float32
    bf16 = jnp.bfloat16
    hbm = pl.BlockSpec(memory_space=pltpu.HBM)
    table = jnp.asarray(base_table(), bf16)
    recv, totals = pl.pallas_call(
        main_kernel,
        out_shape=(
            jax.ShapeDtypeStruct((DEV * ROWS * 2, 128), f32),
            jax.ShapeDtypeStruct((2, 1, 128), f32),
        ),
        in_specs=[hbm] * 6,
        out_specs=[hbm] * 2,
        scratch_shapes=[
            pltpu.VMEM((2, LINES, NK), bf16),
            pltpu.VMEM((3, RADIX, BLOCK), f32),
            pltpu.VMEM((RADIX, BLOCK), jnp.int32),
            pltpu.VMEM((TX, TY), jnp.int32),
            pltpu.VMEM((RADIX, BLOCK, 2 * BLOCK), bf16),
            pltpu.VMEM((RADIX // 2, NK, 2 * BLOCK), bf16),
            pltpu.VMEM((RADIX, LINES // 2, BLOCK), f32),
            pltpu.VMEM((4, 4, 2, LINES // 2, BLOCK), f32),
            pltpu.VMEM((RADIX, LINES // 2, 2 * BLOCK), bf16),
            pltpu.VMEM((2 * KEEP * BLOCK, 128), f32),
            pltpu.VMEM((1, 1, 128), f32),
            pltpu.VMEM((1, 1, 128), f32),
            pltpu.VMEM((DEV // 2, 1, 128), f32),
            pltpu.SemaphoreType.DMA((13,)),
            pltpu.SemaphoreType.DMA((12,)),
        ],
        compiler_params=pltpu.CompilerParams(
            collective_id=0, has_side_effects=True, vmem_limit_bytes=VMEM_BYTES
        ),
        name="main",
    )(
        spectra,
        resample_index.reshape(RADIX, BLOCK),
        resample_weight.reshape(RADIX, BLOCK),
        disp_phase.reshape(RADIX, BLOCK),
        surface_block,
        table,
    )
    return pl.pallas_call(
        place_kernel,
        out_shape=jax.ShapeDtypeStruct((ROWS, GX * TX, GY * TY), f32),
        in_specs=[hbm] * 2,
        out_specs=hbm,
        scratch_shapes=[
            pltpu.VMEM((DEV * ROWS * 2, 128), f32),
            pltpu.VMEM((2, 1, 128), f32),
            pltpu.VMEM((ROWS, GX * TX, GY * TY), f32),
            pltpu.SemaphoreType.DMA((CHUNKS + 2,)),
        ],
        compiler_params=pltpu.CompilerParams(vmem_limit_bytes=VMEM_BYTES),
        name="place",
    )(recv, totals)

def solution(mesh):
    return jax.shard_map(
        on_device,
        mesh=mesh,
        in_specs=(P("gx", "gy", None), P(), P(), P(), P("gx", "gy")),
        out_specs=P(("gx", "gy"), None, None),
        check_vma=False,
    )
```

```python
import itertools
import math

import jax
import jax.numpy as jnp
import numpy as np
from jax import lax
from jax.experimental import pallas as pl
from jax.experimental.pallas import tpu as pltpu
from jax.sharding import PartitionSpec as P

NK = 2048
BLOCK = 128
KEEP = 5
RADIX = 16
GX = 16
GY = 8
DEV = GX * GY
TX = 8
TY = 32
LINES = TX * TY
ROWS = KEEP * BLOCK // DEV
COUNT = 128 * 256 * KEEP * BLOCK
MESH = pl.DeviceIdType.MESH
VMEM_BYTES = 67043328
CHUNKS = 2


def base_table():
    c = np.arange(RADIX)[:, None, None]
    b = np.arange(NK // (2 * RADIX))[None, :, None]
    m = np.arange(BLOCK)[None, None, :]
    angle = 2.0 * math.pi * ((m * (RADIX * b + c)) % NK) / NK
    cos, sin = np.cos(angle), np.sin(angle)
    top = np.concatenate([cos, sin], axis=2)
    low = np.concatenate([-sin, cos], axis=2)
    return np.concatenate([top, low], axis=1).astype(np.float32)


def rot(z, k, n):
    re, im = z
    k = k % n
    if k == 0:
        return re, im
    if 4 * k == n:
        return im, -re
    if 2 * k == n:
        return -re, -im
    if 4 * k == 3 * n:
        return -im, re
    if 8 * k == n:
        h = math.sqrt(0.5)
        return h * (re + im), h * (im - re)
    if 8 * k == 3 * n:
        h = math.sqrt(0.5)
        return h * (im - re), -h * (re + im)
    c, s = math.cos(2 * math.pi * k / n), math.sin(2 * math.pi * k / n)
    return c * re + s * im, c * im - s * re


def add(a, b):
    return a[0] + b[0], a[1] + b[1]


def sub(a, b):
    return a[0] - b[0], a[1] - b[1]


def fft4(z):
    a, b = add(z[0], z[2]), sub(z[0], z[2])
    c, d = add(z[1], z[3]), sub(z[1], z[3])
    d = rot(d, 1, 4)
    return [add(a, c), add(b, d), sub(a, c), sub(b, d)]


def hops(o):
    return sum((0, 1, 2, 1)[v] for v in o[:3])


OFFSETS = sorted(
    [o for o in itertools.product(range(4), range(4), range(4), range(2)) if any(o)],
    key=lambda o: (-hops(o), o),
)


def main_kernel(
    spectra, index, weight, phase, surface, table, recv, totals,
    both, params, idx, surf, tab, hits, x, mid, y, msg, part, total, sums, load, sem,
):
    f32, bf16 = jnp.float32, jnp.bfloat16
    half = LINES // 2
    gx, gy = lax.axis_index("gx"), lax.axis_index("gy")
    me = gx * GY + gy
    zs = [(gx // 4 + d) % 4 for d in range(4)]
    ys = [(gx % 4 + d) % 4 for d in range(4)]
    xs = [(gy // 2 + d) % 4 for d in range(4)]
    cs = [(gy % 2 + d) % 2 for d in range(2)]
    zy = [[z * 4 + v for v in ys] for z in zs]
    xc = [[v * 2 + c for c in cs] for v in xs]
    peers = [(zy[o[0]][o[1]], xc[o[2]][o[3]]) for o in OFFSETS]
    alike = [to for o, to in zip(OFFSETS, peers) if o[3] == 0]
    partner = (zy[0][0], xc[0][1])
    chip = gx * (GY // 2) + gy // 2
    barrier = pltpu.get_barrier_semaphore()

    small = [
        pltpu.make_async_copy(index, idx, load.at[0]),
        pltpu.make_async_copy(weight, params.at[0], load.at[1]),
        pltpu.make_async_copy(phase, params.at[1], load.at[2]),
        pltpu.make_async_copy(surface, surf, load.at[3]),
    ]
    tiles = [
        pltpu.make_async_copy(
            spectra.at[2 * p + q], both.at[q, pl.ds(p * TY, TY)], load.at[4 + 4 * q + p]
        )
        for q in range(2)
        for p in range(4)
    ]
    big = pltpu.make_async_copy(table, tab, load.at[12])
    for copy in small + tiles + [big]:
        copy.start()
    for to in peers:
        pl.semaphore_signal(barrier, inc=1, device_id=to, device_id_type=MESH)
    for copy in small:
        copy.wait()
    cosp = jnp.cos(params[1])
    sinp = jnp.sin(params[1])
    params[1] = cosp
    params[2] = sinp
    tops = [
        jnp.concatenate([surf[2 * p + q : 2 * p + q + 1, :] for p in range(4)], axis=1)
        for q in range(2)
    ]
    row = lax.broadcasted_iota(jnp.int32, (BLOCK, 2 * BLOCK), 0).astype(jnp.int16)
    one = jnp.ones((BLOCK, 2 * BLOCK), bf16)
    zero = jnp.zeros((BLOCK, 2 * BLOCK), bf16)
    nt = (((1,), (1,)), ((), ()))

    def shift(q):
        for copy in tiles[4 * q : 4 * q + 4]:
            copy.wait()
        lines = both[q, :half, :]
        both[q, half:, :] = jnp.concatenate([lines[:, 1:], lines[:, :1]], axis=1)

    def compute(q, acc):
        for n in range(4):
            for e in range(2):
                if q == 0:
                    pick = jnp.concatenate(
                        [idx[n + 8 * e + 4 * h : n + 8 * e + 4 * h + 1, :] for h in range(2)], axis=1
                    ).astype(jnp.int16)
                    for k in range(NK // 128):
                        seen = row + jnp.int16(128 * k) == pick
                        hits[2 * n + e, k * 128 : (k + 1) * 128, :] = jnp.where(seen, one, zero)
                pair = jnp.dot(both[q], hits[2 * n + e], preferred_element_type=f32)
                for h in range(2):
                    at = n + 8 * e + 4 * h
                    lane = slice(h * BLOCK, (h + 1) * BLOCK)
                    w = params[0, at : at + 1, :]
                    x[at] = (1.0 - w) * pair[:half, lane] + w * pair[half:, lane]
            for g in range(half // 16):
                rows = slice(16 * g, 16 * g + 16)
                z = []
                for m in range(4):
                    at = n + 4 * m
                    v = x[at, rows, :]
                    z.append(
                        [
                            (v * params[1 + o, at : at + 1, :]).astype(bf16).astype(f32)
                            for o in range(2)
                        ]
                    )
                for c, value in enumerate(fft4(z)):
                    for o, half_value in enumerate(rot(value, n * c, RADIX)):
                        mid[n, c, o, rows, :] = half_value
        if q == 0:
            big.wait()
        for low in range(4):
            for g in range(half // 16):
                rows = slice(16 * g, 16 * g + 16)
                z = [[mid[n, low, o, rows, :] for o in range(2)] for n in range(4)]
                for high, value in enumerate(fft4(z)):
                    for o in range(2):
                        y[low + 4 * high, rows, o * BLOCK : (o + 1) * BLOCK] = value[o].astype(bf16)
            for c in range(low, RADIX, 4):
                depth = lax.dot_general(tab[c], y[c], nt, preferred_element_type=f32)
                power = depth[:64] * depth[:64] + depth[64:] * depth[64:]
                tile = [power[8 * b : 8 * b + 8] for b in range(8)]
                for k in range(KEEP):
                    kept = tile[k]
                    for s in range(1, 4):
                        kept = jnp.where(tops[q] == s, tile[k + s], kept)
                    acc = acc + kept
                    msg[pl.ds((q * KEEP + k) * BLOCK + c, 8, stride=RADIX), :] = kept
        return acc

    def slab(q, dest):
        return msg.at[pl.ds(q * KEEP * BLOCK + ROWS * dest, ROWS)]

    def landing(q):
        return recv.at[pl.ds((2 * me + q) * ROWS, ROWS)]

    def send(q, among):
        for to in among:
            pltpu.make_async_remote_copy(
                src_ref=slab(q, to[0] * GY + to[1]),
                dst_ref=landing(q),
                send_sem=sem.at[2 * q],
                recv_sem=sem.at[2 * q + 1],
                device_id=to,
                device_id_type=MESH,
            ).start()

    shift(0)
    acc = compute(0, jnp.zeros((8, 128), f32))
    pl.semaphore_wait(barrier, DEV - 1)
    send(0, peers)
    shift(1)
    acc = compute(1, acc)
    part[...] = jnp.sum(acc, axis=0, keepdims=True).reshape(1, 1, 128)
    for to in alike:
        pltpu.make_async_remote_copy(
            src_ref=part,
            dst_ref=sums.at[pl.ds(chip, 1)],
            send_sem=sem.at[4],
            recv_sem=sem.at[5],
            device_id=to,
            device_id_type=MESH,
        ).start()
    send(1, peers)
    own = [pltpu.make_async_copy(slab(q, me), landing(q), sem.at[6 + q]) for q in range(2)]
    own.append(pltpu.make_async_copy(part, sums.at[pl.ds(chip, 1)], sem.at[8]))
    for copy in own:
        copy.start()
    for copy in own:
        copy.wait()
    most = recv.at[pl.ds(0, (DEV - 1) * ROWS)]
    few = sums.at[pl.ds(0, DEV // 2 - 1)]
    pltpu.make_async_copy(few, few, sem.at[5]).wait()
    total[...] = jnp.sum(sums[...], axis=0, keepdims=True)
    for ref, s in ((most, 0), (most, 2), (few, 4), (most, 1)):
        pltpu.make_async_copy(ref, ref, sem.at[s]).wait()
    swap = pltpu.make_async_remote_copy(
        src_ref=total,
        dst_ref=totals.at[pl.ds(1, 1)],
        send_sem=sem.at[9],
        recv_sem=sem.at[10],
        device_id=partner,
        device_id_type=MESH,
    )
    swap.start()
    keep = pltpu.make_async_copy(total, totals.at[pl.ds(0, 1)], sem.at[11])
    keep.start()
    keep.wait()
    swap.wait()
    pltpu.make_async_copy(most, most, sem.at[3]).wait()


def place_kernel(recv, totals, out, rows, both, placed, sem):
    step_rows = DEV * ROWS * 2 // CHUNKS
    step_lines = GX * TX // CHUNKS
    first = pltpu.make_async_copy(totals, both, sem.at[CHUNKS])
    first.start()
    chunks = []
    for i in range(CHUNKS):
        at = pl.ds(i * step_rows, step_rows)
        chunks.append(pltpu.make_async_copy(recv.at[at], rows.at[at], sem.at[i]))
        chunks[-1].start()
    first.wait()
    level = jnp.sum(both[...]) / COUNT + 1e-6
    scale = 1.0 / jnp.full((8, 128), level, jnp.float32)
    lane = lax.broadcasted_iota(jnp.int32, (8, 128), 1) // TY
    pair = lax.broadcasted_iota(jnp.int32, (8, 128), 0) // 2
    step = (pair - lane) % 4
    for i in range(CHUNKS):
        chunks[i].wait()
        for source in range(i * GX // CHUNKS, (i + 1) * GX // CHUNKS):
            for h in range(2):
                for r in range(ROWS):
                    v = rows[pl.ds((source * GY + 4 * h) * 2 * ROWS + r, 8, stride=ROWS), :]
                    w = v
                    for k in range(1, 4):
                        turned = pltpu.roll(pltpu.roll(v, 2 * k, 0), 128 - TY * k, 1)
                        w = jnp.where(step == k, turned, w)
                    placed[r, source * TX : (source + 1) * TX, h * 128 : (h + 1) * 128] = jnp.log(
                        1.0 + w * scale
                    )
        at = pl.ds(i * step_lines, step_lines)
        pltpu.make_async_copy(placed.at[:, at], out.at[:, at], sem.at[CHUNKS + 1]).start()
    pltpu.make_async_copy(placed, out, sem.at[CHUNKS + 1]).wait()


def on_device(spectra, resample_index, resample_weight, disp_phase, surface_block):
    f32 = jnp.float32
    bf16 = jnp.bfloat16
    hbm = pl.BlockSpec(memory_space=pltpu.HBM)
    table = jnp.asarray(base_table(), bf16)
    recv, totals = pl.pallas_call(
        main_kernel,
        out_shape=(
            jax.ShapeDtypeStruct((DEV * ROWS * 2, 128), f32),
            jax.ShapeDtypeStruct((2, 1, 128), f32),
        ),
        in_specs=[hbm] * 6,
        out_specs=[hbm] * 2,
        scratch_shapes=[
            pltpu.VMEM((2, LINES, NK), bf16),
            pltpu.VMEM((3, RADIX, BLOCK), f32),
            pltpu.VMEM((RADIX, BLOCK), jnp.int32),
            pltpu.VMEM((TX, TY), jnp.int32),
            pltpu.VMEM((RADIX, BLOCK, 2 * BLOCK), bf16),
            pltpu.VMEM((RADIX // 2, NK, 2 * BLOCK), bf16),
            pltpu.VMEM((RADIX, LINES // 2, BLOCK), f32),
            pltpu.VMEM((4, 4, 2, LINES // 2, BLOCK), f32),
            pltpu.VMEM((RADIX, LINES // 2, 2 * BLOCK), bf16),
            pltpu.VMEM((2 * KEEP * BLOCK, 128), f32),
            pltpu.VMEM((1, 1, 128), f32),
            pltpu.VMEM((1, 1, 128), f32),
            pltpu.VMEM((DEV // 2, 1, 128), f32),
            pltpu.SemaphoreType.DMA((13,)),
            pltpu.SemaphoreType.DMA((12,)),
        ],
        compiler_params=pltpu.CompilerParams(
            collective_id=0, has_side_effects=True, vmem_limit_bytes=VMEM_BYTES
        ),
        name="main",
    )(
        spectra,
        resample_index.reshape(RADIX, BLOCK),
        resample_weight.reshape(RADIX, BLOCK),
        disp_phase.reshape(RADIX, BLOCK),
        surface_block,
        table,
    )
    return pl.pallas_call(
        place_kernel,
        out_shape=jax.ShapeDtypeStruct((ROWS, GX * TX, GY * TY), f32),
        in_specs=[hbm] * 2,
        out_specs=hbm,
        scratch_shapes=[
            pltpu.VMEM((DEV * ROWS * 2, 128), f32),
            pltpu.VMEM((2, 1, 128), f32),
            pltpu.VMEM((ROWS, GX * TX, GY * TY), f32),
            pltpu.SemaphoreType.DMA((CHUNKS + 2,)),
        ],
        compiler_params=pltpu.CompilerParams(vmem_limit_bytes=VMEM_BYTES),
        name="place",
    )(recv, totals)

def solution(mesh):
    return jax.shard_map(
        on_device,
        mesh=mesh,
        in_specs=(P("gx", "gy", None), P(), P(), P(), P("gx", "gy")),
        out_specs=P(("gx", "gy"), None, None),
        check_vma=False,
    )
```

```python
import itertools
import math

import jax
import jax.numpy as jnp
import numpy as np
from jax import lax
from jax.experimental import pallas as pl
from jax.experimental.pallas import tpu as pltpu
from jax.sharding import PartitionSpec as P

NK = 2048
BLOCK = 128
KEEP = 5
RADIX = 16
GX = 16
GY = 8
DEV = GX * GY
TX = 8
TY = 32
LINES = TX * TY
ROWS = KEEP * BLOCK // DEV
COUNT = 128 * 256 * KEEP * BLOCK
MESH = pl.DeviceIdType.MESH
VMEM_BYTES = 67043328
CHUNKS = 2


def base_table():
    c = np.arange(RADIX)[:, None, None]
    b = np.arange(NK // (2 * RADIX))[None, :, None]
    m = np.arange(BLOCK)[None, None, :]
    angle = 2.0 * math.pi * ((m * (RADIX * b + c)) % NK) / NK
    cos, sin = np.cos(angle), np.sin(angle)
    top = np.concatenate([cos, sin], axis=2)
    low = np.concatenate([-sin, cos], axis=2)
    return np.concatenate([top, low], axis=1).astype(np.float32)


def rot(z, k, n):
    re, im = z
    k = k % n
    if k == 0:
        return re, im
    if 4 * k == n:
        return im, -re
    if 2 * k == n:
        return -re, -im
    if 4 * k == 3 * n:
        return -im, re
    if 8 * k == n:
        h = math.sqrt(0.5)
        return h * (re + im), h * (im - re)
    if 8 * k == 3 * n:
        h = math.sqrt(0.5)
        return h * (im - re), -h * (re + im)
    c, s = math.cos(2 * math.pi * k / n), math.sin(2 * math.pi * k / n)
    return c * re + s * im, c * im - s * re


def add(a, b):
    return a[0] + b[0], a[1] + b[1]


def sub(a, b):
    return a[0] - b[0], a[1] - b[1]


def fft4(z):
    a, b = add(z[0], z[2]), sub(z[0], z[2])
    c, d = add(z[1], z[3]), sub(z[1], z[3])
    d = rot(d, 1, 4)
    return [add(a, c), add(b, d), sub(a, c), sub(b, d)]


def hops(o):
    return sum((0, 1, 2, 1)[v] for v in o[:3])


FAR_FIRST = sorted(
    [o for o in itertools.product(range(4), range(4), range(4), range(2)) if any(o)],
    key=lambda o: (-hops(o), o),
)


def first_link(o):
    for d in (2, 1, 0):
        if o[d]:
            return 3 * d + o[d]
    return 0


def woven(offsets):
    lanes = {}
    for o in offsets:
        lanes.setdefault(first_link(o), []).append(o)
    keyed = [
        ((i + 0.5) / len(lane), link, o) for link, lane in lanes.items() for i, o in enumerate(lane)
    ]
    return [o for _, _, o in sorted(keyed)]


OFFSETS = woven(FAR_FIRST)


def main_kernel(
    spectra, index, weight, phase, surface, table, recv, totals,
    both, params, idx, surf, tab, hits, x, mid, y, msg, part, total, sums, load, sem,
):
    f32, bf16 = jnp.float32, jnp.bfloat16
    half = LINES // 2
    gx, gy = lax.axis_index("gx"), lax.axis_index("gy")
    me = gx * GY + gy
    zs = [(gx // 4 + d) % 4 for d in range(4)]
    ys = [(gx % 4 + d) % 4 for d in range(4)]
    xs = [(gy // 2 + d) % 4 for d in range(4)]
    cs = [(gy % 2 + d) % 2 for d in range(2)]
    zy = [[z * 4 + v for v in ys] for z in zs]
    xc = [[v * 2 + c for c in cs] for v in xs]
    peers = [(zy[o[0]][o[1]], xc[o[2]][o[3]]) for o in OFFSETS]
    alike = [to for o, to in zip(OFFSETS, peers) if o[3] == 0]
    partner = (zy[0][0], xc[0][1])
    chip = gx * (GY // 2) + gy // 2
    barrier = pltpu.get_barrier_semaphore()

    small = [
        pltpu.make_async_copy(index, idx, load.at[0]),
        pltpu.make_async_copy(weight, params.at[0], load.at[1]),
        pltpu.make_async_copy(phase, params.at[1], load.at[2]),
        pltpu.make_async_copy(surface, surf, load.at[3]),
    ]
    tiles = [
        pltpu.make_async_copy(
            spectra.at[2 * p + q], both.at[q, pl.ds(p * TY, TY)], load.at[4 + 4 * q + p]
        )
        for q in range(2)
        for p in range(4)
    ]
    big = pltpu.make_async_copy(table, tab, load.at[12])
    for copy in small + tiles + [big]:
        copy.start()
    for to in peers:
        pl.semaphore_signal(barrier, inc=1, device_id=to, device_id_type=MESH)
    for copy in small:
        copy.wait()
    cosp = jnp.cos(params[1])
    sinp = jnp.sin(params[1])
    params[1] = cosp
    params[2] = sinp
    tops = [
        jnp.concatenate([surf[2 * p + q : 2 * p + q + 1, :] for p in range(4)], axis=1)
        for q in range(2)
    ]
    row = lax.broadcasted_iota(jnp.int32, (BLOCK, 2 * BLOCK), 0).astype(jnp.int16)
    one = jnp.ones((BLOCK, 2 * BLOCK), bf16)
    zero = jnp.zeros((BLOCK, 2 * BLOCK), bf16)
    nt = (((1,), (1,)), ((), ()))

    def shift(q):
        for copy in tiles[4 * q : 4 * q + 4]:
            copy.wait()
        lines = both[q, :half, :]
        both[q, half:, :] = jnp.concatenate([lines[:, 1:], lines[:, :1]], axis=1)

    def compute(q, acc):
        for n in range(4):
            for e in range(2):
                if q == 0:
                    pick = jnp.concatenate(
                        [idx[n + 8 * e + 4 * h : n + 8 * e + 4 * h + 1, :] for h in range(2)], axis=1
                    ).astype(jnp.int16)
                    for k in range(NK // 128):
                        seen = row + jnp.int16(128 * k) == pick
                        hits[2 * n + e, k * 128 : (k + 1) * 128, :] = jnp.where(seen, one, zero)
                pair = jnp.dot(both[q], hits[2 * n + e], preferred_element_type=f32)
                for h in range(2):
                    at = n + 8 * e + 4 * h
                    lane = slice(h * BLOCK, (h + 1) * BLOCK)
                    w = params[0, at : at + 1, :]
                    x[at] = (1.0 - w) * pair[:half, lane] + w * pair[half:, lane]
            for g in range(half // 16):
                rows = slice(16 * g, 16 * g + 16)
                z = []
                for m in range(4):
                    at = n + 4 * m
                    v = x[at, rows, :]
                    z.append(
                        [
                            (v * params[1 + o, at : at + 1, :]).astype(bf16).astype(f32)
                            for o in range(2)
                        ]
                    )
                for c, value in enumerate(fft4(z)):
                    for o, half_value in enumerate(rot(value, n * c, RADIX)):
                        mid[n, c, o, rows, :] = half_value
        if q == 0:
            big.wait()
        for low in range(4):
            for g in range(half // 16):
                rows = slice(16 * g, 16 * g + 16)
                z = [[mid[n, low, o, rows, :] for o in range(2)] for n in range(4)]
                for high, value in enumerate(fft4(z)):
                    for o in range(2):
                        y[low + 4 * high, rows, o * BLOCK : (o + 1) * BLOCK] = value[o].astype(bf16)
            for c in range(low, RADIX, 4):
                depth = lax.dot_general(tab[c], y[c], nt, preferred_element_type=f32)
                power = depth[:64] * depth[:64] + depth[64:] * depth[64:]
                tile = [power[8 * b : 8 * b + 8] for b in range(8)]
                for k in range(KEEP):
                    kept = tile[k]
                    for s in range(1, 4):
                        kept = jnp.where(tops[q] == s, tile[k + s], kept)
                    acc = acc + kept
                    msg[pl.ds((q * KEEP + k) * BLOCK + c, 8, stride=RADIX), :] = kept
        return acc

    def slab(q, dest):
        return msg.at[pl.ds(q * KEEP * BLOCK + ROWS * dest, ROWS)]

    def landing(q):
        return recv.at[pl.ds((2 * me + q) * ROWS, ROWS)]

    def send(q, among):
        for to in among:
            pltpu.make_async_remote_copy(
                src_ref=slab(q, to[0] * GY + to[1]),
                dst_ref=landing(q),
                send_sem=sem.at[2 * q],
                recv_sem=sem.at[2 * q + 1],
                device_id=to,
                device_id_type=MESH,
            ).start()

    shift(0)
    acc = compute(0, jnp.zeros((8, 128), f32))
    pl.semaphore_wait(barrier, DEV - 1)
    send(0, peers)
    shift(1)
    acc = compute(1, acc)
    part[...] = jnp.sum(acc, axis=0, keepdims=True).reshape(1, 1, 128)
    for to in alike:
        pltpu.make_async_remote_copy(
            src_ref=part,
            dst_ref=sums.at[pl.ds(chip, 1)],
            send_sem=sem.at[4],
            recv_sem=sem.at[5],
            device_id=to,
            device_id_type=MESH,
        ).start()
    send(1, peers)
    own = [pltpu.make_async_copy(slab(q, me), landing(q), sem.at[6 + q]) for q in range(2)]
    own.append(pltpu.make_async_copy(part, sums.at[pl.ds(chip, 1)], sem.at[8]))
    for copy in own:
        copy.start()
    for copy in own:
        copy.wait()
    most = recv.at[pl.ds(0, (DEV - 1) * ROWS)]
    few = sums.at[pl.ds(0, DEV // 2 - 1)]
    pltpu.make_async_copy(few, few, sem.at[5]).wait()
    total[...] = jnp.sum(sums[...], axis=0, keepdims=True)
    for s in (0, 1):
        pltpu.make_async_copy(most, most, sem.at[s]).wait()
    swap = pltpu.make_async_remote_copy(
        src_ref=total,
        dst_ref=totals.at[pl.ds(1, 1)],
        send_sem=sem.at[9],
        recv_sem=sem.at[10],
        device_id=partner,
        device_id_type=MESH,
    )
    swap.start()
    keep = pltpu.make_async_copy(total, totals.at[pl.ds(0, 1)], sem.at[11])
    keep.start()
    for ref, s in ((most, 2), (few, 4), (most, 3)):
        pltpu.make_async_copy(ref, ref, sem.at[s]).wait()
    keep.wait()
    swap.wait()


def place_kernel(recv, totals, out, rows, both, placed, sem):
    step_rows = DEV * ROWS * 2 // CHUNKS
    step_lines = GX * TX // CHUNKS
    first = pltpu.make_async_copy(totals, both, sem.at[CHUNKS])
    first.start()
    chunks = []
    for i in range(CHUNKS):
        at = pl.ds(i * step_rows, step_rows)
        chunks.append(pltpu.make_async_copy(recv.at[at], rows.at[at], sem.at[i]))
        chunks[-1].start()
    first.wait()
    level = jnp.sum(both[...]) / COUNT + 1e-6
    scale = 1.0 / jnp.full((8, 128), level, jnp.float32)
    lane = lax.broadcasted_iota(jnp.int32, (8, 128), 1) // TY
    pair = lax.broadcasted_iota(jnp.int32, (8, 128), 0) // 2
    step = (pair - lane) % 4
    for i in range(CHUNKS):
        chunks[i].wait()
        for source in range(i * GX // CHUNKS, (i + 1) * GX // CHUNKS):
            for h in range(2):
                for r in range(ROWS):
                    v = rows[pl.ds((source * GY + 4 * h) * 2 * ROWS + r, 8, stride=ROWS), :]
                    w = v
                    for k in range(1, 4):
                        turned = pltpu.roll(pltpu.roll(v, 2 * k, 0), 128 - TY * k, 1)
                        w = jnp.where(step == k, turned, w)
                    placed[r, source * TX : (source + 1) * TX, h * 128 : (h + 1) * 128] = jnp.log(
                        1.0 + w * scale
                    )
        at = pl.ds(i * step_lines, step_lines)
        pltpu.make_async_copy(placed.at[:, at], out.at[:, at], sem.at[CHUNKS + 1]).start()
    pltpu.make_async_copy(placed, out, sem.at[CHUNKS + 1]).wait()


def on_device(spectra, resample_index, resample_weight, disp_phase, surface_block):
    f32 = jnp.float32
    bf16 = jnp.bfloat16
    hbm = pl.BlockSpec(memory_space=pltpu.HBM)
    table = jnp.asarray(base_table(), bf16)
    recv, totals = pl.pallas_call(
        main_kernel,
        out_shape=(
            jax.ShapeDtypeStruct((DEV * ROWS * 2, 128), f32),
            jax.ShapeDtypeStruct((2, 1, 128), f32),
        ),
        in_specs=[hbm] * 6,
        out_specs=[hbm] * 2,
        scratch_shapes=[
            pltpu.VMEM((2, LINES, NK), bf16),
            pltpu.VMEM((3, RADIX, BLOCK), f32),
            pltpu.VMEM((RADIX, BLOCK), jnp.int32),
            pltpu.VMEM((TX, TY), jnp.int32),
            pltpu.VMEM((RADIX, BLOCK, 2 * BLOCK), bf16),
            pltpu.VMEM((RADIX // 2, NK, 2 * BLOCK), bf16),
            pltpu.VMEM((RADIX, LINES // 2, BLOCK), f32),
            pltpu.VMEM((4, 4, 2, LINES // 2, BLOCK), f32),
            pltpu.VMEM((RADIX, LINES // 2, 2 * BLOCK), bf16),
            pltpu.VMEM((2 * KEEP * BLOCK, 128), f32),
            pltpu.VMEM((1, 1, 128), f32),
            pltpu.VMEM((1, 1, 128), f32),
            pltpu.VMEM((DEV // 2, 1, 128), f32),
            pltpu.SemaphoreType.DMA((13,)),
            pltpu.SemaphoreType.DMA((12,)),
        ],
        compiler_params=pltpu.CompilerParams(
            collective_id=0, has_side_effects=True, vmem_limit_bytes=VMEM_BYTES
        ),
        name="main",
    )(
        spectra,
        resample_index.reshape(RADIX, BLOCK),
        resample_weight.reshape(RADIX, BLOCK),
        disp_phase.reshape(RADIX, BLOCK),
        surface_block,
        table,
    )
    return pl.pallas_call(
        place_kernel,
        out_shape=jax.ShapeDtypeStruct((ROWS, GX * TX, GY * TY), f32),
        in_specs=[hbm] * 2,
        out_specs=hbm,
        scratch_shapes=[
            pltpu.VMEM((DEV * ROWS * 2, 128), f32),
            pltpu.VMEM((2, 1, 128), f32),
            pltpu.VMEM((ROWS, GX * TX, GY * TY), f32),
            pltpu.SemaphoreType.DMA((CHUNKS + 2,)),
        ],
        compiler_params=pltpu.CompilerParams(vmem_limit_bytes=VMEM_BYTES),
        name="place",
    )(recv, totals)

def solution(mesh):
    return jax.shard_map(
        on_device,
        mesh=mesh,
        in_specs=(P("gx", "gy", None), P(), P(), P(), P("gx", "gy")),
        out_specs=P(("gx", "gy"), None, None),
        check_vma=False,
    )
```

```python
import itertools
import math

import jax
import jax.numpy as jnp
import numpy as np
from jax import lax
from jax.experimental import pallas as pl
from jax.experimental.pallas import tpu as pltpu
from jax.sharding import PartitionSpec as P

NK = 2048
BLOCK = 128
KEEP = 5
RADIX = 16
GX = 16
GY = 8
DEV = GX * GY
TX = 8
TY = 32
LINES = TX * TY
ROWS = KEEP * BLOCK // DEV
COUNT = 128 * 256 * KEEP * BLOCK
MESH = pl.DeviceIdType.MESH
VMEM_BYTES = 67043328
CHUNKS = 2
LATE = 1


def base_table():
    c = np.arange(RADIX)[:, None, None]
    b = np.arange(NK // (2 * RADIX))[None, :, None]
    m = np.arange(BLOCK)[None, None, :]
    angle = 2.0 * math.pi * ((m * (RADIX * b + c)) % NK) / NK
    cos, sin = np.cos(angle), np.sin(angle)
    top = np.concatenate([cos, sin], axis=2)
    low = np.concatenate([-sin, cos], axis=2)
    return np.concatenate([top, low], axis=1).astype(np.float32)


def rot(z, k, n):
    re, im = z
    k = k % n
    if k == 0:
        return re, im
    if 4 * k == n:
        return im, -re
    if 2 * k == n:
        return -re, -im
    if 4 * k == 3 * n:
        return -im, re
    if 8 * k == n:
        h = math.sqrt(0.5)
        return h * (re + im), h * (im - re)
    if 8 * k == 3 * n:
        h = math.sqrt(0.5)
        return h * (im - re), -h * (re + im)
    c, s = math.cos(2 * math.pi * k / n), math.sin(2 * math.pi * k / n)
    return c * re + s * im, c * im - s * re


def add(a, b):
    return a[0] + b[0], a[1] + b[1]


def sub(a, b):
    return a[0] - b[0], a[1] - b[1]


def fft4(z):
    a, b = add(z[0], z[2]), sub(z[0], z[2])
    c, d = add(z[1], z[3]), sub(z[1], z[3])
    d = rot(d, 1, 4)
    return [add(a, c), add(b, d), sub(a, c), sub(b, d)]


def hops(o):
    return sum((0, 1, 2, 1)[v] for v in o[:3])


FAR_FIRST = sorted(
    [o for o in itertools.product(range(4), range(4), range(4), range(2)) if any(o)],
    key=lambda o: (-hops(o), o),
)


def first_link(o):
    for d in (2, 1, 0):
        if o[d]:
            return 3 * d + o[d]
    return 0


def woven(offsets):
    lanes = {}
    for o in offsets:
        lanes.setdefault(first_link(o), []).append(o)
    keyed = [
        ((i + 0.5) / len(lane), link, o) for link, lane in lanes.items() for i, o in enumerate(lane)
    ]
    return [o for _, _, o in sorted(keyed)]


OFFSETS = woven(FAR_FIRST)


def main_kernel(
    spectra, index, weight, phase, surface, table, recv, totals,
    both, params, idx, surf, tab, hits, x, mid, y, msg, part, total, sums, load, sem,
):
    f32, bf16 = jnp.float32, jnp.bfloat16
    half = LINES // 2
    gx, gy = lax.axis_index("gx"), lax.axis_index("gy")
    me = gx * GY + gy
    zs = [(gx // 4 + d) % 4 for d in range(4)]
    ys = [(gx % 4 + d) % 4 for d in range(4)]
    xs = [(gy // 2 + d) % 4 for d in range(4)]
    cs = [(gy % 2 + d) % 2 for d in range(2)]
    zy = [[z * 4 + v for v in ys] for z in zs]
    xc = [[v * 2 + c for c in cs] for v in xs]
    peers, greeted = (
        [(zy[o[0]][o[1]], xc[o[2]][o[3]]) for o in order] for order in (OFFSETS, FAR_FIRST)
    )
    alike = [to for o, to in zip(OFFSETS, peers) if o[3] == 0]
    partner = (zy[0][0], xc[0][1])
    chip = gx * (GY // 2) + gy // 2
    barrier = pltpu.get_barrier_semaphore()

    small = [
        pltpu.make_async_copy(index, idx, load.at[0]),
        pltpu.make_async_copy(weight, params.at[0], load.at[1]),
        pltpu.make_async_copy(phase, params.at[1], load.at[2]),
        pltpu.make_async_copy(surface, surf, load.at[3]),
    ]
    tiles = [
        pltpu.make_async_copy(
            spectra.at[2 * p + q], both.at[q, pl.ds(p * TY, TY)], load.at[4 + 4 * q + p]
        )
        for q in range(2)
        for p in range(4)
    ]
    big = pltpu.make_async_copy(table, tab, load.at[12])
    for copy in small + tiles + [big]:
        copy.start()
    for to in greeted:
        pl.semaphore_signal(barrier, inc=1, device_id=to, device_id_type=MESH)
    for copy in small:
        copy.wait()
    cosp = jnp.cos(params[1])
    sinp = jnp.sin(params[1])
    params[1] = cosp
    params[2] = sinp
    tops = [
        jnp.concatenate([surf[2 * p + q : 2 * p + q + 1, :] for p in range(4)], axis=1)
        for q in range(2)
    ]
    row = lax.broadcasted_iota(jnp.int32, (BLOCK, 2 * BLOCK), 0).astype(jnp.int16)
    one = jnp.ones((BLOCK, 2 * BLOCK), bf16)
    zero = jnp.zeros((BLOCK, 2 * BLOCK), bf16)
    nt = (((1,), (1,)), ((), ()))

    def shift(q):
        for copy in tiles[4 * q : 4 * q + 4]:
            copy.wait()
        lines = both[q, :half, :]
        both[q, half:, :] = jnp.concatenate([lines[:, 1:], lines[:, :1]], axis=1)

    def compute(q, acc, meanwhile=None):
        for n in range(4):
            if n == LATE and meanwhile is not None:
                meanwhile()
            for e in range(2):
                if q == 0:
                    pick = jnp.concatenate(
                        [idx[n + 8 * e + 4 * h : n + 8 * e + 4 * h + 1, :] for h in range(2)], axis=1
                    ).astype(jnp.int16)
                    for k in range(NK // 128):
                        seen = row + jnp.int16(128 * k) == pick
                        hits[2 * n + e, k * 128 : (k + 1) * 128, :] = jnp.where(seen, one, zero)
                pair = jnp.dot(both[q], hits[2 * n + e], preferred_element_type=f32)
                for h in range(2):
                    at = n + 8 * e + 4 * h
                    lane = slice(h * BLOCK, (h + 1) * BLOCK)
                    w = params[0, at : at + 1, :]
                    x[at] = (1.0 - w) * pair[:half, lane] + w * pair[half:, lane]
            for g in range(half // 16):
                rows = slice(16 * g, 16 * g + 16)
                z = []
                for m in range(4):
                    at = n + 4 * m
                    v = x[at, rows, :]
                    z.append(
                        [
                            (v * params[1 + o, at : at + 1, :]).astype(bf16).astype(f32)
                            for o in range(2)
                        ]
                    )
                for c, value in enumerate(fft4(z)):
                    for o, half_value in enumerate(rot(value, n * c, RADIX)):
                        mid[n, c, o, rows, :] = half_value
        if q == 0:
            big.wait()
        for low in range(4):
            for g in range(half // 16):
                rows = slice(16 * g, 16 * g + 16)
                z = [[mid[n, low, o, rows, :] for o in range(2)] for n in range(4)]
                for high, value in enumerate(fft4(z)):
                    for o in range(2):
                        y[low + 4 * high, rows, o * BLOCK : (o + 1) * BLOCK] = value[o].astype(bf16)
            for c in range(low, RADIX, 4):
                depth = lax.dot_general(tab[c], y[c], nt, preferred_element_type=f32)
                power = depth[:64] * depth[:64] + depth[64:] * depth[64:]
                tile = [power[8 * b : 8 * b + 8] for b in range(8)]
                for k in range(KEEP):
                    kept = tile[k]
                    for s in range(1, 4):
                        kept = jnp.where(tops[q] == s, tile[k + s], kept)
                    acc = acc + kept
                    msg[pl.ds((q * KEEP + k) * BLOCK + c, 8, stride=RADIX), :] = kept
        return acc

    def slab(q, dest):
        return msg.at[pl.ds(q * KEEP * BLOCK + ROWS * dest, ROWS)]

    def landing(q):
        return recv.at[pl.ds((2 * me + q) * ROWS, ROWS)]

    def send(q, among):
        for to in among:
            pltpu.make_async_remote_copy(
                src_ref=slab(q, to[0] * GY + to[1]),
                dst_ref=landing(q),
                send_sem=sem.at[2 * q],
                recv_sem=sem.at[2 * q + 1],
                device_id=to,
                device_id_type=MESH,
            ).start()

    shift(0)
    acc = compute(0, jnp.zeros((8, 128), f32))
    def release():
        pl.semaphore_wait(barrier, DEV - 1)
        send(0, peers)

    shift(1)
    acc = compute(1, acc, release)
    part[...] = jnp.sum(acc, axis=0, keepdims=True).reshape(1, 1, 128)
    for to in alike:
        pltpu.make_async_remote_copy(
            src_ref=part,
            dst_ref=sums.at[pl.ds(chip, 1)],
            send_sem=sem.at[4],
            recv_sem=sem.at[5],
            device_id=to,
            device_id_type=MESH,
        ).start()
    send(1, peers)
    own = [pltpu.make_async_copy(slab(q, me), landing(q), sem.at[6 + q]) for q in range(2)]
    own.append(pltpu.make_async_copy(part, sums.at[pl.ds(chip, 1)], sem.at[8]))
    for copy in own:
        copy.start()
    for copy in own:
        copy.wait()
    most = recv.at[pl.ds(0, (DEV - 1) * ROWS)]
    few = sums.at[pl.ds(0, DEV // 2 - 1)]
    pltpu.make_async_copy(few, few, sem.at[5]).wait()
    total[...] = jnp.sum(sums[...], axis=0, keepdims=True)
    for s in (0, 1):
        pltpu.make_async_copy(most, most, sem.at[s]).wait()
    swap = pltpu.make_async_remote_copy(
        src_ref=total,
        dst_ref=totals.at[pl.ds(1, 1)],
        send_sem=sem.at[9],
        recv_sem=sem.at[10],
        device_id=partner,
        device_id_type=MESH,
    )
    swap.start()
    keep = pltpu.make_async_copy(total, totals.at[pl.ds(0, 1)], sem.at[11])
    keep.start()
    for ref, s in ((most, 2), (few, 4), (most, 3)):
        pltpu.make_async_copy(ref, ref, sem.at[s]).wait()
    keep.wait()
    swap.wait()


def place_kernel(recv, totals, out, rows, both, placed, sem):
    step_rows = DEV * ROWS * 2 // CHUNKS
    step_lines = GX * TX // CHUNKS
    first = pltpu.make_async_copy(totals, both, sem.at[CHUNKS])
    first.start()
    chunks = []
    for i in range(CHUNKS):
        at = pl.ds(i * step_rows, step_rows)
        chunks.append(pltpu.make_async_copy(recv.at[at], rows.at[at], sem.at[i]))
        chunks[-1].start()
    first.wait()
    level = jnp.sum(both[...]) / COUNT + 1e-6
    scale = 1.0 / jnp.full((8, 128), level, jnp.float32)
    lane = lax.broadcasted_iota(jnp.int32, (8, 128), 1) // TY
    pair = lax.broadcasted_iota(jnp.int32, (8, 128), 0) // 2
    step = (pair - lane) % 4
    for i in range(CHUNKS):
        chunks[i].wait()
        for source in range(i * GX // CHUNKS, (i + 1) * GX // CHUNKS):
            for h in range(2):
                for r in range(ROWS):
                    v = rows[pl.ds((source * GY + 4 * h) * 2 * ROWS + r, 8, stride=ROWS), :]
                    w = v
                    for k in range(1, 4):
                        turned = pltpu.roll(pltpu.roll(v, 2 * k, 0), 128 - TY * k, 1)
                        w = jnp.where(step == k, turned, w)
                    placed[r, source * TX : (source + 1) * TX, h * 128 : (h + 1) * 128] = jnp.log(
                        1.0 + w * scale
                    )
        at = pl.ds(i * step_lines, step_lines)
        pltpu.make_async_copy(placed.at[:, at], out.at[:, at], sem.at[CHUNKS + 1]).start()
    pltpu.make_async_copy(placed, out, sem.at[CHUNKS + 1]).wait()


def on_device(spectra, resample_index, resample_weight, disp_phase, surface_block):
    f32 = jnp.float32
    bf16 = jnp.bfloat16
    hbm = pl.BlockSpec(memory_space=pltpu.HBM)
    table = jnp.asarray(base_table(), bf16)
    recv, totals = pl.pallas_call(
        main_kernel,
        out_shape=(
            jax.ShapeDtypeStruct((DEV * ROWS * 2, 128), f32),
            jax.ShapeDtypeStruct((2, 1, 128), f32),
        ),
        in_specs=[hbm] * 6,
        out_specs=[hbm] * 2,
        scratch_shapes=[
            pltpu.VMEM((2, LINES, NK), bf16),
            pltpu.VMEM((3, RADIX, BLOCK), f32),
            pltpu.VMEM((RADIX, BLOCK), jnp.int32),
            pltpu.VMEM((TX, TY), jnp.int32),
            pltpu.VMEM((RADIX, BLOCK, 2 * BLOCK), bf16),
            pltpu.VMEM((RADIX // 2, NK, 2 * BLOCK), bf16),
            pltpu.VMEM((RADIX, LINES // 2, BLOCK), f32),
            pltpu.VMEM((4, 4, 2, LINES // 2, BLOCK), f32),
            pltpu.VMEM((RADIX, LINES // 2, 2 * BLOCK), bf16),
            pltpu.VMEM((2 * KEEP * BLOCK, 128), f32),
            pltpu.VMEM((1, 1, 128), f32),
            pltpu.VMEM((1, 1, 128), f32),
            pltpu.VMEM((DEV // 2, 1, 128), f32),
            pltpu.SemaphoreType.DMA((13,)),
            pltpu.SemaphoreType.DMA((12,)),
        ],
        compiler_params=pltpu.CompilerParams(
            collective_id=0, has_side_effects=True, vmem_limit_bytes=VMEM_BYTES
        ),
        name="main",
    )(
        spectra,
        resample_index.reshape(RADIX, BLOCK),
        resample_weight.reshape(RADIX, BLOCK),
        disp_phase.reshape(RADIX, BLOCK),
        surface_block,
        table,
    )
    return pl.pallas_call(
        place_kernel,
        out_shape=jax.ShapeDtypeStruct((ROWS, GX * TX, GY * TY), f32),
        in_specs=[hbm] * 2,
        out_specs=hbm,
        scratch_shapes=[
            pltpu.VMEM((DEV * ROWS * 2, 128), f32),
            pltpu.VMEM((2, 1, 128), f32),
            pltpu.VMEM((ROWS, GX * TX, GY * TY), f32),
            pltpu.SemaphoreType.DMA((CHUNKS + 2,)),
        ],
        compiler_params=pltpu.CompilerParams(vmem_limit_bytes=VMEM_BYTES),
        name="place",
    )(recv, totals)

def solution(mesh):
    return jax.shard_map(
        on_device,
        mesh=mesh,
        in_specs=(P("gx", "gy", None), P(), P(), P(), P("gx", "gy")),
        out_specs=P(("gx", "gy"), None, None),
        check_vma=False,
    )
```

```python
import itertools
import math

import jax
import jax.numpy as jnp
import numpy as np
from jax import lax
from jax.experimental import pallas as pl
from jax.experimental.pallas import tpu as pltpu
from jax.sharding import PartitionSpec as P

NK = 2048
BLOCK = 128
KEEP = 5
RADIX = 16
GX = 16
GY = 8
DEV = GX * GY
TX = 8
TY = 32
LINES = TX * TY
ROWS = KEEP * BLOCK // DEV
COUNT = 128 * 256 * KEEP * BLOCK
MESH = pl.DeviceIdType.MESH
VMEM_BYTES = 67043328
CHUNKS = 2


def base_table():
    c = np.arange(RADIX)[:, None, None]
    b = np.arange(NK // (2 * RADIX))[None, :, None]
    m = np.arange(BLOCK)[None, None, :]
    angle = 2.0 * math.pi * ((m * (RADIX * b + c)) % NK) / NK
    cos, sin = np.cos(angle), np.sin(angle)
    top = np.concatenate([cos, sin], axis=2)
    low = np.concatenate([-sin, cos], axis=2)
    return np.concatenate([top, low], axis=1).astype(np.float32)


def rot(z, k, n):
    re, im = z
    k = k % n
    if k == 0:
        return re, im
    if 4 * k == n:
        return im, -re
    if 2 * k == n:
        return -re, -im
    if 4 * k == 3 * n:
        return -im, re
    if 8 * k == n:
        h = math.sqrt(0.5)
        return h * (re + im), h * (im - re)
    if 8 * k == 3 * n:
        h = math.sqrt(0.5)
        return h * (im - re), -h * (re + im)
    c, s = math.cos(2 * math.pi * k / n), math.sin(2 * math.pi * k / n)
    return c * re + s * im, c * im - s * re


def add(a, b):
    return a[0] + b[0], a[1] + b[1]


def sub(a, b):
    return a[0] - b[0], a[1] - b[1]


def fft4(z):
    a, b = add(z[0], z[2]), sub(z[0], z[2])
    c, d = add(z[1], z[3]), sub(z[1], z[3])
    d = rot(d, 1, 4)
    return [add(a, c), add(b, d), sub(a, c), sub(b, d)]


def hops(o):
    return sum((0, 1, 2, 1)[v] for v in o[:3])


FAR_FIRST = sorted(
    [o for o in itertools.product(range(4), range(4), range(4), range(2)) if any(o)],
    key=lambda o: (-hops(o), o),
)


def first_link(o):
    for d in (2, 1, 0):
        if o[d]:
            return 3 * d + o[d]
    return 0


def woven(offsets):
    lanes = {}
    for o in offsets:
        lanes.setdefault(first_link(o), []).append(o)
    keyed = [
        ((i + 0.5) / len(lane), link, o) for link, lane in lanes.items() for i, o in enumerate(lane)
    ]
    return [o for _, _, o in sorted(keyed)]


OFFSETS = woven(FAR_FIRST)


def main_kernel(
    spectra, index, weight, phase, surface, table, recv, totals,
    both, params, idx, surf, tab, hits, x, mid, y, msg, part, total, sums, load, sem,
):
    f32, bf16 = jnp.float32, jnp.bfloat16
    half = LINES // 2
    gx, gy = lax.axis_index("gx"), lax.axis_index("gy")
    me = gx * GY + gy
    zs = [(gx // 4 + d) % 4 for d in range(4)]
    ys = [(gx % 4 + d) % 4 for d in range(4)]
    xs = [(gy // 2 + d) % 4 for d in range(4)]
    cs = [(gy % 2 + d) % 2 for d in range(2)]
    zy = [[z * 4 + v for v in ys] for z in zs]
    xc = [[v * 2 + c for c in cs] for v in xs]
    peers, greeted = (
        [(zy[o[0]][o[1]], xc[o[2]][o[3]]) for o in order] for order in (OFFSETS, FAR_FIRST)
    )
    alike = [to for o, to in zip(OFFSETS, peers) if o[3] == 0]
    partner = (zy[0][0], xc[0][1])
    chip = gx * (GY // 2) + gy // 2
    barrier = pltpu.get_barrier_semaphore()

    small = [
        pltpu.make_async_copy(index, idx, load.at[0]),
        pltpu.make_async_copy(weight, params.at[0], load.at[1]),
        pltpu.make_async_copy(phase, params.at[1], load.at[2]),
        pltpu.make_async_copy(surface, surf, load.at[3]),
    ]
    tiles = [
        pltpu.make_async_copy(
            spectra.at[2 * p + q], both.at[q, pl.ds(p * TY, TY)], load.at[4 + 4 * q + p]
        )
        for q in range(2)
        for p in range(4)
    ]
    big = pltpu.make_async_copy(table, tab, load.at[12])
    for copy in small + tiles + [big]:
        copy.start()
    for to in greeted:
        pl.semaphore_signal(barrier, inc=1, device_id=to, device_id_type=MESH)
    for copy in small:
        copy.wait()
    cosp = jnp.cos(params[1])
    sinp = jnp.sin(params[1])
    params[1] = cosp
    params[2] = sinp
    tops = [
        jnp.concatenate([surf[2 * p + q : 2 * p + q + 1, :] for p in range(4)], axis=1)
        for q in range(2)
    ]
    row = lax.broadcasted_iota(jnp.int32, (BLOCK, 2 * BLOCK), 0).astype(jnp.int16)
    one = jnp.ones((BLOCK, 2 * BLOCK), bf16)
    zero = jnp.zeros((BLOCK, 2 * BLOCK), bf16)
    nt = (((1,), (1,)), ((), ()))

    def shift(q):
        for copy in tiles[4 * q : 4 * q + 4]:
            copy.wait()
        lines = both[q, :half, :]
        both[q, half:, :] = jnp.concatenate([lines[:, 1:], lines[:, :1]], axis=1)

    def compute(q, acc):
        for n in range(4):
            for e in range(2):
                if q == 0:
                    pick = jnp.concatenate(
                        [idx[n + 8 * e + 4 * h : n + 8 * e + 4 * h + 1, :] for h in range(2)], axis=1
                    ).astype(jnp.int16)
                    for k in range(NK // 128):
                        seen = row + jnp.int16(128 * k) == pick
                        hits[2 * n + e, k * 128 : (k + 1) * 128, :] = jnp.where(seen, one, zero)
                pair = jnp.dot(both[q], hits[2 * n + e], preferred_element_type=f32)
                for h in range(2):
                    at = n + 8 * e + 4 * h
                    lane = slice(h * BLOCK, (h + 1) * BLOCK)
                    w = params[0, at : at + 1, :]
                    x[at] = (1.0 - w) * pair[:half, lane] + w * pair[half:, lane]
            for g in range(half // 16):
                rows = slice(16 * g, 16 * g + 16)
                z = []
                for m in range(4):
                    at = n + 4 * m
                    v = x[at, rows, :]
                    z.append(
                        [
                            (v * params[1 + o, at : at + 1, :]).astype(bf16).astype(f32)
                            for o in range(2)
                        ]
                    )
                for c, value in enumerate(fft4(z)):
                    for o, half_value in enumerate(rot(value, n * c, RADIX)):
                        mid[n, c, o, rows, :] = half_value
        if q == 0:
            big.wait()
        for low in range(4):
            for g in range(half // 16):
                rows = slice(16 * g, 16 * g + 16)
                z = [[mid[n, low, o, rows, :] for o in range(2)] for n in range(4)]
                for high, value in enumerate(fft4(z)):
                    for o in range(2):
                        y[low + 4 * high, rows, o * BLOCK : (o + 1) * BLOCK] = value[o].astype(bf16)
            for c in range(low, RADIX, 4):
                depth = lax.dot_general(tab[c], y[c], nt, preferred_element_type=f32)
                power = depth[:64] * depth[:64] + depth[64:] * depth[64:]
                tile = [power[8 * b : 8 * b + 8] for b in range(8)]
                for k in range(KEEP):
                    kept = tile[k]
                    for s in range(1, 4):
                        kept = jnp.where(tops[q] == s, tile[k + s], kept)
                    acc = acc + kept
                    msg[pl.ds((q * KEEP + k) * BLOCK + c, 8, stride=RADIX), :] = kept
        return acc

    def slab(q, dest):
        return msg.at[pl.ds(q * KEEP * BLOCK + ROWS * dest, ROWS)]

    def landing(q):
        return recv.at[pl.ds((2 * me + q) * ROWS, ROWS)]

    def send(q, among):
        for to in among:
            pltpu.make_async_remote_copy(
                src_ref=slab(q, to[0] * GY + to[1]),
                dst_ref=landing(q),
                send_sem=sem.at[2 * q],
                recv_sem=sem.at[2 * q + 1],
                device_id=to,
                device_id_type=MESH,
            ).start()

    shift(0)
    acc = compute(0, jnp.zeros((8, 128), f32))
    pl.semaphore_wait(barrier, DEV - 1)
    send(0, peers[::-1])
    shift(1)
    acc = compute(1, acc)
    part[...] = jnp.sum(acc, axis=0, keepdims=True).reshape(1, 1, 128)
    for to in alike:
        pltpu.make_async_remote_copy(
            src_ref=part,
            dst_ref=sums.at[pl.ds(chip, 1)],
            send_sem=sem.at[4],
            recv_sem=sem.at[5],
            device_id=to,
            device_id_type=MESH,
        ).start()
    send(1, peers)
    own = [pltpu.make_async_copy(slab(q, me), landing(q), sem.at[6 + q]) for q in range(2)]
    own.append(pltpu.make_async_copy(part, sums.at[pl.ds(chip, 1)], sem.at[8]))
    for copy in own:
        copy.start()
    for copy in own:
        copy.wait()
    most = recv.at[pl.ds(0, (DEV - 1) * ROWS)]
    few = sums.at[pl.ds(0, DEV // 2 - 1)]
    pltpu.make_async_copy(few, few, sem.at[5]).wait()
    total[...] = jnp.sum(sums[...], axis=0, keepdims=True)
    for s in (0, 1):
        pltpu.make_async_copy(most, most, sem.at[s]).wait()
    swap = pltpu.make_async_remote_copy(
        src_ref=total,
        dst_ref=totals.at[pl.ds(1, 1)],
        send_sem=sem.at[9],
        recv_sem=sem.at[10],
        device_id=partner,
        device_id_type=MESH,
    )
    swap.start()
    keep = pltpu.make_async_copy(total, totals.at[pl.ds(0, 1)], sem.at[11])
    keep.start()
    for ref, s in ((most, 2), (few, 4), (most, 3)):
        pltpu.make_async_copy(ref, ref, sem.at[s]).wait()
    keep.wait()
    swap.wait()


def place_kernel(recv, totals, out, rows, both, placed, sem):
    step_rows = DEV * ROWS * 2 // CHUNKS
    step_lines = GX * TX // CHUNKS
    first = pltpu.make_async_copy(totals, both, sem.at[CHUNKS])
    first.start()
    chunks = []
    for i in range(CHUNKS):
        at = pl.ds(i * step_rows, step_rows)
        chunks.append(pltpu.make_async_copy(recv.at[at], rows.at[at], sem.at[i]))
        chunks[-1].start()
    first.wait()
    level = jnp.sum(both[...]) / COUNT + 1e-6
    scale = 1.0 / jnp.full((8, 128), level, jnp.float32)
    lane = lax.broadcasted_iota(jnp.int32, (8, 128), 1) // TY
    pair = lax.broadcasted_iota(jnp.int32, (8, 128), 0) // 2
    step = (pair - lane) % 4
    for i in range(CHUNKS):
        chunks[i].wait()
        for source in range(i * GX // CHUNKS, (i + 1) * GX // CHUNKS):
            for h in range(2):
                for r in range(ROWS):
                    v = rows[pl.ds((source * GY + 4 * h) * 2 * ROWS + r, 8, stride=ROWS), :]
                    w = v
                    for k in range(1, 4):
                        turned = pltpu.roll(pltpu.roll(v, 2 * k, 0), 128 - TY * k, 1)
                        w = jnp.where(step == k, turned, w)
                    placed[r, source * TX : (source + 1) * TX, h * 128 : (h + 1) * 128] = jnp.log(
                        1.0 + w * scale
                    )
        at = pl.ds(i * step_lines, step_lines)
        pltpu.make_async_copy(placed.at[:, at], out.at[:, at], sem.at[CHUNKS + 1]).start()
    pltpu.make_async_copy(placed, out, sem.at[CHUNKS + 1]).wait()


def on_device(spectra, resample_index, resample_weight, disp_phase, surface_block):
    f32 = jnp.float32
    bf16 = jnp.bfloat16
    hbm = pl.BlockSpec(memory_space=pltpu.HBM)
    table = jnp.asarray(base_table(), bf16)
    recv, totals = pl.pallas_call(
        main_kernel,
        out_shape=(
            jax.ShapeDtypeStruct((DEV * ROWS * 2, 128), f32),
            jax.ShapeDtypeStruct((2, 1, 128), f32),
        ),
        in_specs=[hbm] * 6,
        out_specs=[hbm] * 2,
        scratch_shapes=[
            pltpu.VMEM((2, LINES, NK), bf16),
            pltpu.VMEM((3, RADIX, BLOCK), f32),
            pltpu.VMEM((RADIX, BLOCK), jnp.int32),
            pltpu.VMEM((TX, TY), jnp.int32),
            pltpu.VMEM((RADIX, BLOCK, 2 * BLOCK), bf16),
            pltpu.VMEM((RADIX // 2, NK, 2 * BLOCK), bf16),
            pltpu.VMEM((RADIX, LINES // 2, BLOCK), f32),
            pltpu.VMEM((4, 4, 2, LINES // 2, BLOCK), f32),
            pltpu.VMEM((RADIX, LINES // 2, 2 * BLOCK), bf16),
            pltpu.VMEM((2 * KEEP * BLOCK, 128), f32),
            pltpu.VMEM((1, 1, 128), f32),
            pltpu.VMEM((1, 1, 128), f32),
            pltpu.VMEM((DEV // 2, 1, 128), f32),
            pltpu.SemaphoreType.DMA((13,)),
            pltpu.SemaphoreType.DMA((12,)),
        ],
        compiler_params=pltpu.CompilerParams(
            collective_id=0, has_side_effects=True, vmem_limit_bytes=VMEM_BYTES
        ),
        name="main",
    )(
        spectra,
        resample_index.reshape(RADIX, BLOCK),
        resample_weight.reshape(RADIX, BLOCK),
        disp_phase.reshape(RADIX, BLOCK),
        surface_block,
        table,
    )
    return pl.pallas_call(
        place_kernel,
        out_shape=jax.ShapeDtypeStruct((ROWS, GX * TX, GY * TY), f32),
        in_specs=[hbm] * 2,
        out_specs=hbm,
        scratch_shapes=[
            pltpu.VMEM((DEV * ROWS * 2, 128), f32),
            pltpu.VMEM((2, 1, 128), f32),
            pltpu.VMEM((ROWS, GX * TX, GY * TY), f32),
            pltpu.SemaphoreType.DMA((CHUNKS + 2,)),
        ],
        compiler_params=pltpu.CompilerParams(vmem_limit_bytes=VMEM_BYTES),
        name="place",
    )(recv, totals)

def solution(mesh):
    return jax.shard_map(
        on_device,
        mesh=mesh,
        in_specs=(P("gx", "gy", None), P(), P(), P(), P("gx", "gy")),
        out_specs=P(("gx", "gy"), None, None),
        check_vma=False,
    )
```

```python
import itertools
import math

import jax
import jax.numpy as jnp
import numpy as np
from jax import lax
from jax.experimental import pallas as pl
from jax.experimental.pallas import tpu as pltpu
from jax.sharding import PartitionSpec as P

NK = 2048
BLOCK = 128
KEEP = 5
RADIX = 16
GX = 16
GY = 8
DEV = GX * GY
TX = 8
TY = 32
LINES = TX * TY
ROWS = KEEP * BLOCK // DEV
COUNT = 128 * 256 * KEEP * BLOCK
MESH = pl.DeviceIdType.MESH
VMEM_BYTES = 67043328
CHUNKS = 2


def base_table():
    c = np.arange(RADIX)[:, None, None]
    b = np.arange(NK // (2 * RADIX))[None, :, None]
    m = np.arange(BLOCK)[None, None, :]
    angle = 2.0 * math.pi * ((m * (RADIX * b + c)) % NK) / NK
    cos, sin = np.cos(angle), np.sin(angle)
    top = np.concatenate([cos, sin], axis=2)
    low = np.concatenate([-sin, cos], axis=2)
    return np.concatenate([top, low], axis=1).astype(np.float32)


def rot(z, k, n):
    re, im = z
    k = k % n
    if k == 0:
        return re, im
    if 4 * k == n:
        return im, -re
    if 2 * k == n:
        return -re, -im
    if 4 * k == 3 * n:
        return -im, re
    if 8 * k == n:
        h = math.sqrt(0.5)
        return h * (re + im), h * (im - re)
    if 8 * k == 3 * n:
        h = math.sqrt(0.5)
        return h * (im - re), -h * (re + im)
    c, s = math.cos(2 * math.pi * k / n), math.sin(2 * math.pi * k / n)
    return c * re + s * im, c * im - s * re


def add(a, b):
    return a[0] + b[0], a[1] + b[1]


def sub(a, b):
    return a[0] - b[0], a[1] - b[1]


def fft4(z):
    a, b = add(z[0], z[2]), sub(z[0], z[2])
    c, d = add(z[1], z[3]), sub(z[1], z[3])
    d = rot(d, 1, 4)
    return [add(a, c), add(b, d), sub(a, c), sub(b, d)]


def hops(o):
    return sum((0, 1, 2, 1)[v] for v in o[:3])


FAR_FIRST = sorted(
    [o for o in itertools.product(range(4), range(4), range(4), range(2)) if any(o)],
    key=lambda o: (-hops(o), o),
)


def first_link(o):
    for d in (2, 1, 0):
        if o[d]:
            return 3 * d + o[d]
    return 0


def woven(offsets):
    lanes = {}
    for o in offsets:
        lanes.setdefault(first_link(o), []).append(o)
    keyed = [
        ((i + 0.5) / len(lane), link, o) for link, lane in lanes.items() for i, o in enumerate(lane)
    ]
    return [o for _, _, o in sorted(keyed)]


OFFSETS = woven(FAR_FIRST)


def main_kernel(
    spectra, index, weight, phase, surface, table, recv, totals,
    both, params, idx, surf, tab, hits, x, mid, y, msg, part, total, sums, load, sem,
):
    f32, bf16 = jnp.float32, jnp.bfloat16
    half = LINES // 2
    gx, gy = lax.axis_index("gx"), lax.axis_index("gy")
    me = gx * GY + gy
    zs = [(gx // 4 + d) % 4 for d in range(4)]
    ys = [(gx % 4 + d) % 4 for d in range(4)]
    xs = [(gy // 2 + d) % 4 for d in range(4)]
    cs = [(gy % 2 + d) % 2 for d in range(2)]
    zy = [[z * 4 + v for v in ys] for z in zs]
    xc = [[v * 2 + c for c in cs] for v in xs]
    peers, greeted = (
        [(zy[o[0]][o[1]], xc[o[2]][o[3]]) for o in order] for order in (OFFSETS, FAR_FIRST)
    )
    alike = [to for o, to in zip(OFFSETS, peers) if o[3] == 0]
    partner = (zy[0][0], xc[0][1])
    chip = gx * (GY // 2) + gy // 2
    barrier = pltpu.get_barrier_semaphore()

    small = [
        pltpu.make_async_copy(index, idx, load.at[0]),
        pltpu.make_async_copy(weight, params.at[0], load.at[1]),
        pltpu.make_async_copy(phase, params.at[1], load.at[2]),
        pltpu.make_async_copy(surface, surf, load.at[3]),
    ]
    tiles = [
        pltpu.make_async_copy(
            spectra.at[2 * p + q], both.at[q, pl.ds(p * TY, TY)], load.at[4 + 4 * q + p]
        )
        for q in range(2)
        for p in range(4)
    ]
    big = pltpu.make_async_copy(table, tab, load.at[12])
    for copy in small + tiles + [big]:
        copy.start()
    for to in greeted:
        pl.semaphore_signal(barrier, inc=1, device_id=to, device_id_type=MESH)
    for copy in small:
        copy.wait()
    cosp = jnp.cos(params[1])
    sinp = jnp.sin(params[1])
    params[1] = cosp
    params[2] = sinp
    tops = [
        jnp.concatenate([surf[2 * p + q : 2 * p + q + 1, :] for p in range(4)], axis=1)
        for q in range(2)
    ]
    row = lax.broadcasted_iota(jnp.int32, (BLOCK, 2 * BLOCK), 0).astype(jnp.int16)
    one = jnp.ones((BLOCK, 2 * BLOCK), bf16)
    zero = jnp.zeros((BLOCK, 2 * BLOCK), bf16)
    nt = (((1,), (1,)), ((), ()))

    def shift(q):
        for copy in tiles[4 * q : 4 * q + 4]:
            copy.wait()
        lines = both[q, :half, :]
        both[q, half:, :] = jnp.concatenate([lines[:, 1:], lines[:, :1]], axis=1)

    def compute(q, acc):
        for n in range(4):
            for e in range(2):
                if q == 0:
                    pick = jnp.concatenate(
                        [idx[n + 8 * e + 4 * h : n + 8 * e + 4 * h + 1, :] for h in range(2)], axis=1
                    ).astype(jnp.int16)
                    for k in range(NK // 128):
                        seen = row + jnp.int16(128 * k) == pick
                        hits[2 * n + e, k * 128 : (k + 1) * 128, :] = jnp.where(seen, one, zero)
                pair = jnp.dot(both[q], hits[2 * n + e], preferred_element_type=f32)
                for h in range(2):
                    at = n + 8 * e + 4 * h
                    lane = slice(h * BLOCK, (h + 1) * BLOCK)
                    w = params[0, at : at + 1, :]
                    x[at] = (1.0 - w) * pair[:half, lane] + w * pair[half:, lane]
            for g in range(half // 16):
                rows = slice(16 * g, 16 * g + 16)
                z = []
                for m in range(4):
                    at = n + 4 * m
                    v = x[at, rows, :]
                    z.append(
                        [
                            (v * params[1 + o, at : at + 1, :]).astype(bf16).astype(f32)
                            for o in range(2)
                        ]
                    )
                for c, value in enumerate(fft4(z)):
                    for o, half_value in enumerate(rot(value, n * c, RADIX)):
                        mid[n, c, o, rows, :] = half_value
        if q == 0:
            big.wait()
        for low in range(4):
            for g in range(half // 16):
                rows = slice(16 * g, 16 * g + 16)
                z = [[mid[n, low, o, rows, :] for o in range(2)] for n in range(4)]
                for high, value in enumerate(fft4(z)):
                    for o in range(2):
                        y[low + 4 * high, rows, o * BLOCK : (o + 1) * BLOCK] = value[o].astype(bf16)
            for c in range(low, RADIX, 4):
                depth = lax.dot_general(tab[c], y[c], nt, preferred_element_type=f32)
                power = depth[:64] * depth[:64] + depth[64:] * depth[64:]
                tile = [power[8 * b : 8 * b + 8] for b in range(8)]
                for k in range(KEEP):
                    kept = tile[k]
                    for s in range(1, 4):
                        kept = jnp.where(tops[q] == s, tile[k + s], kept)
                    acc = acc + kept
                    msg[pl.ds((q * KEEP + k) * BLOCK + c, 8, stride=RADIX), :] = kept
        return acc

    def slab(q, dest):
        return msg.at[pl.ds(q * KEEP * BLOCK + ROWS * dest, ROWS)]

    def landing(q):
        return recv.at[pl.ds((2 * me + q) * ROWS, ROWS)]

    def send(q, among):
        for to in among:
            pltpu.make_async_remote_copy(
                src_ref=slab(q, to[0] * GY + to[1]),
                dst_ref=landing(q),
                send_sem=sem.at[2 * q],
                recv_sem=sem.at[2 * q + 1],
                device_id=to,
                device_id_type=MESH,
            ).start()

    shift(0)
    acc = compute(0, jnp.zeros((8, 128), f32))
    pl.semaphore_wait(barrier, DEV - 1)
    send(0, peers)
    shift(1)
    acc = compute(1, acc)
    part[...] = jnp.sum(acc, axis=0, keepdims=True).reshape(1, 1, 128)
    for to in alike:
        pltpu.make_async_remote_copy(
            src_ref=part,
            dst_ref=sums.at[pl.ds(chip, 1)],
            send_sem=sem.at[4],
            recv_sem=sem.at[5],
            device_id=to,
            device_id_type=MESH,
        ).start()
    send(1, peers)
    own = [pltpu.make_async_copy(slab(q, me), landing(q), sem.at[6 + q]) for q in range(2)]
    own.append(pltpu.make_async_copy(part, sums.at[pl.ds(chip, 1)], sem.at[8]))
    for copy in own:
        copy.start()
    for copy in own:
        copy.wait()
    most = recv.at[pl.ds(0, (DEV - 1) * ROWS)]
    few = sums.at[pl.ds(0, DEV // 2 - 1)]
    pltpu.make_async_copy(few, few, sem.at[5]).wait()
    total[...] = jnp.sum(sums[...], axis=0, keepdims=True)
    for s in (0, 1):
        pltpu.make_async_copy(most, most, sem.at[s]).wait()
    swap = pltpu.make_async_remote_copy(
        src_ref=total,
        dst_ref=totals.at[pl.ds(1, 1)],
        send_sem=sem.at[9],
        recv_sem=sem.at[10],
        device_id=partner,
        device_id_type=MESH,
    )
    swap.start()
    keep = pltpu.make_async_copy(total, totals.at[pl.ds(0, 1)], sem.at[11])
    keep.start()
    for ref, s in ((most, 2), (few, 4), (most, 3)):
        pltpu.make_async_copy(ref, ref, sem.at[s]).wait()
    keep.wait()
    swap.wait()


def place_kernel(recv, totals, out, rows, both, placed, sem):
    step_rows = DEV * ROWS * 2 // CHUNKS
    step_lines = GX * TX // CHUNKS
    first = pltpu.make_async_copy(totals, both, sem.at[CHUNKS])
    first.start()
    chunks = []
    for i in range(CHUNKS):
        at = pl.ds(i * step_rows, step_rows)
        chunks.append(pltpu.make_async_copy(recv.at[at], rows.at[at], sem.at[i]))
        chunks[-1].start()
    first.wait()
    level = jnp.sum(both[...]) / COUNT + 1e-6
    scale = 1.0 / jnp.full((8, 128), level, jnp.float32)
    lane = lax.broadcasted_iota(jnp.int32, (8, 128), 1) // TY
    pair = lax.broadcasted_iota(jnp.int32, (8, 128), 0) // 2
    step = (pair - lane) % 4
    for i in range(CHUNKS):
        chunks[i].wait()
        for source in range(i * GX // CHUNKS, (i + 1) * GX // CHUNKS):
            for h in range(2):
                for r in range(ROWS):
                    v = rows[pl.ds((source * GY + 4 * h) * 2 * ROWS + r, 8, stride=ROWS), :]
                    w = v
                    for k in range(1, 4):
                        turned = pltpu.roll(pltpu.roll(v, 2 * k, 0), 128 - TY * k, 1)
                        w = jnp.where(step == k, turned, w)
                    placed[r, source * TX : (source + 1) * TX, h * 128 : (h + 1) * 128] = jnp.log(
                        1.0 + w * scale
                    )
        at = pl.ds(i * step_lines, step_lines)
        pltpu.make_async_copy(placed.at[:, at], out.at[:, at], sem.at[CHUNKS + 1]).start()
    pltpu.make_async_copy(placed, out, sem.at[CHUNKS + 1]).wait()


def on_device(spectra, resample_index, resample_weight, disp_phase, surface_block):
    f32 = jnp.float32
    bf16 = jnp.bfloat16
    hbm = pl.BlockSpec(memory_space=pltpu.HBM)
    table = jnp.asarray(base_table(), bf16)
    recv, totals = pl.pallas_call(
        main_kernel,
        out_shape=(
            jax.ShapeDtypeStruct((DEV * ROWS * 2, 128), f32),
            jax.ShapeDtypeStruct((2, 1, 128), f32),
        ),
        in_specs=[hbm] * 6,
        out_specs=[hbm] * 2,
        scratch_shapes=[
            pltpu.VMEM((2, LINES, NK), bf16),
            pltpu.VMEM((3, RADIX, BLOCK), f32),
            pltpu.VMEM((RADIX, BLOCK), jnp.int32),
            pltpu.VMEM((TX, TY), jnp.int32),
            pltpu.VMEM((RADIX, BLOCK, 2 * BLOCK), bf16),
            pltpu.VMEM((RADIX // 2, NK, 2 * BLOCK), bf16),
            pltpu.VMEM((RADIX, LINES // 2, BLOCK), f32),
            pltpu.VMEM((4, 4, 2, LINES // 2, BLOCK), f32),
            pltpu.VMEM((RADIX, LINES // 2, 2 * BLOCK), bf16),
            pltpu.VMEM((2 * KEEP * BLOCK, 128), f32),
            pltpu.VMEM((1, 1, 128), f32),
            pltpu.VMEM((1, 1, 128), f32),
            pltpu.VMEM((DEV // 2, 1, 128), f32),
            pltpu.SemaphoreType.DMA((13,)),
            pltpu.SemaphoreType.DMA((12,)),
        ],
        compiler_params=pltpu.CompilerParams(
            collective_id=0, has_side_effects=True, vmem_limit_bytes=VMEM_BYTES
        ),
        name="main",
    )(
        spectra,
        resample_index.reshape(RADIX, BLOCK),
        resample_weight.reshape(RADIX, BLOCK),
        disp_phase.reshape(RADIX, BLOCK),
        surface_block,
        table,
    )
    return pl.pallas_call(
        place_kernel,
        out_shape=jax.ShapeDtypeStruct((ROWS, GX * TX, GY * TY), f32),
        in_specs=[hbm] * 2,
        out_specs=hbm,
        scratch_shapes=[
            pltpu.VMEM((DEV * ROWS * 2, 128), f32),
            pltpu.VMEM((2, 1, 128), f32),
            pltpu.VMEM((ROWS, GX * TX, GY * TY), f32),
            pltpu.SemaphoreType.DMA((CHUNKS + 2,)),
        ],
        compiler_params=pltpu.CompilerParams(vmem_limit_bytes=VMEM_BYTES),
        name="place",
    )(recv, totals)

def solution(mesh):
    return jax.shard_map(
        on_device,
        mesh=mesh,
        in_specs=(P("gx", "gy", None), P(), P(), P(), P("gx", "gy")),
        out_specs=P(("gx", "gy"), None, None),
        check_vma=False,
    )
```

```python
import itertools
import math

import jax
import jax.numpy as jnp
import numpy as np
from jax import lax
from jax.experimental import pallas as pl
from jax.experimental.pallas import tpu as pltpu
from jax.sharding import PartitionSpec as P

NK = 2048
BLOCK = 128
KEEP = 5
RADIX = 16
GX = 16
GY = 8
DEV = GX * GY
TX = 8
TY = 32
LINES = TX * TY
ROWS = KEEP * BLOCK // DEV
COUNT = 128 * 256 * KEEP * BLOCK
MESH = pl.DeviceIdType.MESH
VMEM_BYTES = 67043328
CHUNKS = 2


def base_table():
    c = np.arange(RADIX)[:, None, None]
    b = np.arange(NK // (2 * RADIX))[None, :, None]
    m = np.arange(BLOCK)[None, None, :]
    angle = 2.0 * math.pi * ((m * (RADIX * b + c)) % NK) / NK
    cos, sin = np.cos(angle), np.sin(angle)
    top = np.concatenate([cos, sin], axis=2)
    low = np.concatenate([-sin, cos], axis=2)
    return np.concatenate([top, low], axis=1).astype(np.float32)


def rot(z, k, n):
    re, im = z
    k = k % n
    if k == 0:
        return re, im
    if 4 * k == n:
        return im, -re
    if 2 * k == n:
        return -re, -im
    if 4 * k == 3 * n:
        return -im, re
    if 8 * k == n:
        h = math.sqrt(0.5)
        return h * (re + im), h * (im - re)
    if 8 * k == 3 * n:
        h = math.sqrt(0.5)
        return h * (im - re), -h * (re + im)
    c, s = math.cos(2 * math.pi * k / n), math.sin(2 * math.pi * k / n)
    return c * re + s * im, c * im - s * re


def add(a, b):
    return a[0] + b[0], a[1] + b[1]


def sub(a, b):
    return a[0] - b[0], a[1] - b[1]


def fft4(z):
    a, b = add(z[0], z[2]), sub(z[0], z[2])
    c, d = add(z[1], z[3]), sub(z[1], z[3])
    d = rot(d, 1, 4)
    return [add(a, c), add(b, d), sub(a, c), sub(b, d)]


def hops(o):
    return sum((0, 1, 2, 1)[v] for v in o[:3])


OFFSETS = sorted(
    [o for o in itertools.product(range(4), range(4), range(4), range(2)) if any(o)],
    key=lambda o: (-hops(o), o),
)


def main_kernel(
    spectra, index, weight, phase, surface, table, recv, totals,
    both, params, idx, surf, tab, hits, x, mid, y, msg, part, total, sums, load, sem,
):
    f32, bf16 = jnp.float32, jnp.bfloat16
    half = LINES // 2
    gx, gy = lax.axis_index("gx"), lax.axis_index("gy")
    me = gx * GY + gy
    zs = [(gx // 4 + d) % 4 for d in range(4)]
    ys = [(gx % 4 + d) % 4 for d in range(4)]
    xs = [(gy // 2 + d) % 4 for d in range(4)]
    cs = [(gy % 2 + d) % 2 for d in range(2)]
    zy = [[z * 4 + v for v in ys] for z in zs]
    xc = [[v * 2 + c for c in cs] for v in xs]
    peers = [(zy[o[0]][o[1]], xc[o[2]][o[3]]) for o in OFFSETS]
    alike = [to for o, to in zip(OFFSETS, peers) if o[3] == 0]
    partner = (zy[0][0], xc[0][1])
    chip = gx * (GY // 2) + gy // 2
    barrier = pltpu.get_barrier_semaphore()

    small = [
        pltpu.make_async_copy(index, idx, load.at[0]),
        pltpu.make_async_copy(weight, params.at[0], load.at[1]),
        pltpu.make_async_copy(phase, params.at[1], load.at[2]),
        pltpu.make_async_copy(surface, surf, load.at[3]),
    ]
    tiles = [
        pltpu.make_async_copy(
            spectra.at[2 * p + q], both.at[q, pl.ds(p * TY, TY)], load.at[4 + 4 * q + p]
        )
        for q in range(2)
        for p in range(4)
    ]
    big = pltpu.make_async_copy(table, tab, load.at[12])
    for copy in small + tiles + [big]:
        copy.start()
    for to in peers:
        pl.semaphore_signal(barrier, inc=1, device_id=to, device_id_type=MESH)
    for copy in small:
        copy.wait()
    cosp = jnp.cos(params[1])
    sinp = jnp.sin(params[1])
    params[1] = cosp
    params[2] = sinp
    tops = [
        jnp.concatenate([surf[2 * p + q : 2 * p + q + 1, :] for p in range(4)], axis=1)
        for q in range(2)
    ]
    row = lax.broadcasted_iota(jnp.int32, (BLOCK, 2 * BLOCK), 0).astype(jnp.int16)
    one = jnp.ones((BLOCK, 2 * BLOCK), bf16)
    zero = jnp.zeros((BLOCK, 2 * BLOCK), bf16)
    nt = (((1,), (1,)), ((), ()))

    def shift(q):
        for copy in tiles[4 * q : 4 * q + 4]:
            copy.wait()
        lines = both[q, :half, :]
        both[q, half:, :] = jnp.concatenate([lines[:, 1:], lines[:, :1]], axis=1)

    def compute(q, acc):
        for n in range(4):
            for e in range(2):
                if q == 0:
                    pick = jnp.concatenate(
                        [idx[n + 8 * e + 4 * h : n + 8 * e + 4 * h + 1, :] for h in range(2)], axis=1
                    ).astype(jnp.int16)
                    for k in range(NK // 128):
                        seen = row + jnp.int16(128 * k) == pick
                        hits[2 * n + e, k * 128 : (k + 1) * 128, :] = jnp.where(seen, one, zero)
                pair = jnp.dot(both[q], hits[2 * n + e], preferred_element_type=f32)
                for h in range(2):
                    at = n + 8 * e + 4 * h
                    lane = slice(h * BLOCK, (h + 1) * BLOCK)
                    w = params[0, at : at + 1, :]
                    x[at] = (1.0 - w) * pair[:half, lane] + w * pair[half:, lane]
            for g in range(half // 16):
                rows = slice(16 * g, 16 * g + 16)
                z = []
                for m in range(4):
                    at = n + 4 * m
                    v = x[at, rows, :]
                    z.append(
                        [
                            (v * params[1 + o, at : at + 1, :]).astype(bf16).astype(f32)
                            for o in range(2)
                        ]
                    )
                for c, value in enumerate(fft4(z)):
                    for o, half_value in enumerate(rot(value, n * c, RADIX)):
                        mid[n, c, o, rows, :] = half_value
        if q == 0:
            big.wait()
        for low in range(4):
            for g in range(half // 16):
                rows = slice(16 * g, 16 * g + 16)
                z = [[mid[n, low, o, rows, :] for o in range(2)] for n in range(4)]
                for high, value in enumerate(fft4(z)):
                    for o in range(2):
                        y[low + 4 * high, rows, o * BLOCK : (o + 1) * BLOCK] = value[o].astype(bf16)
            for c in range(low, RADIX, 4):
                depth = lax.dot_general(tab[c], y[c], nt, preferred_element_type=f32)
                power = depth[:64] * depth[:64] + depth[64:] * depth[64:]
                tile = [power[8 * b : 8 * b + 8] for b in range(8)]
                for k in range(KEEP):
                    kept = tile[k]
                    for s in range(1, 4):
                        kept = jnp.where(tops[q] == s, tile[k + s], kept)
                    acc = acc + kept
                    msg[pl.ds((q * KEEP + k) * BLOCK + c, 8, stride=RADIX), :] = kept
        return acc

    def slab(q, dest):
        return msg.at[pl.ds(q * KEEP * BLOCK + ROWS * dest, ROWS)]

    def landing(q):
        return recv.at[pl.ds((2 * me + q) * ROWS, ROWS)]

    def send(q, among):
        for to in among:
            pltpu.make_async_remote_copy(
                src_ref=slab(q, to[0] * GY + to[1]),
                dst_ref=landing(q),
                send_sem=sem.at[2 * q],
                recv_sem=sem.at[2 * q + 1],
                device_id=to,
                device_id_type=MESH,
            ).start()

    shift(0)
    acc = compute(0, jnp.zeros((8, 128), f32))
    pl.semaphore_wait(barrier, DEV - 1)
    send(0, peers)
    shift(1)
    acc = compute(1, acc)
    part[...] = jnp.sum(acc, axis=0, keepdims=True).reshape(1, 1, 128)
    for to in alike:
        pltpu.make_async_remote_copy(
            src_ref=part,
            dst_ref=sums.at[pl.ds(chip, 1)],
            send_sem=sem.at[4],
            recv_sem=sem.at[5],
            device_id=to,
            device_id_type=MESH,
        ).start()
    send(1, peers)
    own = [pltpu.make_async_copy(slab(q, me), landing(q), sem.at[6 + q]) for q in range(2)]
    own.append(pltpu.make_async_copy(part, sums.at[pl.ds(chip, 1)], sem.at[8]))
    for copy in own:
        copy.start()
    for copy in own:
        copy.wait()
    most = recv.at[pl.ds(0, (DEV - 1) * ROWS)]
    few = sums.at[pl.ds(0, DEV // 2 - 1)]
    pltpu.make_async_copy(few, few, sem.at[5]).wait()
    total[...] = jnp.sum(sums[...], axis=0, keepdims=True)
    for s in (0, 1):
        pltpu.make_async_copy(most, most, sem.at[s]).wait()
    swap = pltpu.make_async_remote_copy(
        src_ref=total,
        dst_ref=totals.at[pl.ds(1, 1)],
        send_sem=sem.at[9],
        recv_sem=sem.at[10],
        device_id=partner,
        device_id_type=MESH,
    )
    swap.start()
    keep = pltpu.make_async_copy(total, totals.at[pl.ds(0, 1)], sem.at[11])
    keep.start()
    for ref, s in ((most, 2), (few, 4), (most, 3)):
        pltpu.make_async_copy(ref, ref, sem.at[s]).wait()
    keep.wait()
    swap.wait()


def place_kernel(recv, totals, out, rows, both, placed, sem):
    step_rows = DEV * ROWS * 2 // CHUNKS
    step_lines = GX * TX // CHUNKS
    first = pltpu.make_async_copy(totals, both, sem.at[CHUNKS])
    first.start()
    chunks = []
    for i in range(CHUNKS):
        at = pl.ds(i * step_rows, step_rows)
        chunks.append(pltpu.make_async_copy(recv.at[at], rows.at[at], sem.at[i]))
        chunks[-1].start()
    first.wait()
    level = jnp.sum(both[...]) / COUNT + 1e-6
    scale = 1.0 / jnp.full((8, 128), level, jnp.float32)
    lane = lax.broadcasted_iota(jnp.int32, (8, 128), 1) // TY
    pair = lax.broadcasted_iota(jnp.int32, (8, 128), 0) // 2
    step = (pair - lane) % 4
    for i in range(CHUNKS):
        chunks[i].wait()
        for source in range(i * GX // CHUNKS, (i + 1) * GX // CHUNKS):
            for h in range(2):
                for r in range(ROWS):
                    v = rows[pl.ds((source * GY + 4 * h) * 2 * ROWS + r, 8, stride=ROWS), :]
                    w = v
                    for k in range(1, 4):
                        turned = pltpu.roll(pltpu.roll(v, 2 * k, 0), 128 - TY * k, 1)
                        w = jnp.where(step == k, turned, w)
                    placed[r, source * TX : (source + 1) * TX, h * 128 : (h + 1) * 128] = jnp.log(
                        1.0 + w * scale
                    )
        at = pl.ds(i * step_lines, step_lines)
        pltpu.make_async_copy(placed.at[:, at], out.at[:, at], sem.at[CHUNKS + 1]).start()
    pltpu.make_async_copy(placed, out, sem.at[CHUNKS + 1]).wait()


def on_device(spectra, resample_index, resample_weight, disp_phase, surface_block):
    f32 = jnp.float32
    bf16 = jnp.bfloat16
    hbm = pl.BlockSpec(memory_space=pltpu.HBM)
    table = jnp.asarray(base_table(), bf16)
    recv, totals = pl.pallas_call(
        main_kernel,
        out_shape=(
            jax.ShapeDtypeStruct((DEV * ROWS * 2, 128), f32),
            jax.ShapeDtypeStruct((2, 1, 128), f32),
        ),
        in_specs=[hbm] * 6,
        out_specs=[hbm] * 2,
        scratch_shapes=[
            pltpu.VMEM((2, LINES, NK), bf16),
            pltpu.VMEM((3, RADIX, BLOCK), f32),
            pltpu.VMEM((RADIX, BLOCK), jnp.int32),
            pltpu.VMEM((TX, TY), jnp.int32),
            pltpu.VMEM((RADIX, BLOCK, 2 * BLOCK), bf16),
            pltpu.VMEM((RADIX // 2, NK, 2 * BLOCK), bf16),
            pltpu.VMEM((RADIX, LINES // 2, BLOCK), f32),
            pltpu.VMEM((4, 4, 2, LINES // 2, BLOCK), f32),
            pltpu.VMEM((RADIX, LINES // 2, 2 * BLOCK), bf16),
            pltpu.VMEM((2 * KEEP * BLOCK, 128), f32),
            pltpu.VMEM((1, 1, 128), f32),
            pltpu.VMEM((1, 1, 128), f32),
            pltpu.VMEM((DEV // 2, 1, 128), f32),
            pltpu.SemaphoreType.DMA((13,)),
            pltpu.SemaphoreType.DMA((12,)),
        ],
        compiler_params=pltpu.CompilerParams(
            collective_id=0, has_side_effects=True, vmem_limit_bytes=VMEM_BYTES
        ),
        name="main",
    )(
        spectra,
        resample_index.reshape(RADIX, BLOCK),
        resample_weight.reshape(RADIX, BLOCK),
        disp_phase.reshape(RADIX, BLOCK),
        surface_block,
        table,
    )
    return pl.pallas_call(
        place_kernel,
        out_shape=jax.ShapeDtypeStruct((ROWS, GX * TX, GY * TY), f32),
        in_specs=[hbm] * 2,
        out_specs=hbm,
        scratch_shapes=[
            pltpu.VMEM((DEV * ROWS * 2, 128), f32),
            pltpu.VMEM((2, 1, 128), f32),
            pltpu.VMEM((ROWS, GX * TX, GY * TY), f32),
            pltpu.SemaphoreType.DMA((CHUNKS + 2,)),
        ],
        compiler_params=pltpu.CompilerParams(vmem_limit_bytes=VMEM_BYTES),
        name="place",
    )(recv, totals)

def solution(mesh):
    return jax.shard_map(
        on_device,
        mesh=mesh,
        in_specs=(P("gx", "gy", None), P(), P(), P(), P("gx", "gy")),
        out_specs=P(("gx", "gy"), None, None),
        check_vma=False,
    )
```
